32 devices in a mesh: dp: 8 (over y, x, core), tensor: 4 (over z).
Axes of the slice: x: 2, y: 2, z: 4, core: 2. Of those that a mesh axis runs over, the one named last changes fastest.
Arguments:
- hidden_in: bfloat16 [24576, 1536], P(('dp', 'tensor')), may hold values from -6 to 6
- out_grad: bfloat16 [24576, 1536], P(('dp', 'tensor')), may hold values from -6 to 6
- segment_ids: int32 [8, 1024], P('dp'), may hold values from 0 to 3, never falling along the last dimension, each value on 1 to 512 neighbouring positions
- expert_ids: int32 [24576, 8], P('dp'), may hold values from 0 to 39, all different within a row
- fill_order: int32 [8, 24576], P('dp'), may hold values from 0 to 24575, each once within a row
- attention_gain: bfloat16 [1536], P('dp'), may hold values from 0.5 to 1.5
- query_weight: bfloat16 [1536, 1536], P('dp', 'tensor'), may hold values from -0.625 to 0.625
- key_weight: bfloat16 [1536, 512], P('dp', 'tensor'), may hold values from -0.625 to 0.625
- value_weight: bfloat16 [1536, 512], P('dp', 'tensor'), may hold values from -0.15625 to 0.15625
- output_weight: bfloat16 [1536, 1536], P('tensor', 'dp'), may hold values from -3 to 3
- mixture_gain: bfloat16 [1536], P('dp'), may hold values from 0.5 to 1.5
- router_weight: bfloat16 [1536, 40], P('dp'), may hold values from -0.079589844 to 0.079589844
- gate_weight: bfloat16 [40, 1536, 512], P('tensor', 'dp'), may hold values from -0.15625 to 0.15625
- up_weight: bfloat16 [40, 1536, 512], P('tensor', 'dp'), may hold values from -0.15625 to 0.15625
- down_weight: bfloat16 [40, 512, 1536], P('tensor', None, 'dp'), may hold values from -4 to 4
Outputs:
- block_output: bfloat16 [24576, 1536], P(('dp', 'tensor'))
- input_grad: float32 [24576, 1536], P(('dp', 'tensor'))
- attention_gain_grad: float32 [1536], P(('dp', 'tensor'))
- query_weight_grad: float32 [1536, 1536], P('dp', 'tensor')
- key_weight_grad: float32 [1536, 512], P('dp', 'tensor')
- value_weight_grad: float32 [1536, 512], P('dp', 'tensor')
- output_weight_grad: float32 [1536, 1536], P('tensor', 'dp')
- mixture_gain_grad: float32 [1536], P(('dp', 'tensor'))
- router_weight_grad: float32 [1536, 40], P(('dp', 'tensor'))
- gate_weight_grad: float32 [40, 1536, 512], P('tensor', 'dp')
- up_weight_grad: float32 [40, 1536, 512], P('tensor', 'dp')
- down_weight_grad: float32 [40, 512, 1536], P('tensor', None, 'dp')
The draws below stay inside these ranges and needn't reach their ends.
Inputs may be any that keep to these rules, and one draw needn't show every extreme that they name: `segment_ids`: within a group the continuation numbers never fall; each of the 4 numbers labels 1 to 512 positions. `expert_ids`: A token's 8 experts are distinct. `fill_order`: each row lists every pair number t * 8 + k of the group's tokens once.
All inputs are finite; a program needn't handle non-finite values.
Results may differ from the reference program's by a relative error of at most 0.022.
Values may be sent and summed in bfloat16 or wider, within the bound.
A program may use at most 640 MiB of HBM per device.

```python
import math
import jax
import jax.numpy as jnp
import numpy as np
from jax import lax

D = 1536
HEADS = 24
KV = 8
HD = 64
FF = 512
EXPERTS = 40
TOPK = 8
PROMPT = 2048
NCONT = 4
CONT_TOK = 1024
QBLK = 512
EBLK = 1
CONT_MOST = 512
TOK_GRP = 3072
GROUPS = 8
TOKENS = 24576
CAP = 768
N_DP = 8


def levels(own_key, shape, cuts, least, high):
    loudness = 1.0
    for axis_at, shards_of in cuts:
        draws = jax.random.uniform(jax.random.fold_in(jax.random.fold_in(own_key, 6), axis_at), (shards_of,), jnp.float32, least / len(cuts), high / len(cuts))
        loudness = loudness * jnp.repeat(jnp.exp(draws), shape[axis_at] // shards_of).reshape((-1,) + (1,) * (len(shape) - 1 - axis_at))
    return loudness


def picks_of(stream_key, rows, count, top, lift):
    order = jax.random.permutation(jax.random.fold_in(stream_key, 1), count)
    pull = order
    for power in range(3):
        pull = pull * pull // count
    pull = pull * lift // count
    chance = jax.random.randint(jax.random.fold_in(stream_key, 2), (rows, count), 0, 4096) + pull
    fixed_rows = jax.random.permutation(jax.random.fold_in(stream_key, 3), rows)[jnp.arange(count) % rows]
    chance = jnp.where(jnp.arange(rows)[:, None] == fixed_rows[None, :], 1 << 14, chance)
    priority = chance * count + jnp.arange(count)
    return lax.top_k(priority.astype(jnp.int32), top)[1].astype(jnp.int32)


def profile(amount, total, bound, lean):
    portions = [(1 << 20) // math.isqrt(rank ** lean) + 1 for rank in range(2, amount + 1)]
    surplus, given = total - bound - (amount - 1), [1] * (amount - 1)
    while surplus > 0:
        candidates = [i for i in range(amount - 1) if given[i] < bound]
        pool, remaining = sum([portions[i] for i in candidates]), surplus
        for i in candidates:
            more = min(bound - given[i], max(1, remaining * portions[i] // pool), surplus)
            given[i] = given[i] + more
            surplus = surplus - more
    return np.array([bound] + given)


def uneven(stream_key, count, total, most, skew):
    if count == 2:
        one = jax.random.randint(stream_key, (), max(1, total - most), min(most, total - 1) + 1)
        return jnp.stack([one, total - one])
    tallies = jnp.asarray(profile(count, total, most, skew), jnp.int32)
    pairs = (count - 1) // 2
    donor, taker = tallies[1:1 + 2 * pairs:2], tallies[2:2 + 2 * pairs:2]
    slack = jnp.minimum(donor - 1, most - taker)
    passed = jax.random.randint(jax.random.fold_in(stream_key, 1), (pairs,), 0, 1 << 20) % (slack + 1)
    tallies = tallies.at[1:1 + 2 * pairs:2].set(donor - passed).at[2:2 + 2 * pairs:2].set(taker + passed)
    return tallies[jax.random.permutation(jax.random.fold_in(stream_key, 2), count)]


def normal_values(rng, extent, width, limit, shards=(), kind=jnp.bfloat16):
    entries = width * jax.random.normal(rng, extent, jnp.float32)
    if shards:
        entries = entries * levels(rng, extent, shards, -0.22, 0.18)
    return jnp.clip(entries, -limit, limit).astype(kind)


def setup_inputs(seed: int = 0) -> dict:
    key_of = jax.random.split(jax.random.key(seed), 16)
    return {
        "hidden_in": normal_values(key_of[0], (TOKENS, D), 1.0, 6.0, ((0, 32),)),
        "out_grad": normal_values(key_of[1], (TOKENS, D), 1.0, 6.0, ((0, 32),)),
        "segment_ids": jax.vmap(lambda own: jnp.searchsorted(jnp.cumsum(uneven(own, NCONT, CONT_TOK, CONT_MOST, 1)), jnp.arange(CONT_TOK), side="right"))(jax.random.split(key_of[2], GROUPS)).reshape((GROUPS, CONT_TOK)).astype(jnp.int32),
        "expert_ids": picks_of(key_of[3], TOKENS, EXPERTS, TOPK, 1638),
        "fill_order": jax.vmap(lambda own: jax.random.permutation(own, TOK_GRP * TOPK))(jax.random.split(key_of[4], GROUPS)).reshape((GROUPS, TOK_GRP * TOPK)).astype(jnp.int32),
        "attention_gain": jnp.clip(1.0 + 0.1 * jax.random.normal(key_of[5], (D,), jnp.float32), 0.5, 1.5).astype(jnp.bfloat16),
        "query_weight": normal_values(key_of[6], (D, HEADS * HD), (D // 16) ** -0.5, 0.625, ((0, 8), (1, 4))),
        "key_weight": normal_values(key_of[7], (D, KV * HD), (D // 16) ** -0.5, 0.625, ((0, 8), (1, 4))),
        "value_weight": normal_values(key_of[8], (D, KV * HD), D ** -0.5, 0.15625, ((0, 8), (1, 4))),
        "output_weight": normal_values(key_of[9], (HEADS * HD, D), 4 ** -0.5, 3.0, ((0, 4), (1, 8))),
        "mixture_gain": jnp.clip(1.0 + 0.1 * jax.random.normal(key_of[10], (D,), jnp.float32), 0.5, 1.5).astype(jnp.bfloat16),
        "router_weight": normal_values(key_of[11], (D, EXPERTS), 0.0128, 0.079589844, ((0, 8),)),
        "gate_weight": normal_values(key_of[12], (EXPERTS, D, FF), D ** -0.5, 0.15625, ((0, 4), (1, 8))),
        "up_weight": normal_values(key_of[13], (EXPERTS, D, FF), D ** -0.5, 0.15625, ((0, 4), (1, 8))),
        "down_weight": normal_values(key_of[14], (EXPERTS, FF, D), 2 ** -0.5, 4.0, ((0, 4), (2, 8))),
    }


ATTN_SCALE = 0.015625
RESIDUAL_SCALE = 0.22
NORM_EPS = 1e-06
ROPE_BASE = 10000.0
HIGHEST = lax.Precision.HIGHEST

@jax.custom_vjp
def low(v):
    return lax.optimization_barrier(v.astype(jnp.bfloat16)).astype(jnp.float32)

@jax.custom_vjp
def low_back(v):
    return v

def low_keep(v):
    return (low(v), None)

def low_pass(kept, grad):
    return (grad,)

def back_keep(v):
    return (v, None)

def back_low(kept, grad):
    return (low(grad),)
low.defvjp(low_keep, low_pass)
low_back.defvjp(back_keep, back_low)

def rms_norm(values, gain_row):
    inverse_rms = lax.rsqrt(lax.optimization_barrier(jnp.mean(values * values, axis=-1, keepdims=True)) + NORM_EPS)
    return values * inverse_rms * gain_row

def group_layout(segment_row, prompt_length):
    cont_length = segment_row.shape[0]
    segment_marks = (segment_row[:, None] == jnp.arange(NCONT, dtype=jnp.int32)[None, :]).astype(jnp.int32)
    segment_sizes = lax.optimization_barrier(jnp.sum(segment_marks, axis=0))
    segment_starts = jnp.cumsum(segment_sizes) - segment_sizes
    token_starts = lax.optimization_barrier(jnp.sum(segment_marks * segment_starts[None, :], axis=1))
    inside = jnp.arange(cont_length, dtype=jnp.int32) - token_starts
    positions = jnp.concatenate([jnp.arange(prompt_length, dtype=jnp.int32), prompt_length + inside])
    segments = jnp.concatenate([jnp.zeros((prompt_length,), jnp.int32), segment_row + 1])
    return (positions, segments)

def allowed(query_index, query_segment, key_index, key_segment):
    causal = key_index[None, :] <= query_index[:, None]
    shared = (key_segment[None, :] == 0) | (key_segment[None, :] == query_segment[:, None])
    return causal & shared

def rope_tables(positions, head_size):
    halfway = head_size // 2
    frequency = ROPE_BASE ** (-(2.0 * jnp.arange(halfway, dtype=jnp.float32)) / head_size)
    angles = positions.astype(jnp.float32)[:, None] * frequency[None, :]
    return (jnp.cos(angles), jnp.sin(angles))

def rotate(values, cosine_table, sine_table):
    halfway = values.shape[-1] // 2
    first_half = values[..., :halfway]
    second_half = values[..., halfway:]
    cosine_part = cosine_table[:, None, :]
    sine_part = sine_table[:, None, :]
    return jnp.concatenate([first_half * cosine_part - second_half * sine_part, second_half * cosine_part + first_half * sine_part], axis=-1)

def route_slots(expert_row, order_row):
    pair_count = expert_row.shape[0] * expert_row.shape[1]
    ordered = jnp.take(expert_row.reshape(pair_count), order_row)
    onehot = (ordered[:, None] == jnp.arange(EXPERTS, dtype=jnp.int32)[None, :]).astype(jnp.int32)
    pair_rank = lax.optimization_barrier(jnp.sum(onehot * jnp.cumsum(onehot, axis=0), axis=1)) - 1
    slot_index = jnp.where(pair_rank < CAP, ordered * CAP + pair_rank, EXPERTS * CAP)
    return jnp.full((EXPERTS * CAP,), -1, jnp.int32).at[slot_index].set(order_row, mode='drop')

def attention(query_rot, key_rot, value_low, segments):
    tokens_total = query_rot.shape[0]
    repeat = HEADS // KV
    keys_all = jnp.repeat(key_rot, repeat, axis=1)
    values_all = jnp.repeat(value_low, repeat, axis=1)
    key_index = jnp.arange(tokens_total, dtype=jnp.int32)

    def one_block(block_index):
        row_start = (block_index * QBLK).astype(jnp.int32)
        queries = lax.dynamic_slice_in_dim(query_rot, row_start, QBLK, 0)
        query_index = row_start + jnp.arange(QBLK, dtype=jnp.int32)
        query_segment = lax.dynamic_slice_in_dim(segments, row_start, QBLK, 0)
        scores = low_back(jnp.einsum('qhd,khd->hqk', queries, keys_all, precision=HIGHEST) * ATTN_SCALE)
        visible = allowed(query_index, query_segment, key_index, segments)
        scores = jnp.where(visible[None], scores, -1e+30)
        softmax_weights = low(jax.nn.softmax(scores, axis=-1))
        return jnp.einsum('hqk,khd->qhd', softmax_weights, values_all, precision=HIGHEST)
    blocks = lax.map(jax.checkpoint(one_block), jnp.arange(tokens_total // QBLK, dtype=jnp.int32))
    return blocks.reshape(tokens_total, HEADS, HD)

def group_forward(hidden, params, positions, segments, slot_token, slot_pair, routed_marks):
    attention_gain, query_weight, key_weight, value_weight, output_weight, mixture_gain, router_weight, gate_weight, up_weight, down_weight = params
    tokens_total = hidden.shape[0]
    normed = low(rms_norm(hidden, attention_gain))
    query_pre = low_back(jnp.dot(normed, query_weight, precision=HIGHEST)).reshape(tokens_total, HEADS, HD)
    key_pre = low_back(jnp.dot(normed, key_weight, precision=HIGHEST)).reshape(tokens_total, KV, HD)
    value_low = low(low_back(jnp.dot(normed, value_weight, precision=HIGHEST))).reshape(tokens_total, KV, HD)
    cosine_table, sine_table = rope_tables(positions, HD)
    query_rot = low(rotate(query_pre, cosine_table, sine_table))
    key_rot = low(rotate(key_pre, cosine_table, sine_table))
    mixed = low(low_back(attention(query_rot, key_rot, value_low, segments))).reshape(tokens_total, HEADS * HD)
    attended = low_back(jnp.dot(mixed, output_weight, precision=HIGHEST))
    middle = hidden + RESIDUAL_SCALE * attended
    normed_two = low(rms_norm(middle, mixture_gain))
    logits = jnp.dot(normed_two, router_weight, precision=HIGHEST)
    routed = lax.optimization_barrier(jnp.sum(routed_marks * logits[:, None, :], axis=-1))
    gates = jax.nn.softmax(routed, axis=-1)
    slot_valid = slot_pair >= 0
    slot_gate = jnp.where(slot_valid, jnp.take(gates.reshape(-1), jnp.maximum(slot_pair, 0)), 0.0)
    block_total = EXPERTS // EBLK

    def expert_block(running, block_data):
        gate_part, up_part, down_part, tokens_here, gate_here = block_data
        inputs = low_back(jnp.take(normed_two, tokens_here, axis=0)).reshape(EBLK, CAP, D)
        gate_pre = low_back(jnp.einsum('ecd,edf->ecf', inputs, gate_part, precision=HIGHEST))
        up_pre = low_back(jnp.einsum('ecd,edf->ecf', inputs, up_part, precision=HIGHEST))
        hidden_units = low(gate_here[:, :, None] * jax.nn.silu(gate_pre) * up_pre)
        outputs = low_back(jnp.einsum('ecf,efd->ecd', hidden_units, down_part, precision=HIGHEST))
        return (running.at[tokens_here].add(outputs.reshape(EBLK * CAP, D)), None)
    block_data = (gate_weight.reshape(block_total, EBLK, D, FF), up_weight.reshape(block_total, EBLK, D, FF), down_weight.reshape(block_total, EBLK, FF, D), slot_token.reshape(block_total, EBLK * CAP), slot_gate.reshape(block_total, EBLK, CAP))
    mixture_sum, unused_rest = lax.scan(jax.checkpoint(expert_block), jnp.zeros_like(middle), block_data)
    return middle + RESIDUAL_SCALE * mixture_sum

def reference(hidden_in, out_grad, segment_ids, expert_ids, fill_order, attention_gain, query_weight, key_weight, value_weight, output_weight, mixture_gain, router_weight, gate_weight, up_weight, down_weight):
    params = jax.tree.map(lambda weight: weight.astype(jnp.float32), (attention_gain, query_weight, key_weight, value_weight, output_weight, mixture_gain, router_weight, gate_weight, up_weight, down_weight))

    def one_group(totals, group_data):
        hidden, cotangent, segment_row, expert_row, order_row = group_data
        positions, segments = group_layout(segment_row, PROMPT)
        slot_pair = route_slots(expert_row, order_row)
        slot_token = jnp.maximum(slot_pair, 0) // TOPK
        routed_marks = (expert_row[:, :, None] == jnp.arange(EXPERTS, dtype=jnp.int32)[None, None, :]).astype(jnp.float32)

        def forward(hidden_value, params_value):
            return group_forward(hidden_value, params_value, positions, segments, slot_token, slot_pair, routed_marks)
        output, pullback = jax.vjp(forward, hidden.astype(jnp.float32), params)
        hidden_grad, param_grads = pullback(cotangent.astype(jnp.float32))
        totals = jax.tree.map(lambda running, update: running + update, totals, param_grads)
        return (totals, (output.astype(jnp.bfloat16), hidden_grad))
    zero_grads = jax.tree.map(jnp.zeros_like, params)
    group_data = (hidden_in.reshape(N_DP, TOK_GRP, D), out_grad.reshape(N_DP, TOK_GRP, D), segment_ids, expert_ids.reshape(N_DP, TOK_GRP, TOPK), fill_order)
    grads, (outputs, input_grads) = lax.scan(one_group, zero_grads, group_data)
    return (outputs.reshape(TOKENS, D), input_grads.reshape(TOKENS, D), grads[0], grads[1], grads[2], grads[3], grads[4], grads[5], grads[6], grads[7], grads[8], grads[9])
```

```python
import jax
import jax.numpy as jnp
from jax import lax
from jax.experimental import pallas as pl
from jax.experimental.pallas import tpu as pltpu
from jax.sharding import PartitionSpec as P

D = 1536
HD = 64
EXPERTS = 40
TOPK = 8
PROMPT = 2048
NCONT = 4
QBLK = 512
TOK_GRP = 3072
CAP = 768


ATTN_SCALE = 0.015625
RESIDUAL_SCALE = 0.22
NORM_EPS = 1e-06
ROPE_BASE = 10000.0
MASKED = -1e30
HIGHEST = lax.Precision.HIGHEST


def rms_forward(values, gain_row):
    inverse_rms = lax.rsqrt(jnp.mean(values * values, axis=-1, keepdims=True) + NORM_EPS)
    unit_rows = values * inverse_rms
    return (unit_rows * gain_row, unit_rows, inverse_rms)


def rms_backward(gradient, unit_rows, inverse_rms, gain_row):
    gain_grad = jnp.sum(gradient * unit_rows, axis=0)
    scaled = gradient * gain_row
    mean_term = jnp.mean(scaled * unit_rows, axis=-1, keepdims=True)
    return (inverse_rms * (scaled - unit_rows * mean_term), gain_grad)


def group_layout(segment_row, prompt_length):
    cont_length = segment_row.shape[0]
    segment_marks = (segment_row[:, None] == jnp.arange(NCONT, dtype=jnp.int32)[None, :]).astype(
        jnp.int32
    )
    segment_sizes = jnp.sum(segment_marks, axis=0)
    segment_starts = jnp.cumsum(segment_sizes) - segment_sizes
    token_starts = jnp.sum(segment_marks * segment_starts[None, :], axis=1)
    inside = jnp.arange(cont_length, dtype=jnp.int32) - token_starts
    positions = jnp.concatenate(
        [jnp.arange(prompt_length, dtype=jnp.int32), prompt_length + inside]
    )
    segments = jnp.concatenate([jnp.zeros((prompt_length,), jnp.int32), segment_row + 1])
    return (positions, segments)


def allowed(query_index, query_segment, key_index, key_segment):
    causal = key_index[None, :] <= query_index[:, None]
    shared = (key_segment[None, :] == 0) | (key_segment[None, :] == query_segment[:, None])
    return causal & shared


def rope_tables(positions, head_size):
    halfway = head_size // 2
    frequency = ROPE_BASE ** (-(2.0 * jnp.arange(halfway, dtype=jnp.float32)) / head_size)
    angles = positions.astype(jnp.float32)[:, None] * frequency[None, :]
    return (jnp.cos(angles), jnp.sin(angles))


def rotate(values, cosine_table, sine_table):
    halfway = values.shape[-1] // 2
    first_half = values[..., :halfway]
    second_half = values[..., halfway:]
    cosine_part = cosine_table[:, None, :]
    sine_part = sine_table[:, None, :]
    return jnp.concatenate(
        [
            first_half * cosine_part - second_half * sine_part,
            second_half * cosine_part + first_half * sine_part,
        ],
        axis=-1,
    )


def rotate_back(gradient, cosine_table, sine_table):
    halfway = gradient.shape[-1] // 2
    first_half = gradient[..., :halfway]
    second_half = gradient[..., halfway:]
    cosine_part = cosine_table[:, None, :]
    sine_part = sine_table[:, None, :]
    return jnp.concatenate(
        [
            first_half * cosine_part + second_half * sine_part,
            second_half * cosine_part - first_half * sine_part,
        ],
        axis=-1,
    )


def silu_slope(values):
    sigmoid_part = jax.nn.sigmoid(values)
    return sigmoid_part * (1.0 + values * (1.0 - sigmoid_part))


def route_slots(expert_row, order_row, first_slot, slot_count):
    pair_count = expert_row.shape[0] * expert_row.shape[1]
    ordered = table_lookup(expert_row.reshape(pair_count), order_row)
    onehot = ordered[:, None] == jnp.arange(EXPERTS, dtype=jnp.int32)[None, :]
    rank_block = 256
    blocks = pair_count // rank_block
    pair_marks = onehot.astype(jnp.bfloat16).reshape(blocks, rank_block, EXPERTS)
    lower_ones = (jnp.arange(rank_block)[:, None] >= jnp.arange(rank_block)[None, :]).astype(
        jnp.bfloat16
    )
    within = jnp.einsum(
        "ij,bje->bie", lower_ones, pair_marks, preferred_element_type=jnp.float32
    ).astype(jnp.int32)
    totals = within[:, -1, :]
    before = jnp.cumsum(totals, axis=0) - totals
    counts = (within + before[:, None, :]).reshape(pair_count, EXPERTS)
    pair_rank = jnp.sum(jnp.where(onehot, counts, 0), axis=1) - 1
    local_slot = ordered * CAP + pair_rank - first_slot
    kept = (pair_rank < CAP) & (local_slot >= 0) & (local_slot < slot_count)
    local_slot = jnp.where(kept, local_slot, -1)
    return invert_slots(local_slot, order_row, slot_count)


def _gather_rows_kernel(tok_ref, src_ref, out_ref, buf, sem):
    rows = buf.shape[0]
    base = pl.program_id(0) * rows

    def start(s, carry):
        t = tok_ref[base + s]
        pltpu.make_async_copy(src_ref.at[pl.ds(t, 1)], buf.at[pl.ds(s, 1)], sem).start()
        return carry

    lax.fori_loop(0, rows, start, 0, unroll=8)
    pltpu.make_async_copy(src_ref.at[pl.ds(0, rows)], buf, sem).wait()
    out_ref[...] = buf[...].astype(out_ref.dtype)


def gather_rows(tok, src, rows, out_dtype):
    blocks, width = tok.shape[0] // rows, src.shape[1]
    return pl.pallas_call(
        _gather_rows_kernel,
        grid_spec=pltpu.PrefetchScalarGridSpec(
            num_scalar_prefetch=1,
            grid=(blocks,),
            in_specs=[pl.BlockSpec(memory_space=pl.ANY)],
            out_specs=pl.BlockSpec((rows, width), lambda b, tok: (b, 0)),
            scratch_shapes=[pltpu.VMEM((rows, width), jnp.float32), pltpu.SemaphoreType.DMA(())],
        ),
        out_shape=jax.ShapeDtypeStruct((tok.shape[0], width), out_dtype),
    )(tok, src)


def _combine_rows_kernel(tok_ref, add_ref, out_ref, acc_ref, sem):
    rows = add_ref.shape[0]
    step = pl.program_id(0)

    @pl.when(step == 0)
    def _():
        acc_ref[...] = jnp.zeros_like(acc_ref)

    base = step * rows

    def body(s, carry):
        t = tok_ref[base + s]
        acc_ref[pl.ds(t, 1), :] += add_ref[pl.ds(s, 1), :]
        return carry

    lax.fori_loop(0, rows, body, 0, unroll=8)

    @pl.when(step == pl.num_programs(0) - 1)
    def _():
        copy = pltpu.make_async_copy(acc_ref, out_ref, sem)
        copy.start()
        copy.wait()


def combine_rows(tok, addend, rows, total_rows):
    blocks, width = tok.shape[0] // rows, addend.shape[1]
    return pl.pallas_call(
        _combine_rows_kernel,
        grid_spec=pltpu.PrefetchScalarGridSpec(
            num_scalar_prefetch=1,
            grid=(blocks,),
            in_specs=[pl.BlockSpec((rows, width), lambda b, tok: (b, 0))],
            out_specs=pl.BlockSpec(memory_space=pl.ANY),
            scratch_shapes=[
                pltpu.VMEM((total_rows, width), jnp.float32),
                pltpu.SemaphoreType.DMA(()),
            ],
        ),
        out_shape=jax.ShapeDtypeStruct((total_rows, width), jnp.float32),
        compiler_params=pltpu.CompilerParams(vmem_limit_bytes=48 * 1024 * 1024),
    )(tok, addend)


def table_lookup(table, index):
    lanes = 128
    high_count = table.shape[0] // lanes
    low_marks = (index[:, None] % lanes == jnp.arange(lanes)[None, :]).astype(jnp.bfloat16)
    picked = jnp.dot(
        low_marks,
        table.reshape(high_count, lanes).astype(jnp.bfloat16).T,
        preferred_element_type=jnp.float32,
    )
    high_marks = index[:, None] // lanes == jnp.arange(high_count)[None, :]
    return jnp.sum(jnp.where(high_marks, picked, 0.0), axis=1).astype(jnp.int32)


def invert_slots(local_slot, values, slot_count):
    lanes = 128
    high_count = slot_count // lanes
    column_marks = (local_slot[:, None] // lanes == jnp.arange(high_count)[None, :]).astype(
        jnp.bfloat16
    )
    lane_marks = local_slot[:, None] % lanes == jnp.arange(lanes)[None, :]
    shifted = values + 1
    parts = []
    for digit in (shifted // 256, shifted % 256):
        spread = jnp.where(lane_marks, digit[:, None], 0).astype(jnp.bfloat16)
        parts.append(
            jnp.einsum("ic,il->cl", column_marks, spread, preferred_element_type=jnp.float32)
        )
    return (256.0 * parts[0] + parts[1]).astype(jnp.int32).reshape(slot_count) - 1


def block_scores(query_rot, key_rot, segments, row_start, key_end, local_groups, group_ratio):
    queries = query_rot[row_start:key_end].reshape(
        key_end - row_start, local_groups, group_ratio, HD
    )
    raw_scores = (
        jnp.einsum("qgrd,kgd->grqk", queries, key_rot[:key_end], preferred_element_type=jnp.float32)
        * ATTN_SCALE
    )
    visible = allowed(
        jnp.arange(row_start, key_end, dtype=jnp.int32),
        segments[row_start:key_end],
        jnp.arange(key_end, dtype=jnp.int32),
        segments[:key_end],
    )
    return (jnp.where(visible[None, None], raw_scores, MASKED), queries)


def fetch_experts(gate_weight, up_weight, down_weight):
    return (
        lax.all_gather(gate_weight, "dp", axis=1, tiled=True),
        lax.all_gather(up_weight, "dp", axis=1, tiled=True),
        lax.all_gather(down_weight, "dp", axis=2, tiled=True),
    )


def reduce_experts(grads):
    return (
        lax.psum_scatter(
            grads[0].astype(jnp.bfloat16), "dp", scatter_dimension=1, tiled=True
        ).astype(jnp.float32),
        lax.psum_scatter(
            grads[1].astype(jnp.bfloat16), "dp", scatter_dimension=1, tiled=True
        ).astype(jnp.float32),
        lax.psum_scatter(
            grads[2].astype(jnp.bfloat16), "dp", scatter_dimension=2, tiled=True
        ).astype(jnp.float32),
    )


def local(
    hidden_in,
    out_grad,
    segment_ids,
    expert_ids,
    fill_order,
    attention_gain,
    query_weight,
    key_weight,
    value_weight,
    output_weight,
    mixture_gain,
    router_weight,
    gate_weight,
    up_weight,
    down_weight,
):
    local_heads = query_weight.shape[1] // HD
    local_groups = key_weight.shape[1] // HD
    group_ratio = local_heads // local_groups
    block_count = TOK_GRP // QBLK
    local_experts = gate_weight.shape[0]
    gain_one, query_full, key_full, value_full, output_full, gain_two, router_full = (
        lax.all_gather(attention_gain, "dp", axis=0, tiled=True),
        lax.all_gather(query_weight, "dp", axis=0, tiled=True),
        lax.all_gather(key_weight, "dp", axis=0, tiled=True),
        lax.all_gather(value_weight, "dp", axis=0, tiled=True),
        lax.all_gather(output_weight, "dp", axis=1, tiled=True),
        lax.all_gather(mixture_gain, "dp", axis=0, tiled=True),
        lax.all_gather(router_weight, "dp", axis=0, tiled=True),
    )
    gain_one = gain_one.astype(jnp.float32)
    gain_two = gain_two.astype(jnp.float32)
    residual = hidden_in.astype(jnp.float32)
    normed_shard, unit_one, inverse_one = rms_forward(residual, gain_one)
    normed_full = lax.all_gather(normed_shard.astype(jnp.bfloat16), "tensor", axis=0, tiled=True)
    positions, segments = group_layout(segment_ids[0], PROMPT)
    cosine_table, sine_table = rope_tables(positions, HD)
    query_pre = jnp.dot(normed_full, query_full, preferred_element_type=jnp.float32).reshape(
        TOK_GRP, local_heads, HD
    )
    key_pre = jnp.dot(normed_full, key_full, preferred_element_type=jnp.float32).reshape(
        TOK_GRP, local_groups, HD
    )
    value_low = (
        jnp.dot(normed_full, value_full, preferred_element_type=jnp.float32)
        .astype(jnp.bfloat16)
        .reshape(TOK_GRP, local_groups, HD)
    )
    query_rot = rotate(query_pre, cosine_table, sine_table).astype(jnp.bfloat16)
    key_rot = rotate(key_pre, cosine_table, sine_table).astype(jnp.bfloat16)
    mixed_blocks = []
    logsum_blocks = []
    for block_index in range(block_count):
        row_start = block_index * QBLK
        key_end = row_start + QBLK
        scores, queries = block_scores(
            query_rot, key_rot, segments, row_start, key_end, local_groups, group_ratio
        )
        top_score = jnp.max(scores, axis=-1, keepdims=True)
        shifted_exp = jnp.exp(scores - top_score)
        total_exp = jnp.sum(shifted_exp, axis=-1, keepdims=True)
        soft_weights = (shifted_exp / total_exp).astype(jnp.bfloat16)
        logsum_blocks.append(top_score + jnp.log(total_exp))
        mixed = jnp.einsum(
            "grqk,kgd->qgrd", soft_weights, value_low[:key_end], preferred_element_type=jnp.float32
        )
        mixed_blocks.append(mixed.astype(jnp.bfloat16).reshape(QBLK, local_heads * HD))
    mixed_full = jnp.concatenate(mixed_blocks, axis=0)
    attended = lax.psum_scatter(
        jnp.dot(mixed_full, output_full, preferred_element_type=jnp.float32).astype(jnp.bfloat16),
        "tensor",
        scatter_dimension=0,
        tiled=True,
    ).astype(jnp.float32)
    middle = residual + RESIDUAL_SCALE * attended
    normed_two, unit_two, inverse_two = rms_forward(middle, gain_two)
    mixture_in = lax.all_gather(normed_two.astype(jnp.bfloat16), "tensor", axis=0, tiled=True)
    gate_full, up_full, down_full = fetch_experts(gate_weight, up_weight, down_weight)
    logits = jnp.dot(mixture_in, router_full, preferred_element_type=jnp.float32)
    routed_marks = (
        expert_ids[:, :, None] == jnp.arange(EXPERTS, dtype=jnp.int32)[None, None, :]
    ).astype(jnp.float32)
    routed = jnp.sum(routed_marks * logits[:, None, :], axis=-1)
    gates = jax.nn.softmax(routed, axis=-1)
    slot_count = local_experts * CAP
    first_slot = lax.axis_index("tensor") * slot_count
    slot_pair = route_slots(expert_ids, fill_order[0], first_slot, slot_count)
    slot_valid = slot_pair >= 0
    safe_pair = jnp.maximum(slot_pair, 0)
    slot_token = safe_pair // TOPK
    slot_gate = jnp.where(slot_valid, jnp.take(gates.reshape(-1), safe_pair), 0.0)
    slot_gate = slot_gate.reshape(local_experts, CAP, 1)

    inputs = gather_rows(slot_token, mixture_in.astype(jnp.float32), CAP, jnp.bfloat16).reshape(
        local_experts, CAP, D
    )
    gate_pre = jnp.einsum("ecd,edf->ecf", inputs, gate_full, preferred_element_type=jnp.float32)
    up_pre = jnp.einsum("ecd,edf->ecf", inputs, up_full, preferred_element_type=jnp.float32)
    activated = jax.nn.silu(gate_pre)
    hidden_units = (slot_gate * activated * up_pre).astype(jnp.bfloat16)
    expert_out = jnp.einsum(
        "ecf,efd->ecd", hidden_units, down_full, preferred_element_type=jnp.float32
    )
    mixture_sum = combine_rows(slot_token, expert_out.reshape(slot_count, D), CAP, TOK_GRP)
    mixture_part = lax.psum_scatter(
        mixture_sum.astype(jnp.bfloat16), "tensor", scatter_dimension=0, tiled=True
    ).astype(jnp.float32)
    block_output = (middle + RESIDUAL_SCALE * mixture_part).astype(jnp.bfloat16)
    cotangent_full = lax.all_gather(out_grad, "tensor", axis=0, tiled=True)
    scaled_cotangent = (
        (RESIDUAL_SCALE * cotangent_full.astype(jnp.float32)).astype(jnp.bfloat16).astype(jnp.float32)
    )
    out_rows = gather_rows(slot_token, scaled_cotangent, CAP, jnp.bfloat16).reshape(
        local_experts, CAP, D
    )
    hidden_grad = jnp.einsum("ecd,efd->ecf", out_rows, down_full, preferred_element_type=jnp.float32)
    gate_grad_slot = jnp.sum(activated * up_pre * hidden_grad, axis=-1).reshape(slot_count)
    gate_grad_pair = jnp.zeros((TOK_GRP * TOPK,), jnp.float32).at[safe_pair].add(
        jnp.where(slot_valid, gate_grad_slot, 0.0)
    )
    product_grad = slot_gate * hidden_grad
    gate_pre_grad = (product_grad * up_pre * silu_slope(gate_pre)).astype(jnp.bfloat16)
    up_pre_grad = (product_grad * activated).astype(jnp.bfloat16)
    input_rows = jnp.einsum(
        "ecf,edf->ecd", gate_pre_grad, gate_full, preferred_element_type=jnp.float32
    ) + jnp.einsum("ecf,edf->ecd", up_pre_grad, up_full, preferred_element_type=jnp.float32)
    input_rows = input_rows.astype(jnp.bfloat16).astype(jnp.float32).reshape(slot_count, D)
    grad_in_mixture = combine_rows(slot_token, input_rows, CAP, TOK_GRP)
    expert_parts = (
        jnp.einsum("ecd,ecf->edf", inputs, gate_pre_grad, preferred_element_type=jnp.float32),
        jnp.einsum("ecd,ecf->edf", inputs, up_pre_grad, preferred_element_type=jnp.float32),
        jnp.einsum("ecf,ecd->efd", hidden_units, out_rows, preferred_element_type=jnp.float32),
    )
    expert_parts = reduce_experts(expert_parts)
    gate_weight_grad, up_weight_grad, down_weight_grad = expert_parts
    gates_grad = gate_grad_pair.reshape(TOK_GRP, TOPK)
    routed_grad = gates * (gates_grad - jnp.sum(gates * gates_grad, axis=-1, keepdims=True))
    logits_grad = jnp.sum(routed_marks * routed_grad[:, :, None], axis=1)
    router_part = jnp.einsum(
        "td,te->de", mixture_in, logits_grad, precision=HIGHEST, preferred_element_type=jnp.float32
    )
    grad_in_mixture = grad_in_mixture + jnp.einsum(
        "te,de->td", logits_grad, router_full.astype(jnp.float32), precision=HIGHEST
    )
    mixture_grad_shard = lax.psum_scatter(
        grad_in_mixture.astype(jnp.bfloat16), "tensor", scatter_dimension=0, tiled=True
    ).astype(jnp.float32)
    middle_norm_grad, gain_two_grad = rms_backward(
        mixture_grad_shard, unit_two, inverse_two, gain_two
    )
    middle_grad = out_grad.astype(jnp.float32) + middle_norm_grad
    attended_grad = lax.all_gather(
        (RESIDUAL_SCALE * middle_grad).astype(jnp.bfloat16), "tensor", axis=0, tiled=True
    )
    output_part = jnp.einsum(
        "tf,td->fd", mixed_full, attended_grad, preferred_element_type=jnp.float32
    )
    mixed_grad = jnp.einsum(
        "td,fd->tf", attended_grad, output_full, preferred_element_type=jnp.float32
    ).astype(jnp.bfloat16)
    mixed_grad = mixed_grad.reshape(TOK_GRP, local_groups, group_ratio, HD)
    key_grad = jnp.zeros((TOK_GRP, local_groups, HD), jnp.float32)
    value_grad = jnp.zeros((TOK_GRP, local_groups, HD), jnp.float32)
    query_blocks = []
    for block_index in range(block_count):
        row_start = block_index * QBLK
        key_end = row_start + QBLK
        scores, queries = block_scores(
            query_rot, key_rot, segments, row_start, key_end, local_groups, group_ratio
        )
        soft_full = jnp.exp(scores - logsum_blocks[block_index])
        soft_low = soft_full.astype(jnp.bfloat16)
        out_block = mixed_grad[row_start:key_end]
        weight_grad = jnp.einsum(
            "qgrd,kgd->grqk", out_block, value_low[:key_end], preferred_element_type=jnp.float32
        )
        delta = jnp.sum(soft_full * weight_grad, axis=-1, keepdims=True)
        score_grad = (soft_full * (weight_grad - delta)).astype(jnp.bfloat16)
        query_blocks.append(
            jnp.einsum(
                "grqk,kgd->qgrd", score_grad, key_rot[:key_end], preferred_element_type=jnp.float32
            )
            * ATTN_SCALE
        )
        key_grad = key_grad.at[:key_end].add(
            jnp.einsum("grqk,qgrd->kgd", score_grad, queries, preferred_element_type=jnp.float32)
            * ATTN_SCALE
        )
        value_grad = value_grad.at[:key_end].add(
            jnp.einsum("grqk,qgrd->kgd", soft_low, out_block, preferred_element_type=jnp.float32)
        )
    query_rot_grad = jnp.concatenate(query_blocks, axis=0).reshape(TOK_GRP, local_heads, HD)
    query_grad = (
        rotate_back(query_rot_grad, cosine_table, sine_table)
        .astype(jnp.bfloat16)
        .reshape(TOK_GRP, local_heads * HD)
    )
    key_grad_low = (
        rotate_back(key_grad, cosine_table, sine_table)
        .astype(jnp.bfloat16)
        .reshape(TOK_GRP, local_groups * HD)
    )
    value_grad_low = value_grad.astype(jnp.bfloat16).reshape(TOK_GRP, local_groups * HD)
    query_part = jnp.einsum(
        "td,tf->df", normed_full, query_grad, preferred_element_type=jnp.float32
    )
    key_part = jnp.einsum(
        "td,tf->df", normed_full, key_grad_low, preferred_element_type=jnp.float32
    )
    value_part = jnp.einsum(
        "td,tf->df", normed_full, value_grad_low, preferred_element_type=jnp.float32
    )
    total_rows = jnp.einsum("tf,df->td", query_grad, query_full, preferred_element_type=jnp.float32)
    total_rows = total_rows + jnp.einsum(
        "tf,df->td", key_grad_low, key_full, preferred_element_type=jnp.float32
    )
    normed_grad = lax.psum_scatter(
        (
            total_rows
            + jnp.einsum(
                "tf,df->td", value_grad_low, value_full, preferred_element_type=jnp.float32
            )
        ).astype(jnp.bfloat16),
        "tensor",
        scatter_dimension=0,
        tiled=True,
    ).astype(jnp.float32)
    input_norm_grad, gain_one_grad = rms_backward(normed_grad, unit_one, inverse_one, gain_one)
    input_grad = middle_grad + input_norm_grad
    query_weight_grad, key_weight_grad, value_weight_grad, output_weight_grad = (
        lax.psum_scatter(
            query_part.astype(jnp.bfloat16), "dp", scatter_dimension=0, tiled=True
        ).astype(jnp.float32),
        lax.psum_scatter(
            key_part.astype(jnp.bfloat16), "dp", scatter_dimension=0, tiled=True
        ).astype(jnp.float32),
        lax.psum_scatter(
            value_part.astype(jnp.bfloat16), "dp", scatter_dimension=0, tiled=True
        ).astype(jnp.float32),
        lax.psum_scatter(
            output_part.astype(jnp.bfloat16), "dp", scatter_dimension=1, tiled=True
        ).astype(jnp.float32),
    )
    attention_gain_grad, mixture_gain_grad, router_weight_grad = (
        lax.psum_scatter(gain_one_grad, ("dp", "tensor"), scatter_dimension=0, tiled=True),
        lax.psum_scatter(gain_two_grad, ("dp", "tensor"), scatter_dimension=0, tiled=True),
        lax.psum_scatter(router_part, ("dp", "tensor"), scatter_dimension=0, tiled=True),
    )
    return (
        block_output,
        input_grad,
        attention_gain_grad,
        query_weight_grad,
        key_weight_grad,
        value_weight_grad,
        output_weight_grad,
        mixture_gain_grad,
        router_weight_grad,
        gate_weight_grad,
        up_weight_grad,
        down_weight_grad,
    )


def solution(mesh):
    in_specs = (
        P(("dp", "tensor"), None),
        P(("dp", "tensor"), None),
        P("dp", None),
        P("dp", None),
        P("dp", None),
        P("dp"),
        P("dp", "tensor"),
        P("dp", "tensor"),
        P("dp", "tensor"),
        P("tensor", "dp"),
        P("dp"),
        P("dp", None),
        P("tensor", "dp", None),
        P("tensor", "dp", None),
        P("tensor", None, "dp"),
    )
    out_specs = (
        P(("dp", "tensor"), None),
        P(("dp", "tensor"), None),
        P(("dp", "tensor")),
        P("dp", "tensor"),
        P("dp", "tensor"),
        P("dp", "tensor"),
        P("tensor", "dp"),
        P(("dp", "tensor")),
        P(("dp", "tensor"), None),
        P("tensor", "dp", None),
        P("tensor", "dp", None),
        P("tensor", None, "dp"),
    )
    return jax.shard_map(local, mesh=mesh, in_specs=in_specs, out_specs=out_specs, check_vma=False)
```

```python
import jax
import jax.numpy as jnp
from jax import lax
from jax.experimental import pallas as pl
from jax.experimental.pallas import tpu as pltpu
from jax.sharding import PartitionSpec as P

D = 1536
HD = 64
EXPERTS = 40
TOPK = 8
PROMPT = 2048
NCONT = 4
QBLK = 512
TOK_GRP = 3072
CAP = 768


ATTN_SCALE = 0.015625
RESIDUAL_SCALE = 0.22
NORM_EPS = 1e-06
ROPE_BASE = 10000.0
MASKED = -1e30
HIGHEST = lax.Precision.HIGHEST


def rms_forward(values, gain_row):
    inverse_rms = lax.rsqrt(jnp.mean(values * values, axis=-1, keepdims=True) + NORM_EPS)
    unit_rows = values * inverse_rms
    return (unit_rows * gain_row, unit_rows, inverse_rms)


def rms_backward(gradient, unit_rows, inverse_rms, gain_row):
    gain_grad = jnp.sum(gradient * unit_rows, axis=0)
    scaled = gradient * gain_row
    mean_term = jnp.mean(scaled * unit_rows, axis=-1, keepdims=True)
    return (inverse_rms * (scaled - unit_rows * mean_term), gain_grad)


def group_layout(segment_row, prompt_length):
    cont_length = segment_row.shape[0]
    segment_marks = (segment_row[:, None] == jnp.arange(NCONT, dtype=jnp.int32)[None, :]).astype(
        jnp.int32
    )
    segment_sizes = jnp.sum(segment_marks, axis=0)
    segment_starts = jnp.cumsum(segment_sizes) - segment_sizes
    token_starts = jnp.sum(segment_marks * segment_starts[None, :], axis=1)
    inside = jnp.arange(cont_length, dtype=jnp.int32) - token_starts
    positions = jnp.concatenate(
        [jnp.arange(prompt_length, dtype=jnp.int32), prompt_length + inside]
    )
    segments = jnp.concatenate([jnp.zeros((prompt_length,), jnp.int32), segment_row + 1])
    return (positions, segments)


def allowed(query_index, query_segment, key_index, key_segment):
    causal = key_index[None, :] <= query_index[:, None]
    shared = (key_segment[None, :] == 0) | (key_segment[None, :] == query_segment[:, None])
    return causal & shared


def rope_tables(positions, head_size):
    halfway = head_size // 2
    frequency = ROPE_BASE ** (-(2.0 * jnp.arange(halfway, dtype=jnp.float32)) / head_size)
    angles = positions.astype(jnp.float32)[:, None] * frequency[None, :]
    return (jnp.cos(angles), jnp.sin(angles))


def rotate(values, cosine_table, sine_table):
    halfway = values.shape[-1] // 2
    first_half = values[..., :halfway]
    second_half = values[..., halfway:]
    cosine_part = cosine_table[:, None, :]
    sine_part = sine_table[:, None, :]
    return jnp.concatenate(
        [
            first_half * cosine_part - second_half * sine_part,
            second_half * cosine_part + first_half * sine_part,
        ],
        axis=-1,
    )


def rotate_back(gradient, cosine_table, sine_table):
    halfway = gradient.shape[-1] // 2
    first_half = gradient[..., :halfway]
    second_half = gradient[..., halfway:]
    cosine_part = cosine_table[:, None, :]
    sine_part = sine_table[:, None, :]
    return jnp.concatenate(
        [
            first_half * cosine_part + second_half * sine_part,
            second_half * cosine_part - first_half * sine_part,
        ],
        axis=-1,
    )


def silu_slope(values):
    sigmoid_part = jax.nn.sigmoid(values)
    return sigmoid_part * (1.0 + values * (1.0 - sigmoid_part))


def route_slots(expert_row, order_row, first_slot, slot_count):
    pair_count = expert_row.shape[0] * expert_row.shape[1]
    ordered = table_lookup(expert_row.reshape(pair_count), order_row)
    onehot = ordered[:, None] == jnp.arange(EXPERTS, dtype=jnp.int32)[None, :]
    rank_block = 256
    blocks = pair_count // rank_block
    pair_marks = onehot.astype(jnp.bfloat16).reshape(blocks, rank_block, EXPERTS)
    lower_ones = (jnp.arange(rank_block)[:, None] >= jnp.arange(rank_block)[None, :]).astype(
        jnp.bfloat16
    )
    within = jnp.einsum(
        "ij,bje->bie", lower_ones, pair_marks, preferred_element_type=jnp.float32
    ).astype(jnp.int32)
    totals = within[:, -1, :]
    before = jnp.cumsum(totals, axis=0) - totals
    counts = (within + before[:, None, :]).reshape(pair_count, EXPERTS)
    pair_rank = jnp.sum(jnp.where(onehot, counts, 0), axis=1) - 1
    local_slot = ordered * CAP + pair_rank - first_slot
    kept = (pair_rank < CAP) & (local_slot >= 0) & (local_slot < slot_count)
    local_slot = jnp.where(kept, local_slot, -1)
    return invert_slots(local_slot, order_row, slot_count)


def _gather_rows_kernel(tok_ref, src_ref, out_ref, buf, sem):
    rows = buf.shape[0]
    base = pl.program_id(0) * rows

    def start(s, carry):
        t = tok_ref[base + s]
        pltpu.make_async_copy(src_ref.at[pl.ds(t, 1)], buf.at[pl.ds(s, 1)], sem).start()
        return carry

    lax.fori_loop(0, rows, start, 0, unroll=8)
    pltpu.make_async_copy(src_ref.at[pl.ds(0, rows)], buf, sem).wait()
    out_ref[...] = buf[...].astype(out_ref.dtype)


def gather_rows(tok, src, rows, out_dtype):
    blocks, width = tok.shape[0] // rows, src.shape[1]
    return pl.pallas_call(
        _gather_rows_kernel,
        grid_spec=pltpu.PrefetchScalarGridSpec(
            num_scalar_prefetch=1,
            grid=(blocks,),
            in_specs=[pl.BlockSpec(memory_space=pl.ANY)],
            out_specs=pl.BlockSpec((rows, width), lambda b, tok: (b, 0)),
            scratch_shapes=[pltpu.VMEM((rows, width), jnp.float32), pltpu.SemaphoreType.DMA(())],
        ),
        out_shape=jax.ShapeDtypeStruct((tok.shape[0], width), out_dtype),
    )(tok, src)


def _combine_rows_kernel(tok_ref, add_ref, out_ref, acc_ref, sem):
    rows = add_ref.shape[0]
    step = pl.program_id(0)

    @pl.when(step == 0)
    def _():
        acc_ref[...] = jnp.zeros_like(acc_ref)

    base = step * rows

    def body(s, carry):
        t = tok_ref[base + s]
        acc_ref[pl.ds(t, 1), :] += add_ref[pl.ds(s, 1), :]
        return carry

    lax.fori_loop(0, rows, body, 0, unroll=8)

    @pl.when(step == pl.num_programs(0) - 1)
    def _():
        copy = pltpu.make_async_copy(acc_ref, out_ref, sem)
        copy.start()
        copy.wait()


def combine_rows(tok, addend, rows, total_rows):
    blocks, width = tok.shape[0] // rows, addend.shape[1]
    return pl.pallas_call(
        _combine_rows_kernel,
        grid_spec=pltpu.PrefetchScalarGridSpec(
            num_scalar_prefetch=1,
            grid=(blocks,),
            in_specs=[pl.BlockSpec((rows, width), lambda b, tok: (b, 0))],
            out_specs=pl.BlockSpec(memory_space=pl.ANY),
            scratch_shapes=[
                pltpu.VMEM((total_rows, width), jnp.float32),
                pltpu.SemaphoreType.DMA(()),
            ],
        ),
        out_shape=jax.ShapeDtypeStruct((total_rows, width), jnp.float32),
        compiler_params=pltpu.CompilerParams(vmem_limit_bytes=48 * 1024 * 1024),
    )(tok, addend)


def table_lookup(table, index):
    lanes = 128
    high_count = table.shape[0] // lanes
    low_marks = (index[:, None] % lanes == jnp.arange(lanes)[None, :]).astype(jnp.bfloat16)
    picked = jnp.dot(
        low_marks,
        table.reshape(high_count, lanes).astype(jnp.bfloat16).T,
        preferred_element_type=jnp.float32,
    )
    high_marks = index[:, None] // lanes == jnp.arange(high_count)[None, :]
    return jnp.sum(jnp.where(high_marks, picked, 0.0), axis=1).astype(jnp.int32)


def invert_slots(local_slot, values, slot_count):
    lanes = 128
    high_count = slot_count // lanes
    column_marks = (local_slot[:, None] // lanes == jnp.arange(high_count)[None, :]).astype(
        jnp.bfloat16
    )
    lane_marks = local_slot[:, None] % lanes == jnp.arange(lanes)[None, :]
    shifted = values + 1
    parts = []
    for digit in (shifted // 256, shifted % 256):
        spread = jnp.where(lane_marks, digit[:, None], 0).astype(jnp.bfloat16)
        parts.append(
            jnp.einsum("ic,il->cl", column_marks, spread, preferred_element_type=jnp.float32)
        )
    return (256.0 * parts[0] + parts[1]).astype(jnp.int32).reshape(slot_count) - 1


def block_scores(query_rot, key_rot, segments, row_start, key_end, local_groups, group_ratio):
    queries = query_rot[row_start:key_end].reshape(
        key_end - row_start, local_groups, group_ratio, HD
    )
    raw_scores = (
        jnp.einsum("qgrd,kgd->grqk", queries, key_rot[:key_end], preferred_element_type=jnp.float32)
        * ATTN_SCALE
    )
    visible = allowed(
        jnp.arange(row_start, key_end, dtype=jnp.int32),
        segments[row_start:key_end],
        jnp.arange(key_end, dtype=jnp.int32),
        segments[:key_end],
    )
    return (jnp.where(visible[None, None], raw_scores, MASKED), queries)


def fetch_experts(gate_weight, up_weight, down_weight):
    return (
        lax.all_gather(gate_weight, "dp", axis=1, tiled=True),
        lax.all_gather(up_weight, "dp", axis=1, tiled=True),
        lax.all_gather(down_weight, "dp", axis=2, tiled=True),
    )


def reduce_experts(grads):
    return (
        lax.psum_scatter(grads[0], "dp", scatter_dimension=1, tiled=True).astype(jnp.float32),
        lax.psum_scatter(grads[1], "dp", scatter_dimension=1, tiled=True).astype(jnp.float32),
        lax.psum_scatter(grads[2], "dp", scatter_dimension=2, tiled=True).astype(jnp.float32),
    )


def local(
    hidden_in,
    out_grad,
    segment_ids,
    expert_ids,
    fill_order,
    attention_gain,
    query_weight,
    key_weight,
    value_weight,
    output_weight,
    mixture_gain,
    router_weight,
    gate_weight,
    up_weight,
    down_weight,
):
    local_heads = query_weight.shape[1] // HD
    local_groups = key_weight.shape[1] // HD
    group_ratio = local_heads // local_groups
    block_count = TOK_GRP // QBLK
    local_experts = gate_weight.shape[0]
    gain_one, query_full, key_full, value_full, output_full, gain_two, router_full = (
        lax.all_gather(attention_gain, "dp", axis=0, tiled=True),
        lax.all_gather(query_weight, "dp", axis=0, tiled=True),
        lax.all_gather(key_weight, "dp", axis=0, tiled=True),
        lax.all_gather(value_weight, "dp", axis=0, tiled=True),
        lax.all_gather(output_weight, "dp", axis=1, tiled=True),
        lax.all_gather(mixture_gain, "dp", axis=0, tiled=True),
        lax.all_gather(router_weight, "dp", axis=0, tiled=True),
    )
    gain_one = gain_one.astype(jnp.float32)
    gain_two = gain_two.astype(jnp.float32)
    residual = hidden_in.astype(jnp.float32)
    normed_shard, unit_one, inverse_one = rms_forward(residual, gain_one)
    normed_full = lax.all_gather(normed_shard.astype(jnp.bfloat16), "tensor", axis=0, tiled=True)
    gate_weight, up_weight, normed_full = lax.optimization_barrier(
        (gate_weight, up_weight, normed_full)
    )
    gate_full = lax.all_gather(gate_weight, "dp", axis=1, tiled=True)
    up_full = lax.all_gather(up_weight, "dp", axis=1, tiled=True)
    positions, segments = group_layout(segment_ids[0], PROMPT)
    cosine_table, sine_table = rope_tables(positions, HD)
    query_pre = jnp.dot(normed_full, query_full, preferred_element_type=jnp.float32).reshape(
        TOK_GRP, local_heads, HD
    )
    key_pre = jnp.dot(normed_full, key_full, preferred_element_type=jnp.float32).reshape(
        TOK_GRP, local_groups, HD
    )
    value_low = (
        jnp.dot(normed_full, value_full, preferred_element_type=jnp.float32)
        .astype(jnp.bfloat16)
        .reshape(TOK_GRP, local_groups, HD)
    )
    query_rot = rotate(query_pre, cosine_table, sine_table).astype(jnp.bfloat16)
    key_rot = rotate(key_pre, cosine_table, sine_table).astype(jnp.bfloat16)
    mixed_blocks = []
    logsum_blocks = []
    for block_index in range(block_count):
        row_start = block_index * QBLK
        key_end = row_start + QBLK
        scores, queries = block_scores(
            query_rot, key_rot, segments, row_start, key_end, local_groups, group_ratio
        )
        top_score = jnp.max(scores, axis=-1, keepdims=True)
        shifted_exp = jnp.exp(scores - top_score)
        total_exp = jnp.sum(shifted_exp, axis=-1, keepdims=True)
        soft_weights = (shifted_exp / total_exp).astype(jnp.bfloat16)
        logsum_blocks.append(top_score + jnp.log(total_exp))
        mixed = jnp.einsum(
            "grqk,kgd->qgrd", soft_weights, value_low[:key_end], preferred_element_type=jnp.float32
        )
        mixed_blocks.append(mixed.astype(jnp.bfloat16).reshape(QBLK, local_heads * HD))
    mixed_full = jnp.concatenate(mixed_blocks, axis=0)
    attended_partial = jnp.dot(
        mixed_full, output_full, preferred_element_type=jnp.float32
    ).astype(jnp.bfloat16)
    attended_partial, gate_full, up_full = lax.optimization_barrier(
        (attended_partial, gate_full, up_full)
    )
    attended = lax.psum_scatter(
        attended_partial,
        "tensor",
        scatter_dimension=0,
        tiled=True,
    ).astype(jnp.float32)
    middle = residual + RESIDUAL_SCALE * attended
    normed_two, unit_two, inverse_two = rms_forward(middle, gain_two)
    mixture_in = lax.all_gather(normed_two.astype(jnp.bfloat16), "tensor", axis=0, tiled=True)
    down_weight, mixture_in = lax.optimization_barrier((down_weight, mixture_in))
    down_full = lax.all_gather(down_weight, "dp", axis=2, tiled=True)
    logits = jnp.dot(mixture_in, router_full, preferred_element_type=jnp.float32)
    routed_marks = (
        expert_ids[:, :, None] == jnp.arange(EXPERTS, dtype=jnp.int32)[None, None, :]
    ).astype(jnp.float32)
    routed = jnp.sum(routed_marks * logits[:, None, :], axis=-1)
    gates = jax.nn.softmax(routed, axis=-1)
    slot_count = local_experts * CAP
    first_slot = lax.axis_index("tensor") * slot_count
    slot_pair = route_slots(expert_ids, fill_order[0], first_slot, slot_count)
    slot_valid = slot_pair >= 0
    safe_pair = jnp.maximum(slot_pair, 0)
    slot_token = safe_pair // TOPK
    slot_gate = jnp.where(slot_valid, jnp.take(gates.reshape(-1), safe_pair), 0.0)
    slot_gate = slot_gate.reshape(local_experts, CAP, 1)

    inputs = gather_rows(slot_token, mixture_in.astype(jnp.float32), CAP, jnp.bfloat16).reshape(
        local_experts, CAP, D
    )
    gate_pre = jnp.einsum("ecd,edf->ecf", inputs, gate_full, preferred_element_type=jnp.float32)
    up_pre = jnp.einsum("ecd,edf->ecf", inputs, up_full, preferred_element_type=jnp.float32)
    activated = jax.nn.silu(gate_pre)
    hidden_units = (slot_gate * activated * up_pre).astype(jnp.bfloat16)
    expert_out = jnp.einsum(
        "ecf,efd->ecd", hidden_units, down_full, preferred_element_type=jnp.float32
    )
    mixture_sum = combine_rows(slot_token, expert_out.reshape(slot_count, D), CAP, TOK_GRP)
    out_grad_held, down_full = lax.optimization_barrier((out_grad, down_full))
    cotangent_full = lax.all_gather(out_grad_held, "tensor", axis=0, tiled=True)
    scaled_cotangent = (
        (RESIDUAL_SCALE * cotangent_full.astype(jnp.float32)).astype(jnp.bfloat16).astype(jnp.float32)
    )
    scaled_cotangent, mixture_sum = lax.optimization_barrier((scaled_cotangent, mixture_sum))
    mixture_part = lax.psum_scatter(
        mixture_sum.astype(jnp.bfloat16), "tensor", scatter_dimension=0, tiled=True
    ).astype(jnp.float32)
    out_rows = gather_rows(slot_token, scaled_cotangent, CAP, jnp.bfloat16).reshape(
        local_experts, CAP, D
    )
    hidden_grad = jnp.einsum("ecd,efd->ecf", out_rows, down_full, preferred_element_type=jnp.float32)
    gate_grad_slot = jnp.sum(activated * up_pre * hidden_grad, axis=-1).reshape(slot_count)
    gate_grad_pair = jnp.zeros((TOK_GRP * TOPK,), jnp.float32).at[safe_pair].add(
        jnp.where(slot_valid, gate_grad_slot, 0.0)
    )
    product_grad = slot_gate * hidden_grad
    gate_pre_grad = (product_grad * up_pre * silu_slope(gate_pre)).astype(jnp.bfloat16)
    up_pre_grad = (product_grad * activated).astype(jnp.bfloat16)
    input_rows = jnp.einsum(
        "ecf,edf->ecd", gate_pre_grad, gate_full, preferred_element_type=jnp.float32
    ) + jnp.einsum("ecf,edf->ecd", up_pre_grad, up_full, preferred_element_type=jnp.float32)
    input_rows = input_rows.astype(jnp.bfloat16).astype(jnp.float32).reshape(slot_count, D)
    grad_in_mixture = combine_rows(slot_token, input_rows, CAP, TOK_GRP)
    (inputs, gate_pre_grad, up_pre_grad, hidden_units, out_rows), grad_in_mixture = (
        lax.optimization_barrier(
            ((inputs, gate_pre_grad, up_pre_grad, hidden_units, out_rows), grad_in_mixture)
        )
    )
    expert_parts = (
        jnp.einsum("ecd,ecf->edf", inputs, gate_pre_grad, preferred_element_type=jnp.float32),
        jnp.einsum("ecd,ecf->edf", inputs, up_pre_grad, preferred_element_type=jnp.float32),
        jnp.einsum("ecf,ecd->efd", hidden_units, out_rows, preferred_element_type=jnp.float32),
    )
    expert_parts = tuple(part.astype(jnp.bfloat16) for part in expert_parts)
    gates_grad = gate_grad_pair.reshape(TOK_GRP, TOPK)
    routed_grad = gates * (gates_grad - jnp.sum(gates * gates_grad, axis=-1, keepdims=True))
    logits_grad = jnp.sum(routed_marks * routed_grad[:, :, None], axis=1)
    router_part = jnp.einsum(
        "td,te->de", mixture_in, logits_grad, precision=HIGHEST, preferred_element_type=jnp.float32
    )
    grad_in_mixture = grad_in_mixture + jnp.einsum(
        "te,de->td", logits_grad, router_full.astype(jnp.float32), precision=HIGHEST
    )
    mixture_grad_low, mixture_part = lax.optimization_barrier(
        (grad_in_mixture.astype(jnp.bfloat16), mixture_part)
    )
    block_output = (middle + RESIDUAL_SCALE * mixture_part).astype(jnp.bfloat16)
    mixture_grad_shard = lax.psum_scatter(
        mixture_grad_low, "tensor", scatter_dimension=0, tiled=True
    ).astype(jnp.float32)
    middle_norm_grad, gain_two_grad = rms_backward(
        mixture_grad_shard, unit_two, inverse_two, gain_two
    )
    middle_grad = out_grad.astype(jnp.float32) + middle_norm_grad
    attended_grad = lax.all_gather(
        (RESIDUAL_SCALE * middle_grad).astype(jnp.bfloat16), "tensor", axis=0, tiled=True
    )
    expert_parts, router_part, attended_grad = lax.optimization_barrier(
        (expert_parts, router_part, attended_grad)
    )
    expert_grads = reduce_experts(expert_parts)
    router_weight_grad = lax.psum_scatter(
        router_part, ("dp", "tensor"), scatter_dimension=0, tiled=True
    )
    output_part = jnp.einsum(
        "tf,td->fd", mixed_full, attended_grad, preferred_element_type=jnp.float32
    )
    mixed_grad = jnp.einsum(
        "td,fd->tf", attended_grad, output_full, preferred_element_type=jnp.float32
    ).astype(jnp.bfloat16)
    mixed_grad = mixed_grad.reshape(TOK_GRP, local_groups, group_ratio, HD)
    key_grad = jnp.zeros((TOK_GRP, local_groups, HD), jnp.float32)
    value_grad = jnp.zeros((TOK_GRP, local_groups, HD), jnp.float32)
    query_blocks = []
    for block_index in range(block_count):
        row_start = block_index * QBLK
        key_end = row_start + QBLK
        scores, queries = block_scores(
            query_rot, key_rot, segments, row_start, key_end, local_groups, group_ratio
        )
        soft_full = jnp.exp(scores - logsum_blocks[block_index])
        soft_low = soft_full.astype(jnp.bfloat16)
        out_block = mixed_grad[row_start:key_end]
        weight_grad = jnp.einsum(
            "qgrd,kgd->grqk", out_block, value_low[:key_end], preferred_element_type=jnp.float32
        )
        delta = jnp.sum(soft_full * weight_grad, axis=-1, keepdims=True)
        score_grad = (soft_full * (weight_grad - delta)).astype(jnp.bfloat16)
        query_blocks.append(
            jnp.einsum(
                "grqk,kgd->qgrd", score_grad, key_rot[:key_end], preferred_element_type=jnp.float32
            )
            * ATTN_SCALE
        )
        key_grad = key_grad.at[:key_end].add(
            jnp.einsum("grqk,qgrd->kgd", score_grad, queries, preferred_element_type=jnp.float32)
            * ATTN_SCALE
        )
        value_grad = value_grad.at[:key_end].add(
            jnp.einsum("grqk,qgrd->kgd", soft_low, out_block, preferred_element_type=jnp.float32)
        )
        if block_index == block_count - 2:
            key_grad, value_grad, expert_grads, router_weight_grad = lax.optimization_barrier(
                (key_grad, value_grad, expert_grads, router_weight_grad)
            )
    gate_weight_grad, up_weight_grad, down_weight_grad = expert_grads
    query_rot_grad = jnp.concatenate(query_blocks, axis=0).reshape(TOK_GRP, local_heads, HD)
    query_grad = (
        rotate_back(query_rot_grad, cosine_table, sine_table)
        .astype(jnp.bfloat16)
        .reshape(TOK_GRP, local_heads * HD)
    )
    key_grad_low = (
        rotate_back(key_grad, cosine_table, sine_table)
        .astype(jnp.bfloat16)
        .reshape(TOK_GRP, local_groups * HD)
    )
    value_grad_low = value_grad.astype(jnp.bfloat16).reshape(TOK_GRP, local_groups * HD)
    total_rows = jnp.einsum("tf,df->td", query_grad, query_full, preferred_element_type=jnp.float32)
    total_rows = total_rows + jnp.einsum(
        "tf,df->td", key_grad_low, key_full, preferred_element_type=jnp.float32
    )
    normed_grad_low = (
        total_rows
        + jnp.einsum("tf,df->td", value_grad_low, value_full, preferred_element_type=jnp.float32)
    ).astype(jnp.bfloat16)
    normed_grad_low, query_grad, key_grad_low, value_grad_low = lax.optimization_barrier(
        (normed_grad_low, query_grad, key_grad_low, value_grad_low)
    )
    normed_grad = lax.psum_scatter(
        normed_grad_low, "tensor", scatter_dimension=0, tiled=True
    ).astype(jnp.float32)
    query_part = jnp.einsum(
        "td,tf->df", normed_full, query_grad, preferred_element_type=jnp.float32
    )
    key_part = jnp.einsum(
        "td,tf->df", normed_full, key_grad_low, preferred_element_type=jnp.float32
    )
    value_part = jnp.einsum(
        "td,tf->df", normed_full, value_grad_low, preferred_element_type=jnp.float32
    )
    projection_parts = jnp.concatenate(
        [query_part, key_part, value_part], axis=1
    ).astype(jnp.bfloat16)
    projection_parts, normed_grad = lax.optimization_barrier((projection_parts, normed_grad))
    input_norm_grad, gain_one_grad = rms_backward(normed_grad, unit_one, inverse_one, gain_one)
    input_grad = middle_grad + input_norm_grad
    projection_grads = lax.psum_scatter(
        projection_parts, "dp", scatter_dimension=0, tiled=True
    ).astype(jnp.float32)
    query_width, key_width = query_part.shape[1], key_part.shape[1]
    query_weight_grad = projection_grads[:, :query_width]
    key_weight_grad = projection_grads[:, query_width : query_width + key_width]
    value_weight_grad = projection_grads[:, query_width + key_width :]
    output_weight_grad = lax.psum_scatter(
        output_part.astype(jnp.bfloat16), "dp", scatter_dimension=1, tiled=True
    ).astype(jnp.float32)
    attention_gain_grad, mixture_gain_grad = (
        lax.psum_scatter(gain_one_grad, ("dp", "tensor"), scatter_dimension=0, tiled=True),
        lax.psum_scatter(gain_two_grad, ("dp", "tensor"), scatter_dimension=0, tiled=True),
    )
    return (
        block_output,
        input_grad,
        attention_gain_grad,
        query_weight_grad,
        key_weight_grad,
        value_weight_grad,
        output_weight_grad,
        mixture_gain_grad,
        router_weight_grad,
        gate_weight_grad,
        up_weight_grad,
        down_weight_grad,
    )


def solution(mesh):
    in_specs = (
        P(("dp", "tensor"), None),
        P(("dp", "tensor"), None),
        P("dp", None),
        P("dp", None),
        P("dp", None),
        P("dp"),
        P("dp", "tensor"),
        P("dp", "tensor"),
        P("dp", "tensor"),
        P("tensor", "dp"),
        P("dp"),
        P("dp", None),
        P("tensor", "dp", None),
        P("tensor", "dp", None),
        P("tensor", None, "dp"),
    )
    out_specs = (
        P(("dp", "tensor"), None),
        P(("dp", "tensor"), None),
        P(("dp", "tensor")),
        P("dp", "tensor"),
        P("dp", "tensor"),
        P("dp", "tensor"),
        P("tensor", "dp"),
        P(("dp", "tensor")),
        P(("dp", "tensor"), None),
        P("tensor", "dp", None),
        P("tensor", "dp", None),
        P("tensor", None, "dp"),
    )
    return jax.shard_map(local, mesh=mesh, in_specs=in_specs, out_specs=out_specs, check_vma=False)
```

```python
import jax
import jax.numpy as jnp
from jax import lax
from jax.experimental import pallas as pl
from jax.experimental.pallas import tpu as pltpu
from jax.sharding import PartitionSpec as P

D = 1536
HD = 64
EXPERTS = 40
TOPK = 8
PROMPT = 2048
NCONT = 4
QBLK = 512
TOK_GRP = 3072
CAP = 768


ATTN_SCALE = 0.015625
RESIDUAL_SCALE = 0.22
NORM_EPS = 1e-06
ROPE_BASE = 10000.0
MASKED = -1e30
HIGHEST = lax.Precision.HIGHEST


def rms_forward(values, gain_row):
    inverse_rms = lax.rsqrt(jnp.mean(values * values, axis=-1, keepdims=True) + NORM_EPS)
    unit_rows = values * inverse_rms
    return (unit_rows * gain_row, unit_rows, inverse_rms)


def rms_backward(gradient, unit_rows, inverse_rms, gain_row):
    gain_grad = jnp.sum(gradient * unit_rows, axis=0)
    scaled = gradient * gain_row
    mean_term = jnp.mean(scaled * unit_rows, axis=-1, keepdims=True)
    return (inverse_rms * (scaled - unit_rows * mean_term), gain_grad)


def group_layout(segment_row, prompt_length):
    cont_length = segment_row.shape[0]
    segment_marks = (segment_row[:, None] == jnp.arange(NCONT, dtype=jnp.int32)[None, :]).astype(
        jnp.int32
    )
    segment_sizes = jnp.sum(segment_marks, axis=0)
    segment_starts = jnp.cumsum(segment_sizes) - segment_sizes
    token_starts = jnp.sum(segment_marks * segment_starts[None, :], axis=1)
    inside = jnp.arange(cont_length, dtype=jnp.int32) - token_starts
    positions = jnp.concatenate(
        [jnp.arange(prompt_length, dtype=jnp.int32), prompt_length + inside]
    )
    segments = jnp.concatenate([jnp.zeros((prompt_length,), jnp.int32), segment_row + 1])
    return (positions, segments)


def allowed(query_index, query_segment, key_index, key_segment):
    causal = key_index[None, :] <= query_index[:, None]
    shared = (key_segment[None, :] == 0) | (key_segment[None, :] == query_segment[:, None])
    return causal & shared


def rope_tables(positions, head_size):
    halfway = head_size // 2
    frequency = ROPE_BASE ** (-(2.0 * jnp.arange(halfway, dtype=jnp.float32)) / head_size)
    angles = positions.astype(jnp.float32)[:, None] * frequency[None, :]
    return (jnp.cos(angles), jnp.sin(angles))


def rotate(values, cosine_table, sine_table):
    halfway = values.shape[-1] // 2
    first_half = values[..., :halfway]
    second_half = values[..., halfway:]
    cosine_part = cosine_table[:, None, :]
    sine_part = sine_table[:, None, :]
    return jnp.concatenate(
        [
            first_half * cosine_part - second_half * sine_part,
            second_half * cosine_part + first_half * sine_part,
        ],
        axis=-1,
    )


def rotate_back(gradient, cosine_table, sine_table):
    halfway = gradient.shape[-1] // 2
    first_half = gradient[..., :halfway]
    second_half = gradient[..., halfway:]
    cosine_part = cosine_table[:, None, :]
    sine_part = sine_table[:, None, :]
    return jnp.concatenate(
        [
            first_half * cosine_part + second_half * sine_part,
            second_half * cosine_part - first_half * sine_part,
        ],
        axis=-1,
    )


def silu_slope(values):
    sigmoid_part = jax.nn.sigmoid(values)
    return sigmoid_part * (1.0 + values * (1.0 - sigmoid_part))


def route_slots(expert_row, order_row, first_slot, slot_count):
    pair_count = expert_row.shape[0] * expert_row.shape[1]
    ordered = table_lookup(expert_row.reshape(pair_count), order_row)
    onehot = ordered[:, None] == jnp.arange(EXPERTS, dtype=jnp.int32)[None, :]
    rank_block = 256
    blocks = pair_count // rank_block
    pair_marks = onehot.astype(jnp.bfloat16).reshape(blocks, rank_block, EXPERTS)
    lower_ones = (jnp.arange(rank_block)[:, None] >= jnp.arange(rank_block)[None, :]).astype(
        jnp.bfloat16
    )
    within = jnp.einsum(
        "ij,bje->bie", lower_ones, pair_marks, preferred_element_type=jnp.float32
    ).astype(jnp.int32)
    totals = within[:, -1, :]
    before = jnp.cumsum(totals, axis=0) - totals
    counts = (within + before[:, None, :]).reshape(pair_count, EXPERTS)
    pair_rank = jnp.sum(jnp.where(onehot, counts, 0), axis=1) - 1
    local_slot = ordered * CAP + pair_rank - first_slot
    kept = (pair_rank < CAP) & (local_slot >= 0) & (local_slot < slot_count)
    local_slot = jnp.where(kept, local_slot, -1)
    return invert_slots(local_slot, order_row, slot_count)


def _gather_rows_kernel(tok_ref, *refs):
    count = (len(refs) - 1) // 4
    sources, outs = refs[:count], refs[count : 2 * count]
    copies, rows_bufs, sem = refs[2 * count : 3 * count], refs[3 * count : 4 * count], refs[-1]
    rows = rows_bufs[0].shape[0]
    step = pl.program_id(0)

    @pl.when(step == 0)
    def _():
        for source, copy in zip(sources, copies):
            transfer = pltpu.make_async_copy(source, copy, sem)
            transfer.start()
            transfer.wait()

    base = step * rows

    def body(s, carry):
        t = tok_ref[base + s]
        for copy, rows_buf in zip(copies, rows_bufs):
            rows_buf[pl.ds(s, 1), :] = copy[pl.ds(t, 1), :]
        return carry

    lax.fori_loop(0, rows, body, 0, unroll=8)
    for out, rows_buf in zip(outs, rows_bufs):
        out[...] = rows_buf[...].astype(out.dtype)


def gather_rows(tok, sources, rows, out_dtypes):
    blocks = tok.shape[0] // rows
    return pl.pallas_call(
        _gather_rows_kernel,
        grid_spec=pltpu.PrefetchScalarGridSpec(
            num_scalar_prefetch=1,
            grid=(blocks,),
            in_specs=[pl.BlockSpec(memory_space=pl.ANY) for _ in sources],
            out_specs=[
                pl.BlockSpec((rows, source.shape[1]), lambda b, tok: (b, 0)) for source in sources
            ],
            scratch_shapes=[pltpu.VMEM(source.shape, jnp.float32) for source in sources]
            + [pltpu.VMEM((rows, source.shape[1]), jnp.float32) for source in sources]
            + [pltpu.SemaphoreType.DMA(())],
        ),
        out_shape=[
            jax.ShapeDtypeStruct((tok.shape[0], source.shape[1]), dtype)
            for source, dtype in zip(sources, out_dtypes)
        ],
        compiler_params=pltpu.CompilerParams(vmem_limit_bytes=56 * 1024 * 1024),
    )(tok, *sources)


def _combine_rows_kernel(tok_ref, *refs):
    count = (len(refs) - 1) // 4
    addends, outs = refs[:count], refs[count : 2 * count]
    totals, rows_bufs, sem = refs[2 * count : 3 * count], refs[3 * count : 4 * count], refs[-1]
    rows = rows_bufs[0].shape[0]
    step = pl.program_id(0)

    @pl.when(step == 0)
    def _():
        for total in totals:
            total[...] = jnp.zeros_like(total)

    for addend, rows_buf in zip(addends, rows_bufs):
        rows_buf[...] = addend[...].astype(jnp.float32)
    base = step * rows

    def body(s, carry):
        t = tok_ref[base + s]
        for total, rows_buf in zip(totals, rows_bufs):
            total[pl.ds(t, 1), :] += rows_buf[pl.ds(s, 1), :]
        return carry

    lax.fori_loop(0, rows, body, 0, unroll=8)

    @pl.when(step == pl.num_programs(0) - 1)
    def _():
        for total, out in zip(totals, outs):
            transfer = pltpu.make_async_copy(total, out, sem)
            transfer.start()
            transfer.wait()


def combine_rows(tok, addends, rows, total_rows):
    blocks = tok.shape[0] // rows
    return pl.pallas_call(
        _combine_rows_kernel,
        grid_spec=pltpu.PrefetchScalarGridSpec(
            num_scalar_prefetch=1,
            grid=(blocks,),
            in_specs=[
                pl.BlockSpec((rows, addend.shape[1]), lambda b, tok: (b, 0)) for addend in addends
            ],
            out_specs=[pl.BlockSpec(memory_space=pl.ANY) for _ in addends],
            scratch_shapes=[
                pltpu.VMEM((total_rows, addend.shape[1]), jnp.float32) for addend in addends
            ]
            + [pltpu.VMEM((rows, addend.shape[1]), jnp.float32) for addend in addends]
            + [pltpu.SemaphoreType.DMA(())],
        ),
        out_shape=[
            jax.ShapeDtypeStruct((total_rows, addend.shape[1]), jnp.float32) for addend in addends
        ],
        compiler_params=pltpu.CompilerParams(vmem_limit_bytes=56 * 1024 * 1024),
    )(tok, *addends)


def table_lookup(table, index):
    lanes = 128
    high_count = table.shape[0] // lanes
    low_marks = (index[:, None] % lanes == jnp.arange(lanes)[None, :]).astype(jnp.bfloat16)
    picked = jnp.dot(
        low_marks,
        table.reshape(high_count, lanes).astype(jnp.bfloat16).T,
        preferred_element_type=jnp.float32,
    )
    high_marks = index[:, None] // lanes == jnp.arange(high_count)[None, :]
    return jnp.sum(jnp.where(high_marks, picked, 0.0), axis=1).astype(jnp.int32)


def invert_slots(local_slot, values, slot_count):
    lanes = 128
    high_count = slot_count // lanes
    column_marks = (local_slot[:, None] // lanes == jnp.arange(high_count)[None, :]).astype(
        jnp.bfloat16
    )
    lane_marks = local_slot[:, None] % lanes == jnp.arange(lanes)[None, :]
    shifted = values + 1
    parts = []
    for digit in (shifted // 256, shifted % 256):
        spread = jnp.where(lane_marks, digit[:, None], 0).astype(jnp.bfloat16)
        parts.append(
            jnp.einsum("ic,il->cl", column_marks, spread, preferred_element_type=jnp.float32)
        )
    return (256.0 * parts[0] + parts[1]).astype(jnp.int32).reshape(slot_count) - 1


def block_scores(query_rot, key_rot, segments, row_start, key_end, local_groups, group_ratio):
    queries = query_rot[row_start:key_end].reshape(
        key_end - row_start, local_groups, group_ratio, HD
    )
    raw_scores = (
        jnp.einsum("qgrd,kgd->grqk", queries, key_rot[:key_end], preferred_element_type=jnp.float32)
        * ATTN_SCALE
    )
    visible = allowed(
        jnp.arange(row_start, key_end, dtype=jnp.int32),
        segments[row_start:key_end],
        jnp.arange(key_end, dtype=jnp.int32),
        segments[:key_end],
    )
    return (jnp.where(visible[None, None], raw_scores, MASKED), queries)


def fetch_experts(gate_weight, up_weight, down_weight):
    return (
        lax.all_gather(gate_weight, "dp", axis=1, tiled=True),
        lax.all_gather(up_weight, "dp", axis=1, tiled=True),
        lax.all_gather(down_weight, "dp", axis=2, tiled=True),
    )


def reduce_experts(grads):
    return (
        lax.psum_scatter(grads[0], "dp", scatter_dimension=1, tiled=True).astype(jnp.float32),
        lax.psum_scatter(grads[1], "dp", scatter_dimension=1, tiled=True).astype(jnp.float32),
        lax.psum_scatter(grads[2], "dp", scatter_dimension=2, tiled=True).astype(jnp.float32),
    )


def local(
    hidden_in,
    out_grad,
    segment_ids,
    expert_ids,
    fill_order,
    attention_gain,
    query_weight,
    key_weight,
    value_weight,
    output_weight,
    mixture_gain,
    router_weight,
    gate_weight,
    up_weight,
    down_weight,
):
    local_heads = query_weight.shape[1] // HD
    local_groups = key_weight.shape[1] // HD
    group_ratio = local_heads // local_groups
    block_count = TOK_GRP // QBLK
    local_experts = gate_weight.shape[0]
    gain_one, query_full, key_full, value_full, output_full, gain_two, router_full = (
        lax.all_gather(attention_gain, "dp", axis=0, tiled=True),
        lax.all_gather(query_weight, "dp", axis=0, tiled=True),
        lax.all_gather(key_weight, "dp", axis=0, tiled=True),
        lax.all_gather(value_weight, "dp", axis=0, tiled=True),
        lax.all_gather(output_weight, "dp", axis=1, tiled=True),
        lax.all_gather(mixture_gain, "dp", axis=0, tiled=True),
        lax.all_gather(router_weight, "dp", axis=0, tiled=True),
    )
    gain_one = gain_one.astype(jnp.float32)
    gain_two = gain_two.astype(jnp.float32)
    residual = hidden_in.astype(jnp.float32)
    normed_shard, unit_one, inverse_one = rms_forward(residual, gain_one)
    normed_full = lax.all_gather(normed_shard.astype(jnp.bfloat16), "tensor", axis=0, tiled=True)
    gate_weight, up_weight, normed_full = lax.optimization_barrier(
        (gate_weight, up_weight, normed_full)
    )
    gate_full = lax.all_gather(gate_weight, "dp", axis=1, tiled=True)
    up_full = lax.all_gather(up_weight, "dp", axis=1, tiled=True)
    positions, segments = group_layout(segment_ids[0], PROMPT)
    cosine_table, sine_table = rope_tables(positions, HD)
    query_pre = jnp.dot(normed_full, query_full, preferred_element_type=jnp.float32).reshape(
        TOK_GRP, local_heads, HD
    )
    key_pre = jnp.dot(normed_full, key_full, preferred_element_type=jnp.float32).reshape(
        TOK_GRP, local_groups, HD
    )
    value_low = (
        jnp.dot(normed_full, value_full, preferred_element_type=jnp.float32)
        .astype(jnp.bfloat16)
        .reshape(TOK_GRP, local_groups, HD)
    )
    query_rot = rotate(query_pre, cosine_table, sine_table).astype(jnp.bfloat16)
    key_rot = rotate(key_pre, cosine_table, sine_table).astype(jnp.bfloat16)
    mixed_blocks = []
    logsum_blocks = []
    for block_index in range(block_count):
        row_start = block_index * QBLK
        key_end = row_start + QBLK
        scores, queries = block_scores(
            query_rot, key_rot, segments, row_start, key_end, local_groups, group_ratio
        )
        top_score = jnp.max(scores, axis=-1, keepdims=True)
        shifted_exp = jnp.exp(scores - top_score)
        total_exp = jnp.sum(shifted_exp, axis=-1, keepdims=True)
        soft_weights = (shifted_exp / total_exp).astype(jnp.bfloat16)
        logsum_blocks.append(top_score + jnp.log(total_exp))
        mixed = jnp.einsum(
            "grqk,kgd->qgrd", soft_weights, value_low[:key_end], preferred_element_type=jnp.float32
        )
        mixed_blocks.append(mixed.astype(jnp.bfloat16).reshape(QBLK, local_heads * HD))
    mixed_full = jnp.concatenate(mixed_blocks, axis=0)
    attended_partial = jnp.dot(
        mixed_full, output_full, preferred_element_type=jnp.float32
    ).astype(jnp.bfloat16)
    attended_partial, gate_full, up_full = lax.optimization_barrier(
        (attended_partial, gate_full, up_full)
    )
    attended = lax.psum_scatter(
        attended_partial,
        "tensor",
        scatter_dimension=0,
        tiled=True,
    ).astype(jnp.float32)
    middle = residual + RESIDUAL_SCALE * attended
    normed_two, unit_two, inverse_two = rms_forward(middle, gain_two)
    mixture_in = lax.all_gather(normed_two.astype(jnp.bfloat16), "tensor", axis=0, tiled=True)
    down_weight, mixture_in = lax.optimization_barrier((down_weight, mixture_in))
    down_full = lax.all_gather(down_weight, "dp", axis=2, tiled=True)
    logits = jnp.dot(mixture_in, router_full, preferred_element_type=jnp.float32)
    routed_marks = (
        expert_ids[:, :, None] == jnp.arange(EXPERTS, dtype=jnp.int32)[None, None, :]
    ).astype(jnp.float32)
    routed = jnp.sum(routed_marks * logits[:, None, :], axis=-1)
    gates = jax.nn.softmax(routed, axis=-1)
    slot_count = local_experts * CAP
    first_slot = lax.axis_index("tensor") * slot_count
    slot_pair = route_slots(expert_ids, fill_order[0], first_slot, slot_count)
    slot_valid = slot_pair >= 0
    safe_pair = jnp.maximum(slot_pair, 0)
    slot_token = safe_pair // TOPK
    slot_choice = safe_pair % TOPK
    side_lanes = 128
    gate_table = jnp.pad(gates, ((0, 0), (0, side_lanes - TOPK)))
    inputs, gate_rows = gather_rows(
        slot_token,
        (mixture_in.astype(jnp.float32), gate_table),
        CAP,
        (jnp.bfloat16, jnp.float32),
    )
    inputs = inputs.reshape(local_experts, CAP, D)
    choice_marks = slot_choice[:, None] == jnp.arange(side_lanes)[None, :]
    slot_gate = jnp.sum(jnp.where(choice_marks, gate_rows, 0.0), axis=1)
    slot_gate = jnp.where(slot_valid, slot_gate, 0.0).reshape(local_experts, CAP, 1)
    gate_pre = jnp.einsum("ecd,edf->ecf", inputs, gate_full, preferred_element_type=jnp.float32)
    up_pre = jnp.einsum("ecd,edf->ecf", inputs, up_full, preferred_element_type=jnp.float32)
    activated = jax.nn.silu(gate_pre)
    hidden_units = (slot_gate * activated * up_pre).astype(jnp.bfloat16)
    expert_out = jnp.einsum(
        "ecf,efd->ecd", hidden_units, down_full, preferred_element_type=jnp.float32
    )
    (mixture_sum,) = combine_rows(slot_token, (expert_out.reshape(slot_count, D),), CAP, TOK_GRP)
    out_grad_held, down_full = lax.optimization_barrier((out_grad, down_full))
    cotangent_full = lax.all_gather(out_grad_held, "tensor", axis=0, tiled=True)
    scaled_cotangent = (
        (RESIDUAL_SCALE * cotangent_full.astype(jnp.float32)).astype(jnp.bfloat16).astype(jnp.float32)
    )
    scaled_cotangent, mixture_sum = lax.optimization_barrier((scaled_cotangent, mixture_sum))
    mixture_part = lax.psum_scatter(
        mixture_sum.astype(jnp.bfloat16), "tensor", scatter_dimension=0, tiled=True
    ).astype(jnp.float32)
    (out_rows,) = gather_rows(slot_token, (scaled_cotangent,), CAP, (jnp.bfloat16,))
    out_rows = out_rows.reshape(local_experts, CAP, D)
    hidden_grad = jnp.einsum("ecd,efd->ecf", out_rows, down_full, preferred_element_type=jnp.float32)
    gate_grad_slot = jnp.sum(activated * up_pre * hidden_grad, axis=-1).reshape(slot_count)
    gate_grad_rows = jnp.where(
        choice_marks & slot_valid[:, None], gate_grad_slot[:, None], 0.0
    )
    product_grad = slot_gate * hidden_grad
    gate_pre_grad = (product_grad * up_pre * silu_slope(gate_pre)).astype(jnp.bfloat16)
    up_pre_grad = (product_grad * activated).astype(jnp.bfloat16)
    input_rows = jnp.einsum(
        "ecf,edf->ecd", gate_pre_grad, gate_full, preferred_element_type=jnp.float32
    ) + jnp.einsum("ecf,edf->ecd", up_pre_grad, up_full, preferred_element_type=jnp.float32)
    input_rows = input_rows.astype(jnp.bfloat16).reshape(slot_count, D)
    grad_in_mixture, gate_grad_table = combine_rows(
        slot_token, (input_rows, gate_grad_rows), CAP, TOK_GRP
    )
    (inputs, gate_pre_grad, up_pre_grad, hidden_units, out_rows), grad_in_mixture = (
        lax.optimization_barrier(
            ((inputs, gate_pre_grad, up_pre_grad, hidden_units, out_rows), grad_in_mixture)
        )
    )
    expert_parts = (
        jnp.einsum("ecd,ecf->edf", inputs, gate_pre_grad, preferred_element_type=jnp.float32),
        jnp.einsum("ecd,ecf->edf", inputs, up_pre_grad, preferred_element_type=jnp.float32),
        jnp.einsum("ecf,ecd->efd", hidden_units, out_rows, preferred_element_type=jnp.float32),
    )
    expert_parts = tuple(part.astype(jnp.bfloat16) for part in expert_parts)
    gates_grad = gate_grad_table[:, :TOPK]
    routed_grad = gates * (gates_grad - jnp.sum(gates * gates_grad, axis=-1, keepdims=True))
    logits_grad = jnp.sum(routed_marks * routed_grad[:, :, None], axis=1)
    router_part = jnp.einsum(
        "td,te->de", mixture_in, logits_grad, precision=HIGHEST, preferred_element_type=jnp.float32
    )
    grad_in_mixture = grad_in_mixture + jnp.einsum(
        "te,de->td", logits_grad, router_full.astype(jnp.float32), precision=HIGHEST
    )
    mixture_grad_low, mixture_part = lax.optimization_barrier(
        (grad_in_mixture.astype(jnp.bfloat16), mixture_part)
    )
    block_output = (middle + RESIDUAL_SCALE * mixture_part).astype(jnp.bfloat16)
    mixture_grad_shard = lax.psum_scatter(
        mixture_grad_low, "tensor", scatter_dimension=0, tiled=True
    ).astype(jnp.float32)
    middle_norm_grad, gain_two_grad = rms_backward(
        mixture_grad_shard, unit_two, inverse_two, gain_two
    )
    middle_grad = out_grad.astype(jnp.float32) + middle_norm_grad
    attended_grad = lax.all_gather(
        (RESIDUAL_SCALE * middle_grad).astype(jnp.bfloat16), "tensor", axis=0, tiled=True
    )
    expert_parts, router_part, attended_grad = lax.optimization_barrier(
        (expert_parts, router_part, attended_grad)
    )
    expert_grads = reduce_experts(expert_parts)
    router_weight_grad = lax.psum_scatter(
        router_part, ("dp", "tensor"), scatter_dimension=0, tiled=True
    )
    output_part = jnp.einsum(
        "tf,td->fd", mixed_full, attended_grad, preferred_element_type=jnp.float32
    )
    mixed_grad = jnp.einsum(
        "td,fd->tf", attended_grad, output_full, preferred_element_type=jnp.float32
    ).astype(jnp.bfloat16)
    mixed_grad = mixed_grad.reshape(TOK_GRP, local_groups, group_ratio, HD)
    key_grad = jnp.zeros((TOK_GRP, local_groups, HD), jnp.float32)
    value_grad = jnp.zeros((TOK_GRP, local_groups, HD), jnp.float32)
    query_blocks = []
    for block_index in range(block_count):
        row_start = block_index * QBLK
        key_end = row_start + QBLK
        scores, queries = block_scores(
            query_rot, key_rot, segments, row_start, key_end, local_groups, group_ratio
        )
        soft_full = jnp.exp(scores - logsum_blocks[block_index])
        soft_low = soft_full.astype(jnp.bfloat16)
        out_block = mixed_grad[row_start:key_end]
        weight_grad = jnp.einsum(
            "qgrd,kgd->grqk", out_block, value_low[:key_end], preferred_element_type=jnp.float32
        )
        delta = jnp.sum(soft_full * weight_grad, axis=-1, keepdims=True)
        score_grad = (soft_full * (weight_grad - delta)).astype(jnp.bfloat16)
        query_blocks.append(
            jnp.einsum(
                "grqk,kgd->qgrd", score_grad, key_rot[:key_end], preferred_element_type=jnp.float32
            )
            * ATTN_SCALE
        )
        key_grad = key_grad.at[:key_end].add(
            jnp.einsum("grqk,qgrd->kgd", score_grad, queries, preferred_element_type=jnp.float32)
            * ATTN_SCALE
        )
        value_grad = value_grad.at[:key_end].add(
            jnp.einsum("grqk,qgrd->kgd", soft_low, out_block, preferred_element_type=jnp.float32)
        )
        if block_index == block_count - 2:
            key_grad, value_grad, expert_grads, router_weight_grad = lax.optimization_barrier(
                (key_grad, value_grad, expert_grads, router_weight_grad)
            )
    gate_weight_grad, up_weight_grad, down_weight_grad = expert_grads
    query_rot_grad = jnp.concatenate(query_blocks, axis=0).reshape(TOK_GRP, local_heads, HD)
    query_grad = (
        rotate_back(query_rot_grad, cosine_table, sine_table)
        .astype(jnp.bfloat16)
        .reshape(TOK_GRP, local_heads * HD)
    )
    key_grad_low = (
        rotate_back(key_grad, cosine_table, sine_table)
        .astype(jnp.bfloat16)
        .reshape(TOK_GRP, local_groups * HD)
    )
    value_grad_low = value_grad.astype(jnp.bfloat16).reshape(TOK_GRP, local_groups * HD)
    total_rows = jnp.einsum("tf,df->td", query_grad, query_full, preferred_element_type=jnp.float32)
    total_rows = total_rows + jnp.einsum(
        "tf,df->td", key_grad_low, key_full, preferred_element_type=jnp.float32
    )
    normed_grad_low = (
        total_rows
        + jnp.einsum("tf,df->td", value_grad_low, value_full, preferred_element_type=jnp.float32)
    ).astype(jnp.bfloat16)
    normed_grad_low, query_grad, key_grad_low, value_grad_low = lax.optimization_barrier(
        (normed_grad_low, query_grad, key_grad_low, value_grad_low)
    )
    normed_grad = lax.psum_scatter(
        normed_grad_low, "tensor", scatter_dimension=0, tiled=True
    ).astype(jnp.float32)
    query_part = jnp.einsum(
        "td,tf->df", normed_full, query_grad, preferred_element_type=jnp.float32
    )
    key_part = jnp.einsum(
        "td,tf->df", normed_full, key_grad_low, preferred_element_type=jnp.float32
    )
    value_part = jnp.einsum(
        "td,tf->df", normed_full, value_grad_low, preferred_element_type=jnp.float32
    )
    projection_parts = jnp.concatenate(
        [query_part, key_part, value_part], axis=1
    ).astype(jnp.bfloat16)
    projection_parts, normed_grad = lax.optimization_barrier((projection_parts, normed_grad))
    input_norm_grad, gain_one_grad = rms_backward(normed_grad, unit_one, inverse_one, gain_one)
    input_grad = middle_grad + input_norm_grad
    projection_grads = lax.psum_scatter(
        projection_parts, "dp", scatter_dimension=0, tiled=True
    ).astype(jnp.float32)
    query_width, key_width = query_part.shape[1], key_part.shape[1]
    query_weight_grad = projection_grads[:, :query_width]
    key_weight_grad = projection_grads[:, query_width : query_width + key_width]
    value_weight_grad = projection_grads[:, query_width + key_width :]
    output_weight_grad = lax.psum_scatter(
        output_part.astype(jnp.bfloat16), "dp", scatter_dimension=1, tiled=True
    ).astype(jnp.float32)
    attention_gain_grad, mixture_gain_grad = (
        lax.psum_scatter(gain_one_grad, ("dp", "tensor"), scatter_dimension=0, tiled=True),
        lax.psum_scatter(gain_two_grad, ("dp", "tensor"), scatter_dimension=0, tiled=True),
    )
    return (
        block_output,
        input_grad,
        attention_gain_grad,
        query_weight_grad,
        key_weight_grad,
        value_weight_grad,
        output_weight_grad,
        mixture_gain_grad,
        router_weight_grad,
        gate_weight_grad,
        up_weight_grad,
        down_weight_grad,
    )


def solution(mesh):
    in_specs = (
        P(("dp", "tensor"), None),
        P(("dp", "tensor"), None),
        P("dp", None),
        P("dp", None),
        P("dp", None),
        P("dp"),
        P("dp", "tensor"),
        P("dp", "tensor"),
        P("dp", "tensor"),
        P("tensor", "dp"),
        P("dp"),
        P("dp", None),
        P("tensor", "dp", None),
        P("tensor", "dp", None),
        P("tensor", None, "dp"),
    )
    out_specs = (
        P(("dp", "tensor"), None),
        P(("dp", "tensor"), None),
        P(("dp", "tensor")),
        P("dp", "tensor"),
        P("dp", "tensor"),
        P("dp", "tensor"),
        P("tensor", "dp"),
        P(("dp", "tensor")),
        P(("dp", "tensor"), None),
        P("tensor", "dp", None),
        P("tensor", "dp", None),
        P("tensor", None, "dp"),
    )
    return jax.shard_map(local, mesh=mesh, in_specs=in_specs, out_specs=out_specs, check_vma=False)
```

```python
import jax
import jax.numpy as jnp
from jax import lax
from jax.experimental import pallas as pl
from jax.experimental.pallas import tpu as pltpu
from jax.sharding import PartitionSpec as P

D = 1536
HD = 64
EXPERTS = 40
TOPK = 8
PROMPT = 2048
NCONT = 4
QBLK = 512
TOK_GRP = 3072
CAP = 768


ATTN_SCALE = 0.015625
RESIDUAL_SCALE = 0.22
NORM_EPS = 1e-06
ROPE_BASE = 10000.0
MASKED = -1e30
HIGHEST = lax.Precision.HIGHEST


def rms_forward(values, gain_row):
    inverse_rms = lax.rsqrt(jnp.mean(values * values, axis=-1, keepdims=True) + NORM_EPS)
    unit_rows = values * inverse_rms
    return (unit_rows * gain_row, unit_rows, inverse_rms)


def rms_backward(gradient, unit_rows, inverse_rms, gain_row):
    gain_grad = jnp.sum(gradient * unit_rows, axis=0)
    scaled = gradient * gain_row
    mean_term = jnp.mean(scaled * unit_rows, axis=-1, keepdims=True)
    return (inverse_rms * (scaled - unit_rows * mean_term), gain_grad)


def group_layout(segment_row, prompt_length):
    cont_length = segment_row.shape[0]
    segment_marks = (segment_row[:, None] == jnp.arange(NCONT, dtype=jnp.int32)[None, :]).astype(
        jnp.int32
    )
    segment_sizes = jnp.sum(segment_marks, axis=0)
    segment_starts = jnp.cumsum(segment_sizes) - segment_sizes
    token_starts = jnp.sum(segment_marks * segment_starts[None, :], axis=1)
    inside = jnp.arange(cont_length, dtype=jnp.int32) - token_starts
    positions = jnp.concatenate(
        [jnp.arange(prompt_length, dtype=jnp.int32), prompt_length + inside]
    )
    segments = jnp.concatenate([jnp.zeros((prompt_length,), jnp.int32), segment_row + 1])
    return (positions, segments)


def allowed(query_index, query_segment, key_index, key_segment):
    causal = key_index[None, :] <= query_index[:, None]
    shared = (key_segment[None, :] == 0) | (key_segment[None, :] == query_segment[:, None])
    return causal & shared


def rope_tables(positions, head_size):
    halfway = head_size // 2
    frequency = ROPE_BASE ** (-(2.0 * jnp.arange(halfway, dtype=jnp.float32)) / head_size)
    angles = positions.astype(jnp.float32)[:, None] * frequency[None, :]
    return (jnp.cos(angles), jnp.sin(angles))


def rotate(values, cosine_table, sine_table):
    halfway = values.shape[-1] // 2
    first_half = values[..., :halfway]
    second_half = values[..., halfway:]
    cosine_part = cosine_table[:, None, :]
    sine_part = sine_table[:, None, :]
    return jnp.concatenate(
        [
            first_half * cosine_part - second_half * sine_part,
            second_half * cosine_part + first_half * sine_part,
        ],
        axis=-1,
    )


def rotate_back(gradient, cosine_table, sine_table):
    halfway = gradient.shape[-1] // 2
    first_half = gradient[..., :halfway]
    second_half = gradient[..., halfway:]
    cosine_part = cosine_table[:, None, :]
    sine_part = sine_table[:, None, :]
    return jnp.concatenate(
        [
            first_half * cosine_part + second_half * sine_part,
            second_half * cosine_part - first_half * sine_part,
        ],
        axis=-1,
    )


def silu_slope(values):
    sigmoid_part = jax.nn.sigmoid(values)
    return sigmoid_part * (1.0 + values * (1.0 - sigmoid_part))


def route_slots(expert_row, order_row, first_slot, slot_count):
    pair_count = expert_row.shape[0] * expert_row.shape[1]
    ordered = table_lookup(expert_row.reshape(pair_count), order_row)
    onehot = ordered[:, None] == jnp.arange(EXPERTS, dtype=jnp.int32)[None, :]
    rank_block = 256
    blocks = pair_count // rank_block
    pair_marks = onehot.astype(jnp.bfloat16).reshape(blocks, rank_block, EXPERTS)
    lower_ones = (jnp.arange(rank_block)[:, None] >= jnp.arange(rank_block)[None, :]).astype(
        jnp.bfloat16
    )
    within = jnp.einsum(
        "ij,bje->bie", lower_ones, pair_marks, preferred_element_type=jnp.float32
    ).astype(jnp.int32)
    totals = within[:, -1, :]
    before = jnp.cumsum(totals, axis=0) - totals
    counts = (within + before[:, None, :]).reshape(pair_count, EXPERTS)
    pair_rank = jnp.sum(jnp.where(onehot, counts, 0), axis=1) - 1
    local_slot = ordered * CAP + pair_rank - first_slot
    kept = (pair_rank < CAP) & (local_slot >= 0) & (local_slot < slot_count)
    local_slot = jnp.where(kept, local_slot, -1)
    return invert_slots(local_slot, order_row, slot_count)


def _gather_rows_kernel(tok_ref, *refs):
    count = (len(refs) - 1) // 4
    sources, outs = refs[:count], refs[count : 2 * count]
    copies, rows_bufs, sem = refs[2 * count : 3 * count], refs[3 * count : 4 * count], refs[-1]
    rows = rows_bufs[0].shape[0]
    step = pl.program_id(0)

    @pl.when(step == 0)
    def _():
        for source, copy in zip(sources, copies):
            transfer = pltpu.make_async_copy(source, copy, sem)
            transfer.start()
            transfer.wait()

    base = step * rows

    def body(s, carry):
        t = tok_ref[base + s]
        for copy, rows_buf in zip(copies, rows_bufs):
            rows_buf[pl.ds(s, 1), :] = copy[pl.ds(t, 1), :]
        return carry

    lax.fori_loop(0, rows, body, 0, unroll=8)
    for out, rows_buf in zip(outs, rows_bufs):
        out[...] = rows_buf[...].astype(out.dtype)


def gather_rows(tok, sources, rows, out_dtypes):
    blocks = tok.shape[0] // rows
    return pl.pallas_call(
        _gather_rows_kernel,
        grid_spec=pltpu.PrefetchScalarGridSpec(
            num_scalar_prefetch=1,
            grid=(blocks,),
            in_specs=[pl.BlockSpec(memory_space=pl.ANY) for _ in sources],
            out_specs=[
                pl.BlockSpec((rows, source.shape[1]), lambda b, tok: (b, 0)) for source in sources
            ],
            scratch_shapes=[pltpu.VMEM(source.shape, jnp.float32) for source in sources]
            + [pltpu.VMEM((rows, source.shape[1]), jnp.float32) for source in sources]
            + [pltpu.SemaphoreType.DMA(())],
        ),
        out_shape=[
            jax.ShapeDtypeStruct((tok.shape[0], source.shape[1]), dtype)
            for source, dtype in zip(sources, out_dtypes)
        ],
        compiler_params=pltpu.CompilerParams(vmem_limit_bytes=56 * 1024 * 1024),
    )(tok, *sources)


def _combine_rows_kernel(tok_ref, *refs):
    count = (len(refs) - 1) // 4
    addends, outs = refs[:count], refs[count : 2 * count]
    totals, rows_bufs, sem = refs[2 * count : 3 * count], refs[3 * count : 4 * count], refs[-1]
    rows = rows_bufs[0].shape[0]
    step = pl.program_id(0)

    @pl.when(step == 0)
    def _():
        for total in totals:
            total[...] = jnp.zeros_like(total)

    for addend, rows_buf in zip(addends, rows_bufs):
        rows_buf[...] = addend[...].astype(jnp.float32)
    base = step * rows

    def body(s, carry):
        t = tok_ref[base + s]
        for total, rows_buf in zip(totals, rows_bufs):
            total[pl.ds(t, 1), :] += rows_buf[pl.ds(s, 1), :]
        return carry

    lax.fori_loop(0, rows, body, 0, unroll=8)

    @pl.when(step == pl.num_programs(0) - 1)
    def _():
        for total, out in zip(totals, outs):
            transfer = pltpu.make_async_copy(total, out, sem)
            transfer.start()
            transfer.wait()


def combine_rows(tok, addends, rows, total_rows):
    blocks = tok.shape[0] // rows
    return pl.pallas_call(
        _combine_rows_kernel,
        grid_spec=pltpu.PrefetchScalarGridSpec(
            num_scalar_prefetch=1,
            grid=(blocks,),
            in_specs=[
                pl.BlockSpec((rows, addend.shape[1]), lambda b, tok: (b, 0)) for addend in addends
            ],
            out_specs=[pl.BlockSpec(memory_space=pl.ANY) for _ in addends],
            scratch_shapes=[
                pltpu.VMEM((total_rows, addend.shape[1]), jnp.float32) for addend in addends
            ]
            + [pltpu.VMEM((rows, addend.shape[1]), jnp.float32) for addend in addends]
            + [pltpu.SemaphoreType.DMA(())],
        ),
        out_shape=[
            jax.ShapeDtypeStruct((total_rows, addend.shape[1]), jnp.float32) for addend in addends
        ],
        compiler_params=pltpu.CompilerParams(vmem_limit_bytes=56 * 1024 * 1024),
    )(tok, *addends)


def table_lookup(table, index):
    lanes = 128
    high_count = table.shape[0] // lanes
    low_marks = (index[:, None] % lanes == jnp.arange(lanes)[None, :]).astype(jnp.bfloat16)
    picked = jnp.dot(
        low_marks,
        table.reshape(high_count, lanes).astype(jnp.bfloat16).T,
        preferred_element_type=jnp.float32,
    )
    high_marks = index[:, None] // lanes == jnp.arange(high_count)[None, :]
    return jnp.sum(jnp.where(high_marks, picked, 0.0), axis=1).astype(jnp.int32)


def invert_slots(local_slot, values, slot_count):
    lanes = 128
    high_count = slot_count // lanes
    column_marks = (local_slot[:, None] // lanes == jnp.arange(high_count)[None, :]).astype(
        jnp.bfloat16
    )
    lane_marks = local_slot[:, None] % lanes == jnp.arange(lanes)[None, :]
    shifted = values + 1
    parts = []
    for digit in (shifted // 256, shifted % 256):
        spread = jnp.where(lane_marks, digit[:, None], 0).astype(jnp.bfloat16)
        parts.append(
            jnp.einsum("ic,il->cl", column_marks, spread, preferred_element_type=jnp.float32)
        )
    return (256.0 * parts[0] + parts[1]).astype(jnp.int32).reshape(slot_count) - 1


def block_scores(query_rot, key_rot, segments, row_start, key_end, local_groups, group_ratio):
    queries = query_rot[row_start:key_end].reshape(
        key_end - row_start, local_groups, group_ratio, HD
    )
    raw_scores = (
        jnp.einsum("qgrd,kgd->grqk", queries, key_rot[:key_end], preferred_element_type=jnp.float32)
        * ATTN_SCALE
    )
    visible = allowed(
        jnp.arange(row_start, key_end, dtype=jnp.int32),
        segments[row_start:key_end],
        jnp.arange(key_end, dtype=jnp.int32),
        segments[:key_end],
    )
    return (jnp.where(visible[None, None], raw_scores, MASKED), queries)


def fetch_experts(gate_weight, up_weight, down_weight):
    return (
        lax.all_gather(gate_weight, "dp", axis=1, tiled=True),
        lax.all_gather(up_weight, "dp", axis=1, tiled=True),
        lax.all_gather(down_weight, "dp", axis=2, tiled=True),
    )


def reduce_experts(grads):
    return (
        lax.psum_scatter(grads[0], "dp", scatter_dimension=1, tiled=True).astype(jnp.float32),
        lax.psum_scatter(grads[1], "dp", scatter_dimension=1, tiled=True).astype(jnp.float32),
        jnp.swapaxes(
            lax.psum_scatter(grads[2], "dp", scatter_dimension=1, tiled=True).astype(jnp.float32),
            1,
            2,
        ),
    )


def local(
    hidden_in,
    out_grad,
    segment_ids,
    expert_ids,
    fill_order,
    attention_gain,
    query_weight,
    key_weight,
    value_weight,
    output_weight,
    mixture_gain,
    router_weight,
    gate_weight,
    up_weight,
    down_weight,
):
    local_heads = query_weight.shape[1] // HD
    local_groups = key_weight.shape[1] // HD
    group_ratio = local_heads // local_groups
    block_count = TOK_GRP // QBLK
    local_experts = gate_weight.shape[0]
    gain_one, query_full, key_full, value_full, output_full, gain_two, router_full = (
        lax.all_gather(attention_gain, "dp", axis=0, tiled=True),
        lax.all_gather(query_weight, "dp", axis=0, tiled=True),
        lax.all_gather(key_weight, "dp", axis=0, tiled=True),
        lax.all_gather(value_weight, "dp", axis=0, tiled=True),
        lax.all_gather(output_weight, "dp", axis=1, tiled=True),
        lax.all_gather(mixture_gain, "dp", axis=0, tiled=True),
        lax.all_gather(router_weight, "dp", axis=0, tiled=True),
    )
    output_all = lax.all_gather(output_full, "tensor", axis=0, tiled=True)
    gain_one = gain_one.astype(jnp.float32)
    gain_two = gain_two.astype(jnp.float32)
    residual = hidden_in.astype(jnp.float32)
    normed_shard, unit_one, inverse_one = rms_forward(residual, gain_one)
    normed_full = lax.all_gather(normed_shard.astype(jnp.bfloat16), "tensor", axis=0, tiled=True)
    gate_weight, up_weight, normed_full = lax.optimization_barrier(
        (gate_weight, up_weight, normed_full)
    )
    gate_full = lax.all_gather(gate_weight, "dp", axis=1, tiled=True)
    up_full = lax.all_gather(up_weight, "dp", axis=1, tiled=True)
    positions, segments = group_layout(segment_ids[0], PROMPT)
    cosine_table, sine_table = rope_tables(positions, HD)
    query_pre = jnp.dot(normed_full, query_full, preferred_element_type=jnp.float32).reshape(
        TOK_GRP, local_heads, HD
    )
    key_pre = jnp.dot(normed_full, key_full, preferred_element_type=jnp.float32).reshape(
        TOK_GRP, local_groups, HD
    )
    value_low = (
        jnp.dot(normed_full, value_full, preferred_element_type=jnp.float32)
        .astype(jnp.bfloat16)
        .reshape(TOK_GRP, local_groups, HD)
    )
    query_rot = rotate(query_pre, cosine_table, sine_table).astype(jnp.bfloat16)
    key_rot = rotate(key_pre, cosine_table, sine_table).astype(jnp.bfloat16)
    mixed_blocks = []
    logsum_blocks = []
    for block_index in range(block_count):
        row_start = block_index * QBLK
        key_end = row_start + QBLK
        scores, queries = block_scores(
            query_rot, key_rot, segments, row_start, key_end, local_groups, group_ratio
        )
        top_score = jnp.max(scores, axis=-1, keepdims=True)
        shifted_exp = jnp.exp(scores - top_score)
        total_exp = jnp.sum(shifted_exp, axis=-1, keepdims=True)
        soft_weights = (shifted_exp / total_exp).astype(jnp.bfloat16)
        logsum_blocks.append(top_score + jnp.log(total_exp))
        mixed = jnp.einsum(
            "grqk,kgd->qgrd", soft_weights, value_low[:key_end], preferred_element_type=jnp.float32
        )
        mixed_blocks.append(mixed.astype(jnp.bfloat16).reshape(QBLK, local_heads * HD))
    mixed_full = jnp.concatenate(mixed_blocks, axis=0)
    mixed_full, gate_full, up_full = lax.optimization_barrier((mixed_full, gate_full, up_full))
    mixed_own = lax.all_to_all(mixed_full, "tensor", 0, 1, tiled=True)
    attended = jnp.dot(mixed_own, output_all, preferred_element_type=jnp.float32)
    middle = residual + RESIDUAL_SCALE * attended
    normed_two, unit_two, inverse_two = rms_forward(middle, gain_two)
    mixture_in = lax.all_gather(normed_two.astype(jnp.bfloat16), "tensor", axis=0, tiled=True)
    down_weight, mixture_in = lax.optimization_barrier((down_weight, mixture_in))
    down_full = lax.all_gather(down_weight, "dp", axis=2, tiled=True)
    logits = jnp.dot(mixture_in, router_full, preferred_element_type=jnp.float32)
    routed_marks = (
        expert_ids[:, :, None] == jnp.arange(EXPERTS, dtype=jnp.int32)[None, None, :]
    ).astype(jnp.float32)
    routed = jnp.sum(routed_marks * logits[:, None, :], axis=-1)
    gates = jax.nn.softmax(routed, axis=-1)
    slot_count = local_experts * CAP
    first_slot = lax.axis_index("tensor") * slot_count
    slot_pair = route_slots(expert_ids, fill_order[0], first_slot, slot_count)
    slot_valid = slot_pair >= 0
    safe_pair = jnp.maximum(slot_pair, 0)
    slot_token = safe_pair // TOPK
    slot_choice = safe_pair % TOPK
    side_lanes = 128
    gate_table = jnp.pad(gates, ((0, 0), (0, side_lanes - TOPK)))
    inputs, gate_rows = gather_rows(
        slot_token,
        (mixture_in.astype(jnp.float32), gate_table),
        CAP,
        (jnp.bfloat16, jnp.float32),
    )
    inputs = inputs.reshape(local_experts, CAP, D)
    choice_marks = slot_choice[:, None] == jnp.arange(side_lanes)[None, :]
    slot_gate = jnp.sum(jnp.where(choice_marks, gate_rows, 0.0), axis=1)
    slot_gate = jnp.where(slot_valid, slot_gate, 0.0).reshape(local_experts, CAP, 1)
    gate_pre = jnp.einsum("ecd,edf->ecf", inputs, gate_full, preferred_element_type=jnp.float32)
    up_pre = jnp.einsum("ecd,edf->ecf", inputs, up_full, preferred_element_type=jnp.float32)
    activated = jax.nn.silu(gate_pre)
    hidden_units = (slot_gate * activated * up_pre).astype(jnp.bfloat16)
    expert_out = jnp.einsum(
        "ecf,efd->ecd", hidden_units, down_full, preferred_element_type=jnp.float32
    )
    (mixture_sum,) = combine_rows(slot_token, (expert_out.reshape(slot_count, D),), CAP, TOK_GRP)
    out_grad_held, down_full = lax.optimization_barrier((out_grad, down_full))
    cotangent_full = lax.all_gather(out_grad_held, "tensor", axis=0, tiled=True)
    scaled_cotangent = (
        (RESIDUAL_SCALE * cotangent_full.astype(jnp.float32)).astype(jnp.bfloat16).astype(jnp.float32)
    )
    scaled_cotangent, mixture_sum = lax.optimization_barrier((scaled_cotangent, mixture_sum))
    mixture_part = lax.psum_scatter(
        mixture_sum.astype(jnp.bfloat16), "tensor", scatter_dimension=0, tiled=True
    ).astype(jnp.float32)
    (out_rows,) = gather_rows(slot_token, (scaled_cotangent,), CAP, (jnp.bfloat16,))
    out_rows = out_rows.reshape(local_experts, CAP, D)
    hidden_grad = jnp.einsum("ecd,efd->ecf", out_rows, down_full, preferred_element_type=jnp.float32)
    gate_grad_slot = jnp.sum(activated * up_pre * hidden_grad, axis=-1).reshape(slot_count)
    gate_grad_rows = jnp.where(
        choice_marks & slot_valid[:, None], gate_grad_slot[:, None], 0.0
    )
    product_grad = slot_gate * hidden_grad
    gate_pre_grad = (product_grad * up_pre * silu_slope(gate_pre)).astype(jnp.bfloat16)
    up_pre_grad = (product_grad * activated).astype(jnp.bfloat16)
    input_rows = jnp.einsum(
        "ecf,edf->ecd", gate_pre_grad, gate_full, preferred_element_type=jnp.float32
    ) + jnp.einsum("ecf,edf->ecd", up_pre_grad, up_full, preferred_element_type=jnp.float32)
    input_rows = input_rows.astype(jnp.bfloat16).reshape(slot_count, D)
    grad_in_mixture, gate_grad_table = combine_rows(
        slot_token, (input_rows, gate_grad_rows), CAP, TOK_GRP
    )
    (inputs, gate_pre_grad, up_pre_grad, hidden_units, out_rows), grad_in_mixture = (
        lax.optimization_barrier(
            ((inputs, gate_pre_grad, up_pre_grad, hidden_units, out_rows), grad_in_mixture)
        )
    )
    expert_parts = (
        jnp.einsum("ecd,ecf->edf", inputs, gate_pre_grad, preferred_element_type=jnp.float32),
        jnp.einsum("ecd,ecf->edf", inputs, up_pre_grad, preferred_element_type=jnp.float32),
        jnp.einsum("ecd,ecf->edf", out_rows, hidden_units, preferred_element_type=jnp.float32),
    )
    expert_parts = tuple(part.astype(jnp.bfloat16) for part in expert_parts)
    gates_grad = gate_grad_table[:, :TOPK]
    routed_grad = gates * (gates_grad - jnp.sum(gates * gates_grad, axis=-1, keepdims=True))
    logits_grad = jnp.sum(routed_marks * routed_grad[:, :, None], axis=1)
    router_part = jnp.einsum(
        "td,te->de", mixture_in, logits_grad, precision=HIGHEST, preferred_element_type=jnp.float32
    )
    grad_in_mixture = grad_in_mixture + jnp.einsum(
        "te,de->td", logits_grad, router_full.astype(jnp.float32), precision=HIGHEST
    )
    mixture_grad_low, mixture_part = lax.optimization_barrier(
        (grad_in_mixture.astype(jnp.bfloat16), mixture_part)
    )
    block_output = (middle + RESIDUAL_SCALE * mixture_part).astype(jnp.bfloat16)
    mixture_grad_shard = lax.psum_scatter(
        mixture_grad_low, "tensor", scatter_dimension=0, tiled=True
    ).astype(jnp.float32)
    middle_norm_grad, gain_two_grad = rms_backward(
        mixture_grad_shard, unit_two, inverse_two, gain_two
    )
    middle_grad = out_grad.astype(jnp.float32) + middle_norm_grad
    attended_grad = (RESIDUAL_SCALE * middle_grad).astype(jnp.bfloat16)
    mixed_grad_own = jnp.einsum(
        "td,fd->tf", attended_grad, output_all, preferred_element_type=jnp.float32
    ).astype(jnp.bfloat16)
    mixed_grad = lax.all_to_all(mixed_grad_own, "tensor", 1, 0, tiled=True)
    expert_parts, router_part, mixed_grad = lax.optimization_barrier(
        (expert_parts, router_part, mixed_grad)
    )
    expert_grads = reduce_experts(expert_parts)
    router_weight_grad = lax.psum_scatter(
        router_part, ("dp", "tensor"), scatter_dimension=0, tiled=True
    )
    output_part = jnp.einsum(
        "tf,td->fd", mixed_own, attended_grad, preferred_element_type=jnp.float32
    ).astype(jnp.bfloat16)
    output_part = lax.psum_scatter(output_part, "dp", scatter_dimension=1, tiled=True)
    mixed_grad = mixed_grad.reshape(TOK_GRP, local_groups, group_ratio, HD)
    output_weight_grad = lax.psum_scatter(
        output_part, "tensor", scatter_dimension=0, tiled=True
    ).astype(jnp.float32)
    mixture_gain_grad = lax.psum_scatter(
        gain_two_grad, ("dp", "tensor"), scatter_dimension=0, tiled=True
    )
    key_grad = jnp.zeros((TOK_GRP, local_groups, HD), jnp.float32)
    value_grad = jnp.zeros((TOK_GRP, local_groups, HD), jnp.float32)
    query_blocks = []
    for block_index in range(block_count):
        row_start = block_index * QBLK
        key_end = row_start + QBLK
        scores, queries = block_scores(
            query_rot, key_rot, segments, row_start, key_end, local_groups, group_ratio
        )
        soft_full = jnp.exp(scores - logsum_blocks[block_index])
        soft_low = soft_full.astype(jnp.bfloat16)
        out_block = mixed_grad[row_start:key_end]
        weight_grad = jnp.einsum(
            "qgrd,kgd->grqk", out_block, value_low[:key_end], preferred_element_type=jnp.float32
        )
        delta = jnp.sum(soft_full * weight_grad, axis=-1, keepdims=True)
        score_grad = (soft_full * (weight_grad - delta)).astype(jnp.bfloat16)
        query_blocks.append(
            jnp.einsum(
                "grqk,kgd->qgrd", score_grad, key_rot[:key_end], preferred_element_type=jnp.float32
            )
            * ATTN_SCALE
        )
        key_grad = key_grad.at[:key_end].add(
            jnp.einsum("grqk,qgrd->kgd", score_grad, queries, preferred_element_type=jnp.float32)
            * ATTN_SCALE
        )
        value_grad = value_grad.at[:key_end].add(
            jnp.einsum("grqk,qgrd->kgd", soft_low, out_block, preferred_element_type=jnp.float32)
        )
        if block_index == block_count - 2:
            (
                key_grad,
                value_grad,
                expert_grads,
                router_weight_grad,
                output_weight_grad,
                mixture_gain_grad,
            ) = lax.optimization_barrier(
                (
                    key_grad,
                    value_grad,
                    expert_grads,
                    router_weight_grad,
                    output_weight_grad,
                    mixture_gain_grad,
                )
            )
    gate_weight_grad, up_weight_grad, down_weight_grad = expert_grads
    query_rot_grad = jnp.concatenate(query_blocks, axis=0).reshape(TOK_GRP, local_heads, HD)
    query_grad = (
        rotate_back(query_rot_grad, cosine_table, sine_table)
        .astype(jnp.bfloat16)
        .reshape(TOK_GRP, local_heads * HD)
    )
    key_grad_low = (
        rotate_back(key_grad, cosine_table, sine_table)
        .astype(jnp.bfloat16)
        .reshape(TOK_GRP, local_groups * HD)
    )
    value_grad_low = value_grad.astype(jnp.bfloat16).reshape(TOK_GRP, local_groups * HD)
    total_rows = jnp.einsum("tf,df->td", query_grad, query_full, preferred_element_type=jnp.float32)
    total_rows = total_rows + jnp.einsum(
        "tf,df->td", key_grad_low, key_full, preferred_element_type=jnp.float32
    )
    normed_grad_low = (
        total_rows
        + jnp.einsum("tf,df->td", value_grad_low, value_full, preferred_element_type=jnp.float32)
    ).astype(jnp.bfloat16)
    normed_grad_low, query_grad, key_grad_low, value_grad_low = lax.optimization_barrier(
        (normed_grad_low, query_grad, key_grad_low, value_grad_low)
    )
    normed_grad = lax.psum_scatter(
        normed_grad_low, "tensor", scatter_dimension=0, tiled=True
    ).astype(jnp.float32)
    query_part = jnp.einsum(
        "td,tf->df", normed_full, query_grad, preferred_element_type=jnp.float32
    )
    key_part = jnp.einsum(
        "td,tf->df", normed_full, key_grad_low, preferred_element_type=jnp.float32
    )
    value_part = jnp.einsum(
        "td,tf->df", normed_full, value_grad_low, preferred_element_type=jnp.float32
    )
    projection_parts = jnp.concatenate(
        [query_part, key_part, value_part], axis=1
    ).astype(jnp.bfloat16)
    projection_parts, normed_grad = lax.optimization_barrier((projection_parts, normed_grad))
    input_norm_grad, gain_one_grad = rms_backward(normed_grad, unit_one, inverse_one, gain_one)
    input_grad = middle_grad + input_norm_grad
    projection_grads = lax.psum_scatter(
        projection_parts, "dp", scatter_dimension=0, tiled=True
    ).astype(jnp.float32)
    query_width, key_width = query_part.shape[1], key_part.shape[1]
    query_weight_grad = projection_grads[:, :query_width]
    key_weight_grad = projection_grads[:, query_width : query_width + key_width]
    value_weight_grad = projection_grads[:, query_width + key_width :]

    attention_gain_grad = lax.psum_scatter(
        gain_one_grad, ("dp", "tensor"), scatter_dimension=0, tiled=True
    )
    return (
        block_output,
        input_grad,
        attention_gain_grad,
        query_weight_grad,
        key_weight_grad,
        value_weight_grad,
        output_weight_grad,
        mixture_gain_grad,
        router_weight_grad,
        gate_weight_grad,
        up_weight_grad,
        down_weight_grad,
    )


def solution(mesh):
    in_specs = (
        P(("dp", "tensor"), None),
        P(("dp", "tensor"), None),
        P("dp", None),
        P("dp", None),
        P("dp", None),
        P("dp"),
        P("dp", "tensor"),
        P("dp", "tensor"),
        P("dp", "tensor"),
        P("tensor", "dp"),
        P("dp"),
        P("dp", None),
        P("tensor", "dp", None),
        P("tensor", "dp", None),
        P("tensor", None, "dp"),
    )
    out_specs = (
        P(("dp", "tensor"), None),
        P(("dp", "tensor"), None),
        P(("dp", "tensor")),
        P("dp", "tensor"),
        P("dp", "tensor"),
        P("dp", "tensor"),
        P("tensor", "dp"),
        P(("dp", "tensor")),
        P(("dp", "tensor"), None),
        P("tensor", "dp", None),
        P("tensor", "dp", None),
        P("tensor", None, "dp"),
    )
    return jax.shard_map(local, mesh=mesh, in_specs=in_specs, out_specs=out_specs, check_vma=False)
```

```python
import jax
import jax.numpy as jnp
from jax import lax
from jax.experimental import pallas as pl
from jax.experimental.pallas import tpu as pltpu
from jax.sharding import PartitionSpec as P

D = 1536
HD = 64
EXPERTS = 40
TOPK = 8
PROMPT = 2048
NCONT = 4
QBLK = 512
TOK_GRP = 3072
CAP = 768


ATTN_SCALE = 0.015625
RESIDUAL_SCALE = 0.22
NORM_EPS = 1e-06
ROPE_BASE = 10000.0
MASKED = -1e30
HIGHEST = lax.Precision.HIGHEST


def rms_forward(values, gain_row):
    inverse_rms = lax.rsqrt(jnp.mean(values * values, axis=-1, keepdims=True) + NORM_EPS)
    unit_rows = values * inverse_rms
    return (unit_rows * gain_row, unit_rows, inverse_rms)


def rms_backward(gradient, unit_rows, inverse_rms, gain_row):
    gain_grad = jnp.sum(gradient * unit_rows, axis=0)
    scaled = gradient * gain_row
    mean_term = jnp.mean(scaled * unit_rows, axis=-1, keepdims=True)
    return (inverse_rms * (scaled - unit_rows * mean_term), gain_grad)


def group_layout(segment_row, prompt_length):
    cont_length = segment_row.shape[0]
    segment_marks = (segment_row[:, None] == jnp.arange(NCONT, dtype=jnp.int32)[None, :]).astype(
        jnp.int32
    )
    segment_sizes = jnp.sum(segment_marks, axis=0)
    segment_starts = jnp.cumsum(segment_sizes) - segment_sizes
    token_starts = jnp.sum(segment_marks * segment_starts[None, :], axis=1)
    inside = jnp.arange(cont_length, dtype=jnp.int32) - token_starts
    positions = jnp.concatenate(
        [jnp.arange(prompt_length, dtype=jnp.int32), prompt_length + inside]
    )
    segments = jnp.concatenate([jnp.zeros((prompt_length,), jnp.int32), segment_row + 1])
    return (positions, segments)


def allowed(query_index, query_segment, key_index, key_segment):
    causal = key_index[None, :] <= query_index[:, None]
    shared = (key_segment[None, :] == 0) | (key_segment[None, :] == query_segment[:, None])
    return causal & shared


def rope_tables(positions, head_size):
    halfway = head_size // 2
    frequency = ROPE_BASE ** (-(2.0 * jnp.arange(halfway, dtype=jnp.float32)) / head_size)
    angles = positions.astype(jnp.float32)[:, None] * frequency[None, :]
    return (jnp.cos(angles), jnp.sin(angles))


def rotate(values, cosine_table, sine_table):
    halfway = values.shape[-1] // 2
    first_half = values[..., :halfway]
    second_half = values[..., halfway:]
    cosine_part = cosine_table[:, None, :]
    sine_part = sine_table[:, None, :]
    return jnp.concatenate(
        [
            first_half * cosine_part - second_half * sine_part,
            second_half * cosine_part + first_half * sine_part,
        ],
        axis=-1,
    )


def rotate_back(gradient, cosine_table, sine_table):
    halfway = gradient.shape[-1] // 2
    first_half = gradient[..., :halfway]
    second_half = gradient[..., halfway:]
    cosine_part = cosine_table[:, None, :]
    sine_part = sine_table[:, None, :]
    return jnp.concatenate(
        [
            first_half * cosine_part + second_half * sine_part,
            second_half * cosine_part - first_half * sine_part,
        ],
        axis=-1,
    )


def silu_slope(values):
    sigmoid_part = jax.nn.sigmoid(values)
    return sigmoid_part * (1.0 + values * (1.0 - sigmoid_part))


def route_slots(expert_row, order_row, first_slot, slot_count):
    pair_count = expert_row.shape[0] * expert_row.shape[1]
    ordered = table_lookup(expert_row.reshape(pair_count), order_row)
    onehot = ordered[:, None] == jnp.arange(EXPERTS, dtype=jnp.int32)[None, :]
    rank_block = 256
    blocks = pair_count // rank_block
    pair_marks = onehot.astype(jnp.bfloat16).reshape(blocks, rank_block, EXPERTS)
    lower_ones = (jnp.arange(rank_block)[:, None] >= jnp.arange(rank_block)[None, :]).astype(
        jnp.bfloat16
    )
    within = jnp.einsum(
        "ij,bje->bie", lower_ones, pair_marks, preferred_element_type=jnp.float32
    ).astype(jnp.int32)
    totals = within[:, -1, :]
    before = jnp.cumsum(totals, axis=0) - totals
    counts = (within + before[:, None, :]).reshape(pair_count, EXPERTS)
    pair_rank = jnp.sum(jnp.where(onehot, counts, 0), axis=1) - 1
    local_slot = ordered * CAP + pair_rank - first_slot
    kept = (pair_rank < CAP) & (local_slot >= 0) & (local_slot < slot_count)
    local_slot = jnp.where(kept, local_slot, -1)
    return invert_slots(local_slot, order_row, slot_count)


def _gather_rows_kernel(tok_ref, *refs):
    count = (len(refs) - 1) // 4
    sources, outs = refs[:count], refs[count : 2 * count]
    copies, rows_bufs, sem = refs[2 * count : 3 * count], refs[3 * count : 4 * count], refs[-1]
    rows = rows_bufs[0].shape[0]
    step = pl.program_id(0)

    @pl.when(step == 0)
    def _():
        for source, copy in zip(sources, copies):
            transfer = pltpu.make_async_copy(source, copy, sem)
            transfer.start()
            transfer.wait()

    base = step * rows

    def body(s, carry):
        t = tok_ref[base + s]
        for copy, rows_buf in zip(copies, rows_bufs):
            rows_buf[pl.ds(s, 1), :] = copy[pl.ds(t, 1), :]
        return carry

    lax.fori_loop(0, rows, body, 0, unroll=8)
    for out, rows_buf in zip(outs, rows_bufs):
        out[...] = rows_buf[...].astype(out.dtype)


def gather_rows(tok, sources, rows, out_dtypes):
    blocks = tok.shape[0] // rows
    return pl.pallas_call(
        _gather_rows_kernel,
        grid_spec=pltpu.PrefetchScalarGridSpec(
            num_scalar_prefetch=1,
            grid=(blocks,),
            in_specs=[pl.BlockSpec(memory_space=pl.ANY) for _ in sources],
            out_specs=[
                pl.BlockSpec((rows, source.shape[1]), lambda b, tok: (b, 0)) for source in sources
            ],
            scratch_shapes=[pltpu.VMEM(source.shape, jnp.float32) for source in sources]
            + [pltpu.VMEM((rows, source.shape[1]), jnp.float32) for source in sources]
            + [pltpu.SemaphoreType.DMA(())],
        ),
        out_shape=[
            jax.ShapeDtypeStruct((tok.shape[0], source.shape[1]), dtype)
            for source, dtype in zip(sources, out_dtypes)
        ],
        compiler_params=pltpu.CompilerParams(vmem_limit_bytes=56 * 1024 * 1024),
    )(tok, *sources)


def _combine_rows_kernel(tok_ref, *refs):
    count = (len(refs) - 1) // 4
    addends, outs = refs[:count], refs[count : 2 * count]
    totals, rows_bufs, sem = refs[2 * count : 3 * count], refs[3 * count : 4 * count], refs[-1]
    rows = rows_bufs[0].shape[0]
    step = pl.program_id(0)

    @pl.when(step == 0)
    def _():
        for total in totals:
            total[...] = jnp.zeros_like(total)

    for addend, rows_buf in zip(addends, rows_bufs):
        rows_buf[...] = addend[...].astype(jnp.float32)
    base = step * rows

    def body(s, carry):
        t = tok_ref[base + s]
        for total, rows_buf in zip(totals, rows_bufs):
            total[pl.ds(t, 1), :] += rows_buf[pl.ds(s, 1), :]
        return carry

    lax.fori_loop(0, rows, body, 0, unroll=8)

    @pl.when(step == pl.num_programs(0) - 1)
    def _():
        for total, out in zip(totals, outs):
            transfer = pltpu.make_async_copy(total, out, sem)
            transfer.start()
            transfer.wait()


def combine_rows(tok, addends, rows, total_rows):
    blocks = tok.shape[0] // rows
    return pl.pallas_call(
        _combine_rows_kernel,
        grid_spec=pltpu.PrefetchScalarGridSpec(
            num_scalar_prefetch=1,
            grid=(blocks,),
            in_specs=[
                pl.BlockSpec((rows, addend.shape[1]), lambda b, tok: (b, 0)) for addend in addends
            ],
            out_specs=[pl.BlockSpec(memory_space=pl.ANY) for _ in addends],
            scratch_shapes=[
                pltpu.VMEM((total_rows, addend.shape[1]), jnp.float32) for addend in addends
            ]
            + [pltpu.VMEM((rows, addend.shape[1]), jnp.float32) for addend in addends]
            + [pltpu.SemaphoreType.DMA(())],
        ),
        out_shape=[
            jax.ShapeDtypeStruct((total_rows, addend.shape[1]), jnp.float32) for addend in addends
        ],
        compiler_params=pltpu.CompilerParams(vmem_limit_bytes=56 * 1024 * 1024),
    )(tok, *addends)


def table_lookup(table, index):
    lanes = 128
    high_count = table.shape[0] // lanes
    low_marks = (index[:, None] % lanes == jnp.arange(lanes)[None, :]).astype(jnp.bfloat16)
    picked = jnp.dot(
        low_marks,
        table.reshape(high_count, lanes).astype(jnp.bfloat16).T,
        preferred_element_type=jnp.float32,
    )
    high_marks = index[:, None] // lanes == jnp.arange(high_count)[None, :]
    return jnp.sum(jnp.where(high_marks, picked, 0.0), axis=1).astype(jnp.int32)


def invert_slots(local_slot, values, slot_count):
    lanes = 128
    high_count = slot_count // lanes
    column_marks = (local_slot[:, None] // lanes == jnp.arange(high_count)[None, :]).astype(
        jnp.bfloat16
    )
    lane_marks = local_slot[:, None] % lanes == jnp.arange(lanes)[None, :]
    shifted = values + 1
    parts = []
    for digit in (shifted // 256, shifted % 256):
        spread = jnp.where(lane_marks, digit[:, None], 0).astype(jnp.bfloat16)
        parts.append(
            jnp.einsum("ic,il->cl", column_marks, spread, preferred_element_type=jnp.float32)
        )
    return (256.0 * parts[0] + parts[1]).astype(jnp.int32).reshape(slot_count) - 1


def block_scores(query_rot, key_rot, segments, row_start, key_end, local_groups, group_ratio):
    queries = query_rot[row_start:key_end].reshape(
        key_end - row_start, local_groups, group_ratio, HD
    )
    raw_scores = (
        jnp.einsum("qgrd,kgd->grqk", queries, key_rot[:key_end], preferred_element_type=jnp.float32)
        * ATTN_SCALE
    )
    visible = allowed(
        jnp.arange(row_start, key_end, dtype=jnp.int32),
        segments[row_start:key_end],
        jnp.arange(key_end, dtype=jnp.int32),
        segments[:key_end],
    )
    return (jnp.where(visible[None, None], raw_scores, MASKED), queries)


def fetch_experts(gate_weight, up_weight, down_weight):
    return (
        lax.all_gather(gate_weight, "dp", axis=1, tiled=True),
        lax.all_gather(up_weight, "dp", axis=1, tiled=True),
        lax.all_gather(down_weight, "dp", axis=2, tiled=True),
    )


def reduce_experts(grads):
    return (
        lax.psum_scatter(grads[0], "dp", scatter_dimension=1, tiled=True).astype(jnp.float32),
        lax.psum_scatter(grads[1], "dp", scatter_dimension=1, tiled=True).astype(jnp.float32),
        jnp.swapaxes(
            lax.psum_scatter(grads[2], "dp", scatter_dimension=1, tiled=True).astype(jnp.float32),
            1,
            2,
        ),
    )


def local(
    hidden_in,
    out_grad,
    segment_ids,
    expert_ids,
    fill_order,
    attention_gain,
    query_weight,
    key_weight,
    value_weight,
    output_weight,
    mixture_gain,
    router_weight,
    gate_weight,
    up_weight,
    down_weight,
):
    local_heads = query_weight.shape[1] // HD
    local_groups = key_weight.shape[1] // HD
    group_ratio = local_heads // local_groups
    block_count = TOK_GRP // QBLK
    local_experts = gate_weight.shape[0]
    gain_one, query_full, key_full, value_full, gain_two, router_full = (
        lax.all_gather(attention_gain, "dp", axis=0, tiled=True),
        lax.all_gather(query_weight, "dp", axis=0, tiled=True),
        lax.all_gather(key_weight, "dp", axis=0, tiled=True),
        lax.all_gather(value_weight, "dp", axis=0, tiled=True),
        lax.all_gather(mixture_gain, "dp", axis=0, tiled=True),
        lax.all_gather(router_weight, "dp", axis=0, tiled=True),
    )
    output_all = lax.all_gather(
        lax.all_gather(output_weight, "tensor", axis=0, tiled=True), "dp", axis=1, tiled=True
    )
    gain_one = gain_one.astype(jnp.float32)
    gain_two = gain_two.astype(jnp.float32)
    residual = hidden_in.astype(jnp.float32)
    normed_shard, unit_one, inverse_one = rms_forward(residual, gain_one)
    normed_full = lax.all_gather(normed_shard.astype(jnp.bfloat16), "tensor", axis=0, tiled=True)
    gate_weight, up_weight, normed_full = lax.optimization_barrier(
        (gate_weight, up_weight, normed_full)
    )
    gate_full = lax.all_gather(gate_weight, "dp", axis=1, tiled=True)
    up_full = lax.all_gather(up_weight, "dp", axis=1, tiled=True)
    positions, segments = group_layout(segment_ids[0], PROMPT)
    cosine_table, sine_table = rope_tables(positions, HD)
    query_pre = jnp.dot(normed_full, query_full, preferred_element_type=jnp.float32).reshape(
        TOK_GRP, local_heads, HD
    )
    key_pre = jnp.dot(normed_full, key_full, preferred_element_type=jnp.float32).reshape(
        TOK_GRP, local_groups, HD
    )
    value_low = (
        jnp.dot(normed_full, value_full, preferred_element_type=jnp.float32)
        .astype(jnp.bfloat16)
        .reshape(TOK_GRP, local_groups, HD)
    )
    query_rot = rotate(query_pre, cosine_table, sine_table).astype(jnp.bfloat16)
    key_rot = rotate(key_pre, cosine_table, sine_table).astype(jnp.bfloat16)
    mixed_blocks = []
    logsum_blocks = []
    for block_index in range(block_count):
        row_start = block_index * QBLK
        key_end = row_start + QBLK
        scores, queries = block_scores(
            query_rot, key_rot, segments, row_start, key_end, local_groups, group_ratio
        )
        top_score = jnp.max(scores, axis=-1, keepdims=True)
        shifted_exp = jnp.exp(scores - top_score)
        total_exp = jnp.sum(shifted_exp, axis=-1, keepdims=True)
        soft_weights = (shifted_exp / total_exp).astype(jnp.bfloat16)
        logsum_blocks.append(top_score + jnp.log(total_exp))
        mixed = jnp.einsum(
            "grqk,kgd->qgrd", soft_weights, value_low[:key_end], preferred_element_type=jnp.float32
        )
        mixed_blocks.append(mixed.astype(jnp.bfloat16).reshape(QBLK, local_heads * HD))
    mixed_full = jnp.concatenate(mixed_blocks, axis=0)
    mixed_full, gate_full, up_full = lax.optimization_barrier((mixed_full, gate_full, up_full))
    mixed_own = lax.all_to_all(mixed_full, "tensor", 0, 1, tiled=True)
    attended = jnp.dot(mixed_own, output_all, preferred_element_type=jnp.float32)
    middle = residual + RESIDUAL_SCALE * attended
    normed_two, unit_two, inverse_two = rms_forward(middle, gain_two)
    mixture_in = lax.all_gather(normed_two.astype(jnp.bfloat16), "tensor", axis=0, tiled=True)
    down_weight, mixture_in = lax.optimization_barrier((down_weight, mixture_in))
    down_full = lax.all_gather(down_weight, "dp", axis=2, tiled=True)
    logits = jnp.dot(mixture_in, router_full, preferred_element_type=jnp.float32)
    routed_marks = (
        expert_ids[:, :, None] == jnp.arange(EXPERTS, dtype=jnp.int32)[None, None, :]
    ).astype(jnp.float32)
    routed = jnp.sum(routed_marks * logits[:, None, :], axis=-1)
    gates = jax.nn.softmax(routed, axis=-1)
    slot_count = local_experts * CAP
    first_slot = lax.axis_index("tensor") * slot_count
    slot_pair = route_slots(expert_ids, fill_order[0], first_slot, slot_count)
    slot_valid = slot_pair >= 0
    safe_pair = jnp.maximum(slot_pair, 0)
    slot_token = safe_pair // TOPK
    slot_choice = safe_pair % TOPK
    side_lanes = 128
    gate_table = jnp.pad(gates, ((0, 0), (0, side_lanes - TOPK)))
    inputs, gate_rows = gather_rows(
        slot_token,
        (mixture_in.astype(jnp.float32), gate_table),
        CAP,
        (jnp.bfloat16, jnp.float32),
    )
    inputs = inputs.reshape(local_experts, CAP, D)
    choice_marks = slot_choice[:, None] == jnp.arange(side_lanes)[None, :]
    slot_gate = jnp.sum(jnp.where(choice_marks, gate_rows, 0.0), axis=1)
    slot_gate = jnp.where(slot_valid, slot_gate, 0.0).reshape(local_experts, CAP, 1)
    gate_pre = jnp.einsum("ecd,edf->ecf", inputs, gate_full, preferred_element_type=jnp.float32)
    up_pre = jnp.einsum("ecd,edf->ecf", inputs, up_full, preferred_element_type=jnp.float32)
    activated = jax.nn.silu(gate_pre)
    hidden_units = (slot_gate * activated * up_pre).astype(jnp.bfloat16)
    expert_out = jnp.einsum(
        "ecf,efd->ecd", hidden_units, down_full, preferred_element_type=jnp.float32
    )
    (mixture_sum,) = combine_rows(slot_token, (expert_out.reshape(slot_count, D),), CAP, TOK_GRP)
    out_grad_held, down_full = lax.optimization_barrier((out_grad, down_full))
    cotangent_full = lax.all_gather(out_grad_held, "tensor", axis=0, tiled=True)
    projection_local, cotangent_full = lax.optimization_barrier(
        (jnp.concatenate([query_weight, key_weight, value_weight], axis=1), cotangent_full)
    )
    projection_all = lax.all_gather(
        lax.all_gather(projection_local, "tensor", axis=1, tiled=True), "dp", axis=0, tiled=True
    )
    scaled_cotangent = (
        (RESIDUAL_SCALE * cotangent_full.astype(jnp.float32)).astype(jnp.bfloat16).astype(jnp.float32)
    )
    scaled_cotangent, mixture_sum = lax.optimization_barrier((scaled_cotangent, mixture_sum))
    mixture_part = lax.psum_scatter(
        mixture_sum.astype(jnp.bfloat16), "tensor", scatter_dimension=0, tiled=True
    ).astype(jnp.float32)
    (out_rows,) = gather_rows(slot_token, (scaled_cotangent,), CAP, (jnp.bfloat16,))
    out_rows = out_rows.reshape(local_experts, CAP, D)
    hidden_grad = jnp.einsum("ecd,efd->ecf", out_rows, down_full, preferred_element_type=jnp.float32)
    gate_grad_slot = jnp.sum(activated * up_pre * hidden_grad, axis=-1).reshape(slot_count)
    gate_grad_rows = jnp.where(
        choice_marks & slot_valid[:, None], gate_grad_slot[:, None], 0.0
    )
    product_grad = slot_gate * hidden_grad
    gate_pre_grad = (product_grad * up_pre * silu_slope(gate_pre)).astype(jnp.bfloat16)
    up_pre_grad = (product_grad * activated).astype(jnp.bfloat16)
    input_rows = jnp.einsum(
        "ecf,edf->ecd", gate_pre_grad, gate_full, preferred_element_type=jnp.float32
    ) + jnp.einsum("ecf,edf->ecd", up_pre_grad, up_full, preferred_element_type=jnp.float32)
    input_rows = input_rows.astype(jnp.bfloat16).reshape(slot_count, D)
    grad_in_mixture, gate_grad_table = combine_rows(
        slot_token, (input_rows, gate_grad_rows), CAP, TOK_GRP
    )
    (inputs, gate_pre_grad, up_pre_grad, hidden_units, out_rows), grad_in_mixture, projection_all = (
        lax.optimization_barrier(
            (
                (inputs, gate_pre_grad, up_pre_grad, hidden_units, out_rows),
                grad_in_mixture,
                projection_all,
            )
        )
    )
    expert_parts = (
        jnp.einsum("ecd,ecf->edf", inputs, gate_pre_grad, preferred_element_type=jnp.float32),
        jnp.einsum("ecd,ecf->edf", inputs, up_pre_grad, preferred_element_type=jnp.float32),
        jnp.einsum("ecd,ecf->edf", out_rows, hidden_units, preferred_element_type=jnp.float32),
    )
    expert_parts = tuple(part.astype(jnp.bfloat16) for part in expert_parts)
    gates_grad = gate_grad_table[:, :TOPK]
    routed_grad = gates * (gates_grad - jnp.sum(gates * gates_grad, axis=-1, keepdims=True))
    logits_grad = jnp.sum(routed_marks * routed_grad[:, :, None], axis=1)
    router_part = jnp.einsum(
        "td,te->de", mixture_in, logits_grad, precision=HIGHEST, preferred_element_type=jnp.float32
    )
    grad_in_mixture = grad_in_mixture + jnp.einsum(
        "te,de->td", logits_grad, router_full.astype(jnp.float32), precision=HIGHEST
    )
    mixture_grad_low, mixture_part = lax.optimization_barrier(
        (grad_in_mixture.astype(jnp.bfloat16), mixture_part)
    )
    block_output = (middle + RESIDUAL_SCALE * mixture_part).astype(jnp.bfloat16)
    mixture_grad_shard = lax.psum_scatter(
        mixture_grad_low, "tensor", scatter_dimension=0, tiled=True
    ).astype(jnp.float32)
    middle_norm_grad, gain_two_grad = rms_backward(
        mixture_grad_shard, unit_two, inverse_two, gain_two
    )
    middle_grad = out_grad.astype(jnp.float32) + middle_norm_grad
    attended_grad = (RESIDUAL_SCALE * middle_grad).astype(jnp.bfloat16)
    mixed_grad_own = jnp.einsum(
        "td,fd->tf", attended_grad, output_all, preferred_element_type=jnp.float32
    ).astype(jnp.bfloat16)
    mixed_grad = lax.all_to_all(mixed_grad_own, "tensor", 1, 0, tiled=True)
    expert_parts, router_part, mixed_grad = lax.optimization_barrier(
        (expert_parts, router_part, mixed_grad)
    )
    expert_grads = reduce_experts(expert_parts)
    router_and_gain = lax.psum_scatter(
        jnp.concatenate([router_part, gain_two_grad[:, None]], axis=1),
        ("dp", "tensor"),
        scatter_dimension=0,
        tiled=True,
    )
    router_weight_grad = router_and_gain[:, : router_part.shape[1]]
    mixture_gain_grad = router_and_gain[:, router_part.shape[1]]
    output_part = jnp.einsum(
        "tf,td->fd", mixed_own, attended_grad, preferred_element_type=jnp.float32
    ).astype(jnp.bfloat16)
    output_part = lax.psum_scatter(output_part, "dp", scatter_dimension=1, tiled=True)
    mixed_grad = mixed_grad.reshape(TOK_GRP, local_groups, group_ratio, HD)
    output_weight_grad = lax.psum_scatter(
        output_part, "tensor", scatter_dimension=0, tiled=True
    ).astype(jnp.float32)
    key_grad = jnp.zeros((TOK_GRP, local_groups, HD), jnp.float32)
    value_grad = jnp.zeros((TOK_GRP, local_groups, HD), jnp.float32)
    query_blocks = []
    for block_index in range(block_count):
        row_start = block_index * QBLK
        key_end = row_start + QBLK
        scores, queries = block_scores(
            query_rot, key_rot, segments, row_start, key_end, local_groups, group_ratio
        )
        soft_full = jnp.exp(scores - logsum_blocks[block_index])
        soft_low = soft_full.astype(jnp.bfloat16)
        out_block = mixed_grad[row_start:key_end]
        weight_grad = jnp.einsum(
            "qgrd,kgd->grqk", out_block, value_low[:key_end], preferred_element_type=jnp.float32
        )
        delta = jnp.sum(soft_full * weight_grad, axis=-1, keepdims=True)
        score_grad = (soft_full * (weight_grad - delta)).astype(jnp.bfloat16)
        query_blocks.append(
            jnp.einsum(
                "grqk,kgd->qgrd", score_grad, key_rot[:key_end], preferred_element_type=jnp.float32
            )
            * ATTN_SCALE
        )
        key_grad = key_grad.at[:key_end].add(
            jnp.einsum("grqk,qgrd->kgd", score_grad, queries, preferred_element_type=jnp.float32)
            * ATTN_SCALE
        )
        value_grad = value_grad.at[:key_end].add(
            jnp.einsum("grqk,qgrd->kgd", soft_low, out_block, preferred_element_type=jnp.float32)
        )
        if block_index == block_count - 2:
            (
                key_grad,
                value_grad,
                expert_grads,
                router_weight_grad,
                output_weight_grad,
                mixture_gain_grad,
            ) = lax.optimization_barrier(
                (
                    key_grad,
                    value_grad,
                    expert_grads,
                    router_weight_grad,
                    output_weight_grad,
                    mixture_gain_grad,
                )
            )
    gate_weight_grad, up_weight_grad, down_weight_grad = expert_grads
    query_rot_grad = jnp.concatenate(query_blocks, axis=0).reshape(TOK_GRP, local_heads, HD)
    query_grad = (
        rotate_back(query_rot_grad, cosine_table, sine_table)
        .astype(jnp.bfloat16)
        .reshape(TOK_GRP, local_heads * HD)
    )
    key_grad_low = (
        rotate_back(key_grad, cosine_table, sine_table)
        .astype(jnp.bfloat16)
        .reshape(TOK_GRP, local_groups * HD)
    )
    value_grad_low = value_grad.astype(jnp.bfloat16).reshape(TOK_GRP, local_groups * HD)
    projection_grad = jnp.concatenate([query_grad, key_grad_low, value_grad_low], axis=1)
    projection_grad_own = lax.all_to_all(projection_grad, "tensor", 0, 1, tiled=True)
    normed_grad = jnp.einsum(
        "tf,df->td", projection_grad_own, projection_all, preferred_element_type=jnp.float32
    )
    query_part = jnp.einsum(
        "td,tf->df", normed_full, query_grad, preferred_element_type=jnp.float32
    )
    key_part = jnp.einsum(
        "td,tf->df", normed_full, key_grad_low, preferred_element_type=jnp.float32
    )
    value_part = jnp.einsum(
        "td,tf->df", normed_full, value_grad_low, preferred_element_type=jnp.float32
    )
    projection_parts = jnp.concatenate(
        [query_part, key_part, value_part], axis=1
    ).astype(jnp.bfloat16)
    projection_parts, normed_grad = lax.optimization_barrier((projection_parts, normed_grad))
    input_norm_grad, gain_one_grad = rms_backward(normed_grad, unit_one, inverse_one, gain_one)
    input_grad = middle_grad + input_norm_grad
    projection_grads = lax.psum_scatter(
        projection_parts, "dp", scatter_dimension=0, tiled=True
    ).astype(jnp.float32)
    query_width, key_width = query_part.shape[1], key_part.shape[1]
    query_weight_grad = projection_grads[:, :query_width]
    key_weight_grad = projection_grads[:, query_width : query_width + key_width]
    value_weight_grad = projection_grads[:, query_width + key_width :]

    attention_gain_grad = lax.psum_scatter(
        gain_one_grad, ("dp", "tensor"), scatter_dimension=0, tiled=True
    )
    return (
        block_output,
        input_grad,
        attention_gain_grad,
        query_weight_grad,
        key_weight_grad,
        value_weight_grad,
        output_weight_grad,
        mixture_gain_grad,
        router_weight_grad,
        gate_weight_grad,
        up_weight_grad,
        down_weight_grad,
    )


def solution(mesh):
    in_specs = (
        P(("dp", "tensor"), None),
        P(("dp", "tensor"), None),
        P("dp", None),
        P("dp", None),
        P("dp", None),
        P("dp"),
        P("dp", "tensor"),
        P("dp", "tensor"),
        P("dp", "tensor"),
        P("tensor", "dp"),
        P("dp"),
        P("dp", None),
        P("tensor", "dp", None),
        P("tensor", "dp", None),
        P("tensor", None, "dp"),
    )
    out_specs = (
        P(("dp", "tensor"), None),
        P(("dp", "tensor"), None),
        P(("dp", "tensor")),
        P("dp", "tensor"),
        P("dp", "tensor"),
        P("dp", "tensor"),
        P("tensor", "dp"),
        P(("dp", "tensor")),
        P(("dp", "tensor"), None),
        P("tensor", "dp", None),
        P("tensor", "dp", None),
        P("tensor", None, "dp"),
    )
    return jax.shard_map(local, mesh=mesh, in_specs=in_specs, out_specs=out_specs, check_vma=False)
```

```python
import jax
import jax.numpy as jnp
from jax import lax
from jax.experimental import pallas as pl
from jax.experimental.pallas import tpu as pltpu
from jax.sharding import PartitionSpec as P

D = 1536
HD = 64
EXPERTS = 40
TOPK = 8
PROMPT = 2048
NCONT = 4
QBLK = 512
TOK_GRP = 3072
CAP = 768


ATTN_SCALE = 0.015625
RESIDUAL_SCALE = 0.22
NORM_EPS = 1e-06
ROPE_BASE = 10000.0
MASKED = -1e30
HIGHEST = lax.Precision.HIGHEST


def rms_forward(values, gain_row):
    inverse_rms = lax.rsqrt(jnp.mean(values * values, axis=-1, keepdims=True) + NORM_EPS)
    unit_rows = values * inverse_rms
    return (unit_rows * gain_row, unit_rows, inverse_rms)


def rms_backward(gradient, unit_rows, inverse_rms, gain_row):
    gain_grad = jnp.sum(gradient * unit_rows, axis=0)
    scaled = gradient * gain_row
    mean_term = jnp.mean(scaled * unit_rows, axis=-1, keepdims=True)
    return (inverse_rms * (scaled - unit_rows * mean_term), gain_grad)


def group_layout(segment_row, prompt_length):
    cont_length = segment_row.shape[0]
    segment_marks = (segment_row[:, None] == jnp.arange(NCONT, dtype=jnp.int32)[None, :]).astype(
        jnp.int32
    )
    segment_sizes = jnp.sum(segment_marks, axis=0)
    segment_starts = jnp.cumsum(segment_sizes) - segment_sizes
    token_starts = jnp.sum(segment_marks * segment_starts[None, :], axis=1)
    inside = jnp.arange(cont_length, dtype=jnp.int32) - token_starts
    positions = jnp.concatenate(
        [jnp.arange(prompt_length, dtype=jnp.int32), prompt_length + inside]
    )
    segments = jnp.concatenate([jnp.zeros((prompt_length,), jnp.int32), segment_row + 1])
    return (positions, segments)


def allowed(query_index, query_segment, key_index, key_segment):
    causal = key_index[None, :] <= query_index[:, None]
    shared = (key_segment[None, :] == 0) | (key_segment[None, :] == query_segment[:, None])
    return causal & shared


def rope_tables(positions, head_size):
    halfway = head_size // 2
    frequency = ROPE_BASE ** (-(2.0 * jnp.arange(halfway, dtype=jnp.float32)) / head_size)
    angles = positions.astype(jnp.float32)[:, None] * frequency[None, :]
    return (jnp.cos(angles), jnp.sin(angles))


def rotate(values, cosine_table, sine_table):
    halfway = values.shape[-1] // 2
    first_half = values[..., :halfway]
    second_half = values[..., halfway:]
    cosine_part = cosine_table[:, None, :]
    sine_part = sine_table[:, None, :]
    return jnp.concatenate(
        [
            first_half * cosine_part - second_half * sine_part,
            second_half * cosine_part + first_half * sine_part,
        ],
        axis=-1,
    )


def rotate_back(gradient, cosine_table, sine_table):
    halfway = gradient.shape[-1] // 2
    first_half = gradient[..., :halfway]
    second_half = gradient[..., halfway:]
    cosine_part = cosine_table[:, None, :]
    sine_part = sine_table[:, None, :]
    return jnp.concatenate(
        [
            first_half * cosine_part + second_half * sine_part,
            second_half * cosine_part - first_half * sine_part,
        ],
        axis=-1,
    )


def silu_slope(values):
    sigmoid_part = jax.nn.sigmoid(values)
    return sigmoid_part * (1.0 + values * (1.0 - sigmoid_part))


def route_slots(expert_row, order_row, first_slot, slot_count):
    pair_count = expert_row.shape[0] * expert_row.shape[1]
    ordered = table_lookup(expert_row.reshape(pair_count), order_row)
    onehot = ordered[:, None] == jnp.arange(EXPERTS, dtype=jnp.int32)[None, :]
    rank_block = 256
    blocks = pair_count // rank_block
    pair_marks = onehot.astype(jnp.bfloat16).reshape(blocks, rank_block, EXPERTS)
    lower_ones = (jnp.arange(rank_block)[:, None] >= jnp.arange(rank_block)[None, :]).astype(
        jnp.bfloat16
    )
    within = jnp.einsum(
        "ij,bje->bie", lower_ones, pair_marks, preferred_element_type=jnp.float32
    ).astype(jnp.int32)
    totals = within[:, -1, :]
    before = jnp.cumsum(totals, axis=0) - totals
    counts = (within + before[:, None, :]).reshape(pair_count, EXPERTS)
    pair_rank = jnp.sum(jnp.where(onehot, counts, 0), axis=1) - 1
    local_slot = ordered * CAP + pair_rank - first_slot
    kept = (pair_rank < CAP) & (local_slot >= 0) & (local_slot < slot_count)
    local_slot = jnp.where(kept, local_slot, -1)
    return invert_slots(local_slot, order_row, slot_count)


def _gather_rows_kernel(tok_ref, *refs):
    count = (len(refs) - 1) // 4
    sources, outs = refs[:count], refs[count : 2 * count]
    copies, rows_bufs, sem = refs[2 * count : 3 * count], refs[3 * count : 4 * count], refs[-1]
    rows = rows_bufs[0].shape[0]
    step = pl.program_id(0)

    @pl.when(step == 0)
    def _():
        for source, copy in zip(sources, copies):
            transfer = pltpu.make_async_copy(source, copy, sem)
            transfer.start()
            transfer.wait()

    base = step * rows

    def body(s, carry):
        t = tok_ref[base + s]
        for copy, rows_buf in zip(copies, rows_bufs):
            rows_buf[pl.ds(s, 1), :] = copy[pl.ds(t, 1), :]
        return carry

    lax.fori_loop(0, rows, body, 0, unroll=8)
    for out, rows_buf in zip(outs, rows_bufs):
        out[...] = rows_buf[...].astype(out.dtype)


def gather_rows(tok, sources, rows, out_dtypes):
    blocks = tok.shape[0] // rows
    return pl.pallas_call(
        _gather_rows_kernel,
        grid_spec=pltpu.PrefetchScalarGridSpec(
            num_scalar_prefetch=1,
            grid=(blocks,),
            in_specs=[pl.BlockSpec(memory_space=pl.ANY) for _ in sources],
            out_specs=[
                pl.BlockSpec((rows, source.shape[1]), lambda b, tok: (b, 0)) for source in sources
            ],
            scratch_shapes=[pltpu.VMEM(source.shape, jnp.float32) for source in sources]
            + [pltpu.VMEM((rows, source.shape[1]), jnp.float32) for source in sources]
            + [pltpu.SemaphoreType.DMA(())],
        ),
        out_shape=[
            jax.ShapeDtypeStruct((tok.shape[0], source.shape[1]), dtype)
            for source, dtype in zip(sources, out_dtypes)
        ],
        compiler_params=pltpu.CompilerParams(vmem_limit_bytes=56 * 1024 * 1024),
    )(tok, *sources)


def _combine_rows_kernel(tok_ref, *refs):
    count = (len(refs) - 1) // 4
    addends, outs = refs[:count], refs[count : 2 * count]
    totals, rows_bufs, sem = refs[2 * count : 3 * count], refs[3 * count : 4 * count], refs[-1]
    rows = rows_bufs[0].shape[0]
    step = pl.program_id(0)

    @pl.when(step == 0)
    def _():
        for total in totals:
            total[...] = jnp.zeros_like(total)

    for addend, rows_buf in zip(addends, rows_bufs):
        rows_buf[...] = addend[...].astype(jnp.float32)
    base = step * rows

    def body(s, carry):
        t = tok_ref[base + s]
        for total, rows_buf in zip(totals, rows_bufs):
            total[pl.ds(t, 1), :] += rows_buf[pl.ds(s, 1), :]
        return carry

    lax.fori_loop(0, rows, body, 0, unroll=8)

    @pl.when(step == pl.num_programs(0) - 1)
    def _():
        for total, out in zip(totals, outs):
            transfer = pltpu.make_async_copy(total, out, sem)
            transfer.start()
            transfer.wait()


def combine_rows(tok, addends, rows, total_rows):
    blocks = tok.shape[0] // rows
    return pl.pallas_call(
        _combine_rows_kernel,
        grid_spec=pltpu.PrefetchScalarGridSpec(
            num_scalar_prefetch=1,
            grid=(blocks,),
            in_specs=[
                pl.BlockSpec((rows, addend.shape[1]), lambda b, tok: (b, 0)) for addend in addends
            ],
            out_specs=[pl.BlockSpec(memory_space=pl.ANY) for _ in addends],
            scratch_shapes=[
                pltpu.VMEM((total_rows, addend.shape[1]), jnp.float32) for addend in addends
            ]
            + [pltpu.VMEM((rows, addend.shape[1]), jnp.float32) for addend in addends]
            + [pltpu.SemaphoreType.DMA(())],
        ),
        out_shape=[
            jax.ShapeDtypeStruct((total_rows, addend.shape[1]), jnp.float32) for addend in addends
        ],
        compiler_params=pltpu.CompilerParams(vmem_limit_bytes=56 * 1024 * 1024),
    )(tok, *addends)


def table_lookup(table, index):
    lanes = 128
    high_count = table.shape[0] // lanes
    low_marks = (index[:, None] % lanes == jnp.arange(lanes)[None, :]).astype(jnp.bfloat16)
    picked = jnp.dot(
        low_marks,
        table.reshape(high_count, lanes).astype(jnp.bfloat16).T,
        preferred_element_type=jnp.float32,
    )
    high_marks = index[:, None] // lanes == jnp.arange(high_count)[None, :]
    return jnp.sum(jnp.where(high_marks, picked, 0.0), axis=1).astype(jnp.int32)


def invert_slots(local_slot, values, slot_count):
    lanes = 128
    high_count = slot_count // lanes
    column_marks = (local_slot[:, None] // lanes == jnp.arange(high_count)[None, :]).astype(
        jnp.bfloat16
    )
    lane_marks = local_slot[:, None] % lanes == jnp.arange(lanes)[None, :]
    shifted = values + 1
    parts = []
    for digit in (shifted // 256, shifted % 256):
        spread = jnp.where(lane_marks, digit[:, None], 0).astype(jnp.bfloat16)
        parts.append(
            jnp.einsum("ic,il->cl", column_marks, spread, preferred_element_type=jnp.float32)
        )
    return (256.0 * parts[0] + parts[1]).astype(jnp.int32).reshape(slot_count) - 1


def block_scores(query_rot, key_rot, segments, row_start, key_end, local_groups, group_ratio):
    queries = query_rot[row_start:key_end].reshape(
        key_end - row_start, local_groups, group_ratio, HD
    )
    raw_scores = (
        jnp.einsum("qgrd,kgd->grqk", queries, key_rot[:key_end], preferred_element_type=jnp.float32)
        * ATTN_SCALE
    )
    visible = allowed(
        jnp.arange(row_start, key_end, dtype=jnp.int32),
        segments[row_start:key_end],
        jnp.arange(key_end, dtype=jnp.int32),
        segments[:key_end],
    )
    return (jnp.where(visible[None, None], raw_scores, MASKED), queries)


def fetch_experts(gate_weight, up_weight, down_weight):
    return (
        lax.all_gather(gate_weight, "dp", axis=1, tiled=True),
        lax.all_gather(up_weight, "dp", axis=1, tiled=True),
        lax.all_gather(down_weight, "dp", axis=2, tiled=True),
    )


def reduce_experts(grads):
    return (
        lax.psum_scatter(grads[0], "dp", scatter_dimension=1, tiled=True).astype(jnp.float32),
        lax.psum_scatter(grads[1], "dp", scatter_dimension=1, tiled=True).astype(jnp.float32),
        jnp.swapaxes(
            lax.psum_scatter(grads[2], "dp", scatter_dimension=1, tiled=True).astype(jnp.float32),
            1,
            2,
        ),
    )


def local(
    hidden_in,
    out_grad,
    segment_ids,
    expert_ids,
    fill_order,
    attention_gain,
    query_weight,
    key_weight,
    value_weight,
    output_weight,
    mixture_gain,
    router_weight,
    gate_weight,
    up_weight,
    down_weight,
):
    local_heads = query_weight.shape[1] // HD
    local_groups = key_weight.shape[1] // HD
    group_ratio = local_heads // local_groups
    block_count = TOK_GRP // QBLK
    local_experts = gate_weight.shape[0]
    gain_one, query_full, key_full, value_full, gain_two, router_full = (
        lax.all_gather(attention_gain, "dp", axis=0, tiled=True),
        lax.all_gather(query_weight, "dp", axis=0, tiled=True),
        lax.all_gather(key_weight, "dp", axis=0, tiled=True),
        lax.all_gather(value_weight, "dp", axis=0, tiled=True),
        lax.all_gather(mixture_gain, "dp", axis=0, tiled=True),
        lax.all_gather(router_weight, "dp", axis=0, tiled=True),
    )
    output_all = lax.all_gather(
        lax.all_gather(output_weight, "tensor", axis=0, tiled=True), "dp", axis=1, tiled=True
    )
    gain_one = gain_one.astype(jnp.float32)
    gain_two = gain_two.astype(jnp.float32)
    residual = hidden_in.astype(jnp.float32)
    normed_shard, unit_one, inverse_one = rms_forward(residual, gain_one)
    normed_full = lax.all_gather(normed_shard.astype(jnp.bfloat16), "tensor", axis=0, tiled=True)
    gate_weight, up_weight, normed_full = lax.optimization_barrier(
        (gate_weight, up_weight, normed_full)
    )
    gate_full = lax.all_gather(gate_weight, "dp", axis=1, tiled=True)
    up_full = lax.all_gather(up_weight, "dp", axis=1, tiled=True)
    positions, segments = group_layout(segment_ids[0], PROMPT)
    cosine_table, sine_table = rope_tables(positions, HD)
    query_pre = jnp.dot(normed_full, query_full, preferred_element_type=jnp.float32).reshape(
        TOK_GRP, local_heads, HD
    )
    key_pre = jnp.dot(normed_full, key_full, preferred_element_type=jnp.float32).reshape(
        TOK_GRP, local_groups, HD
    )
    value_low = (
        jnp.dot(normed_full, value_full, preferred_element_type=jnp.float32)
        .astype(jnp.bfloat16)
        .reshape(TOK_GRP, local_groups, HD)
    )
    query_rot = rotate(query_pre, cosine_table, sine_table).astype(jnp.bfloat16)
    key_rot = rotate(key_pre, cosine_table, sine_table).astype(jnp.bfloat16)
    mixed_blocks = []
    logsum_blocks = []
    for block_index in range(block_count):
        row_start = block_index * QBLK
        key_end = row_start + QBLK
        scores, queries = block_scores(
            query_rot, key_rot, segments, row_start, key_end, local_groups, group_ratio
        )
        top_score = jnp.max(scores, axis=-1, keepdims=True)
        shifted_exp = jnp.exp(scores - top_score)
        total_exp = jnp.sum(shifted_exp, axis=-1, keepdims=True)
        soft_weights = (shifted_exp / total_exp).astype(jnp.bfloat16)
        logsum_blocks.append(top_score + jnp.log(total_exp))
        mixed = jnp.einsum(
            "grqk,kgd->qgrd", soft_weights, value_low[:key_end], preferred_element_type=jnp.float32
        )
        mixed_blocks.append(mixed.astype(jnp.bfloat16).reshape(QBLK, local_heads * HD))
    mixed_full = jnp.concatenate(mixed_blocks, axis=0)
    mixed_full, gate_full, up_full = lax.optimization_barrier((mixed_full, gate_full, up_full))
    mixed_own = lax.all_to_all(mixed_full, "tensor", 0, 1, tiled=True)
    attended = jnp.dot(mixed_own, output_all, preferred_element_type=jnp.float32)
    middle = residual + RESIDUAL_SCALE * attended
    normed_two, unit_two, inverse_two = rms_forward(middle, gain_two)
    mixture_in = lax.all_gather(normed_two.astype(jnp.bfloat16), "tensor", axis=0, tiled=True)
    down_weight, mixture_in = lax.optimization_barrier((down_weight, mixture_in))
    down_full = lax.all_gather(down_weight, "dp", axis=2, tiled=True)
    logits = jnp.dot(mixture_in, router_full, preferred_element_type=jnp.float32)
    routed_marks = (
        expert_ids[:, :, None] == jnp.arange(EXPERTS, dtype=jnp.int32)[None, None, :]
    ).astype(jnp.float32)
    routed = jnp.sum(routed_marks * logits[:, None, :], axis=-1)
    gates = jax.nn.softmax(routed, axis=-1)
    slot_count = local_experts * CAP
    first_slot = lax.axis_index("tensor") * slot_count
    slot_pair = route_slots(expert_ids, fill_order[0], first_slot, slot_count)
    slot_valid = slot_pair >= 0
    safe_pair = jnp.maximum(slot_pair, 0)
    slot_token = safe_pair // TOPK
    slot_choice = safe_pair % TOPK
    side_lanes = 128
    gate_table = jnp.pad(gates, ((0, 0), (0, side_lanes - TOPK)))
    inputs, gate_rows = gather_rows(
        slot_token,
        (mixture_in.astype(jnp.float32), gate_table),
        CAP,
        (jnp.bfloat16, jnp.float32),
    )
    inputs = inputs.reshape(local_experts, CAP, D)
    choice_marks = slot_choice[:, None] == jnp.arange(side_lanes)[None, :]
    slot_gate = jnp.sum(jnp.where(choice_marks, gate_rows, 0.0), axis=1)
    slot_gate = jnp.where(slot_valid, slot_gate, 0.0).reshape(local_experts, CAP, 1)
    gate_pre = jnp.einsum("ecd,edf->ecf", inputs, gate_full, preferred_element_type=jnp.float32)
    up_pre = jnp.einsum("ecd,edf->ecf", inputs, up_full, preferred_element_type=jnp.float32)
    activated = jax.nn.silu(gate_pre)
    hidden_units = (slot_gate * activated * up_pre).astype(jnp.bfloat16)
    expert_out = jnp.einsum(
        "ecf,efd->ecd", hidden_units, down_full, preferred_element_type=jnp.float32
    )
    (mixture_sum,) = combine_rows(slot_token, (expert_out.reshape(slot_count, D),), CAP, TOK_GRP)
    out_grad_held, down_full = lax.optimization_barrier((out_grad, down_full))
    cotangent_full = lax.all_gather(out_grad_held, "tensor", axis=0, tiled=True)
    scaled_cotangent = (
        (RESIDUAL_SCALE * cotangent_full.astype(jnp.float32)).astype(jnp.bfloat16).astype(jnp.float32)
    )
    scaled_cotangent, mixture_sum, projection_local = lax.optimization_barrier(
        (
            scaled_cotangent,
            mixture_sum,
            jnp.concatenate([query_weight, key_weight, value_weight], axis=1),
        )
    )
    projection_all = lax.all_gather(
        lax.all_gather(projection_local, "tensor", axis=1, tiled=True), "dp", axis=0, tiled=True
    )
    mixture_part = lax.psum_scatter(
        mixture_sum.astype(jnp.bfloat16), "tensor", scatter_dimension=0, tiled=True
    ).astype(jnp.float32)
    (out_rows,) = gather_rows(slot_token, (scaled_cotangent,), CAP, (jnp.bfloat16,))
    out_rows = out_rows.reshape(local_experts, CAP, D)
    hidden_grad = jnp.einsum("ecd,efd->ecf", out_rows, down_full, preferred_element_type=jnp.float32)
    gate_grad_slot = jnp.sum(activated * up_pre * hidden_grad, axis=-1).reshape(slot_count)
    gate_grad_rows = jnp.where(
        choice_marks & slot_valid[:, None], gate_grad_slot[:, None], 0.0
    )
    product_grad = slot_gate * hidden_grad
    gate_pre_grad = (product_grad * up_pre * silu_slope(gate_pre)).astype(jnp.bfloat16)
    up_pre_grad = (product_grad * activated).astype(jnp.bfloat16)
    input_rows = jnp.einsum(
        "ecf,edf->ecd", gate_pre_grad, gate_full, preferred_element_type=jnp.float32
    ) + jnp.einsum("ecf,edf->ecd", up_pre_grad, up_full, preferred_element_type=jnp.float32)
    input_rows = input_rows.astype(jnp.bfloat16).reshape(slot_count, D)
    grad_in_mixture, gate_grad_table = combine_rows(
        slot_token, (input_rows, gate_grad_rows), CAP, TOK_GRP
    )
    (inputs, gate_pre_grad, up_pre_grad, hidden_units, out_rows), grad_in_mixture, projection_all = (
        lax.optimization_barrier(
            (
                (inputs, gate_pre_grad, up_pre_grad, hidden_units, out_rows),
                grad_in_mixture,
                projection_all,
            )
        )
    )
    expert_parts = (
        jnp.einsum("ecd,ecf->edf", inputs, gate_pre_grad, preferred_element_type=jnp.float32),
        jnp.einsum("ecd,ecf->edf", inputs, up_pre_grad, preferred_element_type=jnp.float32),
        jnp.einsum("ecd,ecf->edf", out_rows, hidden_units, preferred_element_type=jnp.float32),
    )
    expert_parts = tuple(part.astype(jnp.bfloat16) for part in expert_parts)
    gates_grad = gate_grad_table[:, :TOPK]
    routed_grad = gates * (gates_grad - jnp.sum(gates * gates_grad, axis=-1, keepdims=True))
    logits_grad = jnp.sum(routed_marks * routed_grad[:, :, None], axis=1)
    router_part = jnp.einsum(
        "td,te->de", mixture_in, logits_grad, precision=HIGHEST, preferred_element_type=jnp.float32
    )
    grad_in_mixture = grad_in_mixture + jnp.einsum(
        "te,de->td", logits_grad, router_full.astype(jnp.float32), precision=HIGHEST
    )
    mixture_grad_low, mixture_part = lax.optimization_barrier(
        (grad_in_mixture.astype(jnp.bfloat16), mixture_part)
    )
    block_output = (middle + RESIDUAL_SCALE * mixture_part).astype(jnp.bfloat16)
    mixture_grad_shard = lax.psum_scatter(
        mixture_grad_low, "tensor", scatter_dimension=0, tiled=True
    ).astype(jnp.float32)
    middle_norm_grad, gain_two_grad = rms_backward(
        mixture_grad_shard, unit_two, inverse_two, gain_two
    )
    middle_grad = out_grad.astype(jnp.float32) + middle_norm_grad
    attended_grad = (RESIDUAL_SCALE * middle_grad).astype(jnp.bfloat16)
    mixed_grad_own = jnp.einsum(
        "td,fd->tf", attended_grad, output_all, preferred_element_type=jnp.float32
    ).astype(jnp.bfloat16)
    mixed_grad = lax.all_to_all(mixed_grad_own, "tensor", 1, 0, tiled=True)
    expert_parts, router_part, mixed_grad = lax.optimization_barrier(
        (expert_parts, router_part, mixed_grad)
    )
    expert_grads = reduce_experts(expert_parts)
    router_and_gain = lax.psum_scatter(
        jnp.concatenate([router_part, gain_two_grad[:, None]], axis=1),
        ("dp", "tensor"),
        scatter_dimension=0,
        tiled=True,
    )
    router_weight_grad = router_and_gain[:, : router_part.shape[1]]
    mixture_gain_grad = router_and_gain[:, router_part.shape[1]]
    output_part = jnp.einsum(
        "tf,td->fd", mixed_own, attended_grad, preferred_element_type=jnp.float32
    ).astype(jnp.bfloat16)
    output_part = lax.psum_scatter(output_part, "dp", scatter_dimension=1, tiled=True)
    mixed_grad = mixed_grad.reshape(TOK_GRP, local_groups, group_ratio, HD)
    output_weight_grad = lax.psum_scatter(
        output_part, "tensor", scatter_dimension=0, tiled=True
    ).astype(jnp.float32)
    key_grad = jnp.zeros((TOK_GRP, local_groups, HD), jnp.float32)
    value_grad = jnp.zeros((TOK_GRP, local_groups, HD), jnp.float32)
    query_blocks = []
    for block_index in range(block_count):
        row_start = block_index * QBLK
        key_end = row_start + QBLK
        scores, queries = block_scores(
            query_rot, key_rot, segments, row_start, key_end, local_groups, group_ratio
        )
        soft_full = jnp.exp(scores - logsum_blocks[block_index])
        soft_low = soft_full.astype(jnp.bfloat16)
        out_block = mixed_grad[row_start:key_end]
        weight_grad = jnp.einsum(
            "qgrd,kgd->grqk", out_block, value_low[:key_end], preferred_element_type=jnp.float32
        )
        delta = jnp.sum(soft_full * weight_grad, axis=-1, keepdims=True)
        score_grad = (soft_full * (weight_grad - delta)).astype(jnp.bfloat16)
        query_blocks.append(
            jnp.einsum(
                "grqk,kgd->qgrd", score_grad, key_rot[:key_end], preferred_element_type=jnp.float32
            )
            * ATTN_SCALE
        )
        key_grad = key_grad.at[:key_end].add(
            jnp.einsum("grqk,qgrd->kgd", score_grad, queries, preferred_element_type=jnp.float32)
            * ATTN_SCALE
        )
        value_grad = value_grad.at[:key_end].add(
            jnp.einsum("grqk,qgrd->kgd", soft_low, out_block, preferred_element_type=jnp.float32)
        )
        if block_index == block_count - 1:
            (
                key_grad,
                value_grad,
                expert_grads,
                router_weight_grad,
                output_weight_grad,
                mixture_gain_grad,
            ) = lax.optimization_barrier(
                (
                    key_grad,
                    value_grad,
                    expert_grads,
                    router_weight_grad,
                    output_weight_grad,
                    mixture_gain_grad,
                )
            )
    gate_weight_grad, up_weight_grad, down_weight_grad = expert_grads
    query_rot_grad = jnp.concatenate(query_blocks, axis=0).reshape(TOK_GRP, local_heads, HD)
    query_grad = (
        rotate_back(query_rot_grad, cosine_table, sine_table)
        .astype(jnp.bfloat16)
        .reshape(TOK_GRP, local_heads * HD)
    )
    key_grad_low = (
        rotate_back(key_grad, cosine_table, sine_table)
        .astype(jnp.bfloat16)
        .reshape(TOK_GRP, local_groups * HD)
    )
    value_grad_low = value_grad.astype(jnp.bfloat16).reshape(TOK_GRP, local_groups * HD)
    projection_grad = jnp.concatenate([query_grad, key_grad_low, value_grad_low], axis=1)
    projection_grad_own = lax.all_to_all(projection_grad, "tensor", 0, 1, tiled=True)
    normed_grad = jnp.einsum(
        "tf,df->td", projection_grad_own, projection_all, preferred_element_type=jnp.float32
    )
    query_part = jnp.einsum(
        "td,tf->df", normed_full, query_grad, preferred_element_type=jnp.float32
    )
    key_part = jnp.einsum(
        "td,tf->df", normed_full, key_grad_low, preferred_element_type=jnp.float32
    )
    value_part = jnp.einsum(
        "td,tf->df", normed_full, value_grad_low, preferred_element_type=jnp.float32
    )
    projection_parts = jnp.concatenate(
        [query_part, key_part, value_part], axis=1
    ).astype(jnp.bfloat16)
    projection_parts, normed_grad = lax.optimization_barrier((projection_parts, normed_grad))
    input_norm_grad, gain_one_grad = rms_backward(normed_grad, unit_one, inverse_one, gain_one)
    input_grad = middle_grad + input_norm_grad
    projection_grads = lax.psum_scatter(
        projection_parts, "dp", scatter_dimension=0, tiled=True
    ).astype(jnp.float32)
    query_width, key_width = query_part.shape[1], key_part.shape[1]
    query_weight_grad = projection_grads[:, :query_width]
    key_weight_grad = projection_grads[:, query_width : query_width + key_width]
    value_weight_grad = projection_grads[:, query_width + key_width :]

    attention_gain_grad = lax.psum_scatter(
        gain_one_grad, ("dp", "tensor"), scatter_dimension=0, tiled=True
    )
    return (
        block_output,
        input_grad,
        attention_gain_grad,
        query_weight_grad,
        key_weight_grad,
        value_weight_grad,
        output_weight_grad,
        mixture_gain_grad,
        router_weight_grad,
        gate_weight_grad,
        up_weight_grad,
        down_weight_grad,
    )


def solution(mesh):
    in_specs = (
        P(("dp", "tensor"), None),
        P(("dp", "tensor"), None),
        P("dp", None),
        P("dp", None),
        P("dp", None),
        P("dp"),
        P("dp", "tensor"),
        P("dp", "tensor"),
        P("dp", "tensor"),
        P("tensor", "dp"),
        P("dp"),
        P("dp", None),
        P("tensor", "dp", None),
        P("tensor", "dp", None),
        P("tensor", None, "dp"),
    )
    out_specs = (
        P(("dp", "tensor"), None),
        P(("dp", "tensor"), None),
        P(("dp", "tensor")),
        P("dp", "tensor"),
        P("dp", "tensor"),
        P("dp", "tensor"),
        P("tensor", "dp"),
        P(("dp", "tensor")),
        P(("dp", "tensor"), None),
        P("tensor", "dp", None),
        P("tensor", "dp", None),
        P("tensor", None, "dp"),
    )
    return jax.shard_map(local, mesh=mesh, in_specs=in_specs, out_specs=out_specs, check_vma=False)
```

```python
import jax
import jax.numpy as jnp
from jax import lax
from jax.experimental import pallas as pl
from jax.experimental.pallas import tpu as pltpu
from jax.sharding import PartitionSpec as P

D = 1536
HD = 64
EXPERTS = 40
TOPK = 8
PROMPT = 2048
NCONT = 4
QBLK = 512
TOK_GRP = 3072
CAP = 768


ATTN_SCALE = 0.015625
RESIDUAL_SCALE = 0.22
NORM_EPS = 1e-06
ROPE_BASE = 10000.0
MASKED = -1e30
HIGHEST = lax.Precision.HIGHEST


def rms_forward(values, gain_row):
    inverse_rms = lax.rsqrt(jnp.mean(values * values, axis=-1, keepdims=True) + NORM_EPS)
    unit_rows = values * inverse_rms
    return (unit_rows * gain_row, unit_rows, inverse_rms)


def rms_backward(gradient, unit_rows, inverse_rms, gain_row):
    gain_grad = jnp.sum(gradient * unit_rows, axis=0)
    scaled = gradient * gain_row
    mean_term = jnp.mean(scaled * unit_rows, axis=-1, keepdims=True)
    return (inverse_rms * (scaled - unit_rows * mean_term), gain_grad)


def group_layout(segment_row, prompt_length):
    cont_length = segment_row.shape[0]
    segment_marks = (segment_row[:, None] == jnp.arange(NCONT, dtype=jnp.int32)[None, :]).astype(
        jnp.int32
    )
    segment_sizes = jnp.sum(segment_marks, axis=0)
    segment_starts = jnp.cumsum(segment_sizes) - segment_sizes
    token_starts = jnp.sum(segment_marks * segment_starts[None, :], axis=1)
    inside = jnp.arange(cont_length, dtype=jnp.int32) - token_starts
    positions = jnp.concatenate(
        [jnp.arange(prompt_length, dtype=jnp.int32), prompt_length + inside]
    )
    segments = jnp.concatenate([jnp.zeros((prompt_length,), jnp.int32), segment_row + 1])
    return (positions, segments)


def allowed(query_index, query_segment, key_index, key_segment):
    causal = key_index[None, :] <= query_index[:, None]
    shared = (key_segment[None, :] == 0) | (key_segment[None, :] == query_segment[:, None])
    return causal & shared


def rope_tables(positions, head_size):
    halfway = head_size // 2
    frequency = ROPE_BASE ** (-(2.0 * jnp.arange(halfway, dtype=jnp.float32)) / head_size)
    angles = positions.astype(jnp.float32)[:, None] * frequency[None, :]
    return (jnp.cos(angles), jnp.sin(angles))


def rotate(values, cosine_table, sine_table):
    halfway = values.shape[-1] // 2
    first_half = values[..., :halfway]
    second_half = values[..., halfway:]
    cosine_part = cosine_table[:, None, :]
    sine_part = sine_table[:, None, :]
    return jnp.concatenate(
        [
            first_half * cosine_part - second_half * sine_part,
            second_half * cosine_part + first_half * sine_part,
        ],
        axis=-1,
    )


def rotate_back(gradient, cosine_table, sine_table):
    halfway = gradient.shape[-1] // 2
    first_half = gradient[..., :halfway]
    second_half = gradient[..., halfway:]
    cosine_part = cosine_table[:, None, :]
    sine_part = sine_table[:, None, :]
    return jnp.concatenate(
        [
            first_half * cosine_part + second_half * sine_part,
            second_half * cosine_part - first_half * sine_part,
        ],
        axis=-1,
    )


def silu_slope(values):
    sigmoid_part = jax.nn.sigmoid(values)
    return sigmoid_part * (1.0 + values * (1.0 - sigmoid_part))


def route_slots(expert_row, order_row, first_slot, slot_count):
    pair_count = expert_row.shape[0] * expert_row.shape[1]
    ordered = table_lookup(expert_row.reshape(pair_count), order_row)
    onehot = ordered[:, None] == jnp.arange(EXPERTS, dtype=jnp.int32)[None, :]
    rank_block = 256
    blocks = pair_count // rank_block
    pair_marks = onehot.astype(jnp.bfloat16).reshape(blocks, rank_block, EXPERTS)
    lower_ones = (jnp.arange(rank_block)[:, None] >= jnp.arange(rank_block)[None, :]).astype(
        jnp.bfloat16
    )
    within = jnp.einsum(
        "ij,bje->bie", lower_ones, pair_marks, preferred_element_type=jnp.float32
    ).astype(jnp.int32)
    totals = within[:, -1, :]
    before = jnp.cumsum(totals, axis=0) - totals
    counts = (within + before[:, None, :]).reshape(pair_count, EXPERTS)
    pair_rank = jnp.sum(jnp.where(onehot, counts, 0), axis=1) - 1
    local_slot = ordered * CAP + pair_rank - first_slot
    kept = (pair_rank < CAP) & (local_slot >= 0) & (local_slot < slot_count)
    local_slot = jnp.where(kept, local_slot, -1)
    return invert_slots(local_slot, order_row, slot_count)


def _gather_rows_kernel(tok_ref, *refs):
    count = (len(refs) - 1) // 4
    sources, outs = refs[:count], refs[count : 2 * count]
    copies, rows_bufs, sem = refs[2 * count : 3 * count], refs[3 * count : 4 * count], refs[-1]
    rows = rows_bufs[0].shape[0]
    step = pl.program_id(0)

    @pl.when(step == 0)
    def _():
        for source, copy in zip(sources, copies):
            transfer = pltpu.make_async_copy(source, copy, sem)
            transfer.start()
            transfer.wait()

    base = step * rows

    def body(s, carry):
        t = tok_ref[base + s]
        for copy, rows_buf in zip(copies, rows_bufs):
            rows_buf[pl.ds(s, 1), :] = copy[pl.ds(t, 1), :]
        return carry

    lax.fori_loop(0, rows, body, 0, unroll=8)
    for out, rows_buf in zip(outs, rows_bufs):
        out[...] = rows_buf[...].astype(out.dtype)


def gather_rows(tok, sources, rows, out_dtypes):
    blocks = tok.shape[0] // rows
    return pl.pallas_call(
        _gather_rows_kernel,
        grid_spec=pltpu.PrefetchScalarGridSpec(
            num_scalar_prefetch=1,
            grid=(blocks,),
            in_specs=[pl.BlockSpec(memory_space=pl.ANY) for _ in sources],
            out_specs=[
                pl.BlockSpec((rows, source.shape[1]), lambda b, tok: (b, 0)) for source in sources
            ],
            scratch_shapes=[pltpu.VMEM(source.shape, jnp.float32) for source in sources]
            + [pltpu.VMEM((rows, source.shape[1]), jnp.float32) for source in sources]
            + [pltpu.SemaphoreType.DMA(())],
        ),
        out_shape=[
            jax.ShapeDtypeStruct((tok.shape[0], source.shape[1]), dtype)
            for source, dtype in zip(sources, out_dtypes)
        ],
        compiler_params=pltpu.CompilerParams(vmem_limit_bytes=56 * 1024 * 1024),
    )(tok, *sources)


def _combine_rows_kernel(tok_ref, *refs):
    count = (len(refs) - 1) // 4
    addends, outs = refs[:count], refs[count : 2 * count]
    totals, rows_bufs, sem = refs[2 * count : 3 * count], refs[3 * count : 4 * count], refs[-1]
    rows = rows_bufs[0].shape[0]
    step = pl.program_id(0)

    @pl.when(step == 0)
    def _():
        for total in totals:
            total[...] = jnp.zeros_like(total)

    for addend, rows_buf in zip(addends, rows_bufs):
        rows_buf[...] = addend[...].astype(jnp.float32)
    base = step * rows

    def body(s, carry):
        t = tok_ref[base + s]
        for total, rows_buf in zip(totals, rows_bufs):
            total[pl.ds(t, 1), :] += rows_buf[pl.ds(s, 1), :]
        return carry

    lax.fori_loop(0, rows, body, 0, unroll=8)

    @pl.when(step == pl.num_programs(0) - 1)
    def _():
        for total, out in zip(totals, outs):
            transfer = pltpu.make_async_copy(total, out, sem)
            transfer.start()
            transfer.wait()


def combine_rows(tok, addends, rows, total_rows):
    blocks = tok.shape[0] // rows
    return pl.pallas_call(
        _combine_rows_kernel,
        grid_spec=pltpu.PrefetchScalarGridSpec(
            num_scalar_prefetch=1,
            grid=(blocks,),
            in_specs=[
                pl.BlockSpec((rows, addend.shape[1]), lambda b, tok: (b, 0)) for addend in addends
            ],
            out_specs=[pl.BlockSpec(memory_space=pl.ANY) for _ in addends],
            scratch_shapes=[
                pltpu.VMEM((total_rows, addend.shape[1]), jnp.float32) for addend in addends
            ]
            + [pltpu.VMEM((rows, addend.shape[1]), jnp.float32) for addend in addends]
            + [pltpu.SemaphoreType.DMA(())],
        ),
        out_shape=[
            jax.ShapeDtypeStruct((total_rows, addend.shape[1]), jnp.float32) for addend in addends
        ],
        compiler_params=pltpu.CompilerParams(vmem_limit_bytes=56 * 1024 * 1024),
    )(tok, *addends)


def table_lookup(table, index):
    lanes = 128
    high_count = table.shape[0] // lanes
    low_marks = (index[:, None] % lanes == jnp.arange(lanes)[None, :]).astype(jnp.bfloat16)
    picked = jnp.dot(
        low_marks,
        table.reshape(high_count, lanes).astype(jnp.bfloat16).T,
        preferred_element_type=jnp.float32,
    )
    high_marks = index[:, None] // lanes == jnp.arange(high_count)[None, :]
    return jnp.sum(jnp.where(high_marks, picked, 0.0), axis=1).astype(jnp.int32)


def invert_slots(local_slot, values, slot_count):
    lanes = 128
    high_count = slot_count // lanes
    column_marks = (local_slot[:, None] // lanes == jnp.arange(high_count)[None, :]).astype(
        jnp.bfloat16
    )
    lane_marks = local_slot[:, None] % lanes == jnp.arange(lanes)[None, :]
    shifted = values + 1
    parts = []
    for digit in (shifted // 256, shifted % 256):
        spread = jnp.where(lane_marks, digit[:, None], 0).astype(jnp.bfloat16)
        parts.append(
            jnp.einsum("ic,il->cl", column_marks, spread, preferred_element_type=jnp.float32)
        )
    return (256.0 * parts[0] + parts[1]).astype(jnp.int32).reshape(slot_count) - 1


def block_scores(query_rot, key_rot, segments, row_start, key_end, local_groups, group_ratio):
    queries = query_rot[row_start:key_end].reshape(
        key_end - row_start, local_groups, group_ratio, HD
    )
    raw_scores = (
        jnp.einsum("qgrd,kgd->grqk", queries, key_rot[:key_end], preferred_element_type=jnp.float32)
        * ATTN_SCALE
    )
    visible = allowed(
        jnp.arange(row_start, key_end, dtype=jnp.int32),
        segments[row_start:key_end],
        jnp.arange(key_end, dtype=jnp.int32),
        segments[:key_end],
    )
    return (jnp.where(visible[None, None], raw_scores, MASKED), queries)


def fetch_experts(gate_weight, up_weight, down_weight):
    return (
        lax.all_gather(gate_weight, "dp", axis=1, tiled=True),
        lax.all_gather(up_weight, "dp", axis=1, tiled=True),
        lax.all_gather(down_weight, "dp", axis=2, tiled=True),
    )


def reduce_experts(grads):
    return (
        lax.psum_scatter(grads[0], "dp", scatter_dimension=1, tiled=True).astype(jnp.float32),
        lax.psum_scatter(grads[1], "dp", scatter_dimension=1, tiled=True).astype(jnp.float32),
        jnp.swapaxes(
            lax.psum_scatter(grads[2], "dp", scatter_dimension=1, tiled=True).astype(jnp.float32),
            1,
            2,
        ),
    )


def local(
    hidden_in,
    out_grad,
    segment_ids,
    expert_ids,
    fill_order,
    attention_gain,
    query_weight,
    key_weight,
    value_weight,
    output_weight,
    mixture_gain,
    router_weight,
    gate_weight,
    up_weight,
    down_weight,
):
    local_heads = query_weight.shape[1] // HD
    local_groups = key_weight.shape[1] // HD
    group_ratio = local_heads // local_groups
    block_count = TOK_GRP // QBLK
    local_experts = gate_weight.shape[0]
    gain_one, query_full, key_full, value_full, gain_two, router_full = (
        lax.all_gather(attention_gain, "dp", axis=0, tiled=True),
        lax.all_gather(query_weight, "dp", axis=0, tiled=True),
        lax.all_gather(key_weight, "dp", axis=0, tiled=True),
        lax.all_gather(value_weight, "dp", axis=0, tiled=True),
        lax.all_gather(mixture_gain, "dp", axis=0, tiled=True),
        lax.all_gather(router_weight, "dp", axis=0, tiled=True),
    )
    output_all = lax.all_gather(
        lax.all_gather(output_weight, "tensor", axis=0, tiled=True), "dp", axis=1, tiled=True
    )
    gain_one = gain_one.astype(jnp.float32)
    gain_two = gain_two.astype(jnp.float32)
    residual = hidden_in.astype(jnp.float32)
    normed_shard, unit_one, inverse_one = rms_forward(residual, gain_one)
    normed_full = lax.all_gather(normed_shard.astype(jnp.bfloat16), "tensor", axis=0, tiled=True)
    gate_weight, up_weight, normed_full = lax.optimization_barrier(
        (gate_weight, up_weight, normed_full)
    )
    gate_full = lax.all_gather(gate_weight, "dp", axis=1, tiled=True)
    up_full = lax.all_gather(up_weight, "dp", axis=1, tiled=True)
    positions, segments = group_layout(segment_ids[0], PROMPT)
    cosine_table, sine_table = rope_tables(positions, HD)
    query_pre = jnp.dot(normed_full, query_full, preferred_element_type=jnp.float32).reshape(
        TOK_GRP, local_heads, HD
    )
    key_pre = jnp.dot(normed_full, key_full, preferred_element_type=jnp.float32).reshape(
        TOK_GRP, local_groups, HD
    )
    value_low = (
        jnp.dot(normed_full, value_full, preferred_element_type=jnp.float32)
        .astype(jnp.bfloat16)
        .reshape(TOK_GRP, local_groups, HD)
    )
    query_rot = rotate(query_pre, cosine_table, sine_table).astype(jnp.bfloat16)
    key_rot = rotate(key_pre, cosine_table, sine_table).astype(jnp.bfloat16)
    mixed_blocks = []
    logsum_blocks = []
    for block_index in range(block_count):
        row_start = block_index * QBLK
        key_end = row_start + QBLK
        scores, queries = block_scores(
            query_rot, key_rot, segments, row_start, key_end, local_groups, group_ratio
        )
        top_score = jnp.max(scores, axis=-1, keepdims=True)
        shifted_exp = jnp.exp(scores - top_score)
        total_exp = jnp.sum(shifted_exp, axis=-1, keepdims=True)
        soft_weights = (shifted_exp / total_exp).astype(jnp.bfloat16)
        logsum_blocks.append(top_score + jnp.log(total_exp))
        mixed = jnp.einsum(
            "grqk,kgd->qgrd", soft_weights, value_low[:key_end], preferred_element_type=jnp.float32
        )
        mixed_blocks.append(mixed.astype(jnp.bfloat16).reshape(QBLK, local_heads * HD))
    mixed_full = jnp.concatenate(mixed_blocks, axis=0)
    mixed_full, gate_full, up_full = lax.optimization_barrier((mixed_full, gate_full, up_full))
    mixed_own = lax.all_to_all(mixed_full, "tensor", 0, 1, tiled=True)
    attended = jnp.dot(mixed_own, output_all, preferred_element_type=jnp.float32)
    middle = residual + RESIDUAL_SCALE * attended
    normed_two, unit_two, inverse_two = rms_forward(middle, gain_two)
    mixture_in = lax.all_gather(normed_two.astype(jnp.bfloat16), "tensor", axis=0, tiled=True)
    down_weight, mixture_in = lax.optimization_barrier((down_weight, mixture_in))
    down_full = lax.all_gather(down_weight, "dp", axis=2, tiled=True)
    logits = jnp.dot(mixture_in, router_full, preferred_element_type=jnp.float32)
    routed_marks = (
        expert_ids[:, :, None] == jnp.arange(EXPERTS, dtype=jnp.int32)[None, None, :]
    ).astype(jnp.float32)
    routed = jnp.sum(routed_marks * logits[:, None, :], axis=-1)
    gates = jax.nn.softmax(routed, axis=-1)
    slot_count = local_experts * CAP
    first_slot = lax.axis_index("tensor") * slot_count
    slot_pair = route_slots(expert_ids, fill_order[0], first_slot, slot_count)
    slot_valid = slot_pair >= 0
    safe_pair = jnp.maximum(slot_pair, 0)
    slot_token = safe_pair // TOPK
    slot_choice = safe_pair % TOPK
    side_lanes = 128
    gate_table = jnp.pad(gates, ((0, 0), (0, side_lanes - TOPK)))
    inputs, gate_rows = gather_rows(
        slot_token,
        (mixture_in.astype(jnp.float32), gate_table),
        CAP,
        (jnp.bfloat16, jnp.float32),
    )
    inputs = inputs.reshape(local_experts, CAP, D)
    choice_marks = slot_choice[:, None] == jnp.arange(side_lanes)[None, :]
    slot_gate = jnp.sum(jnp.where(choice_marks, gate_rows, 0.0), axis=1)
    slot_gate = jnp.where(slot_valid, slot_gate, 0.0).reshape(local_experts, CAP, 1)
    gate_pre = jnp.einsum("ecd,edf->ecf", inputs, gate_full, preferred_element_type=jnp.float32)
    up_pre = jnp.einsum("ecd,edf->ecf", inputs, up_full, preferred_element_type=jnp.float32)
    activated = jax.nn.silu(gate_pre)
    hidden_units = (slot_gate * activated * up_pre).astype(jnp.bfloat16)
    expert_out = jnp.einsum(
        "ecf,efd->ecd", hidden_units, down_full, preferred_element_type=jnp.float32
    )
    (mixture_sum,) = combine_rows(slot_token, (expert_out.reshape(slot_count, D),), CAP, TOK_GRP)
    out_grad_held, down_full = lax.optimization_barrier((out_grad, down_full))
    cotangent_full = lax.all_gather(out_grad_held, "tensor", axis=0, tiled=True)
    scaled_cotangent = (
        (RESIDUAL_SCALE * cotangent_full.astype(jnp.float32)).astype(jnp.bfloat16).astype(jnp.float32)
    )
    scaled_cotangent, mixture_sum, projection_local = lax.optimization_barrier(
        (
            scaled_cotangent,
            mixture_sum,
            jnp.concatenate([query_weight, key_weight, value_weight], axis=1),
        )
    )
    projection_all = lax.all_gather(
        lax.all_gather(projection_local, "tensor", axis=1, tiled=True), "dp", axis=0, tiled=True
    )
    mixture_part = lax.psum_scatter(
        mixture_sum.astype(jnp.bfloat16), "tensor", scatter_dimension=0, tiled=True
    ).astype(jnp.float32)
    (out_rows,) = gather_rows(slot_token, (scaled_cotangent,), CAP, (jnp.bfloat16,))
    out_rows = out_rows.reshape(local_experts, CAP, D)
    hidden_grad = jnp.einsum("ecd,efd->ecf", out_rows, down_full, preferred_element_type=jnp.float32)
    gate_grad_slot = jnp.sum(activated * up_pre * hidden_grad, axis=-1).reshape(slot_count)
    gate_grad_rows = jnp.where(
        choice_marks & slot_valid[:, None], gate_grad_slot[:, None], 0.0
    )
    product_grad = slot_gate * hidden_grad
    gate_pre_grad = (product_grad * up_pre * silu_slope(gate_pre)).astype(jnp.bfloat16)
    up_pre_grad = (product_grad * activated).astype(jnp.bfloat16)
    input_rows = jnp.einsum(
        "ecf,edf->ecd", gate_pre_grad, gate_full, preferred_element_type=jnp.float32
    ) + jnp.einsum("ecf,edf->ecd", up_pre_grad, up_full, preferred_element_type=jnp.float32)
    input_rows = input_rows.astype(jnp.bfloat16).reshape(slot_count, D)
    grad_in_mixture, gate_grad_table = combine_rows(
        slot_token, (input_rows, gate_grad_rows), CAP, TOK_GRP
    )
    (inputs, gate_pre_grad, up_pre_grad, hidden_units, out_rows), grad_in_mixture, projection_all = (
        lax.optimization_barrier(
            (
                (inputs, gate_pre_grad, up_pre_grad, hidden_units, out_rows),
                grad_in_mixture,
                projection_all,
            )
        )
    )
    expert_parts = (
        jnp.einsum("ecd,ecf->edf", inputs, gate_pre_grad, preferred_element_type=jnp.float32),
        jnp.einsum("ecd,ecf->edf", inputs, up_pre_grad, preferred_element_type=jnp.float32),
        jnp.einsum("ecd,ecf->edf", out_rows, hidden_units, preferred_element_type=jnp.float32),
    )
    expert_parts = tuple(part.astype(jnp.bfloat16) for part in expert_parts)
    gates_grad = gate_grad_table[:, :TOPK]
    routed_grad = gates * (gates_grad - jnp.sum(gates * gates_grad, axis=-1, keepdims=True))
    logits_grad = jnp.sum(routed_marks * routed_grad[:, :, None], axis=1)
    router_part = jnp.einsum(
        "td,te->de", mixture_in, logits_grad, precision=HIGHEST, preferred_element_type=jnp.float32
    )
    grad_in_mixture = grad_in_mixture + jnp.einsum(
        "te,de->td", logits_grad, router_full.astype(jnp.float32), precision=HIGHEST
    )
    mixture_grad_low, mixture_part = lax.optimization_barrier(
        (grad_in_mixture.astype(jnp.bfloat16), mixture_part)
    )
    block_output = (middle + RESIDUAL_SCALE * mixture_part).astype(jnp.bfloat16)
    mixture_grad_shard = lax.psum_scatter(
        mixture_grad_low, "tensor", scatter_dimension=0, tiled=True
    ).astype(jnp.float32)
    middle_norm_grad, gain_two_grad = rms_backward(
        mixture_grad_shard, unit_two, inverse_two, gain_two
    )
    middle_grad = out_grad.astype(jnp.float32) + middle_norm_grad
    attended_grad = (RESIDUAL_SCALE * middle_grad).astype(jnp.bfloat16)
    mixed_grad_own = jnp.einsum(
        "td,fd->tf", attended_grad, output_all, preferred_element_type=jnp.float32
    ).astype(jnp.bfloat16)
    mixed_grad = lax.all_to_all(mixed_grad_own, "tensor", 1, 0, tiled=True)
    expert_parts, router_part, mixed_grad = lax.optimization_barrier(
        (expert_parts, router_part, mixed_grad)
    )
    expert_grads = reduce_experts(expert_parts)
    router_and_gain = lax.psum_scatter(
        jnp.concatenate([router_part, gain_two_grad[:, None]], axis=1),
        ("dp", "tensor"),
        scatter_dimension=0,
        tiled=True,
    )
    router_weight_grad = router_and_gain[:, : router_part.shape[1]]
    mixture_gain_grad = router_and_gain[:, router_part.shape[1]]
    output_part = jnp.einsum(
        "tf,td->fd", mixed_own, attended_grad, preferred_element_type=jnp.float32
    ).astype(jnp.bfloat16)
    output_part = lax.psum_scatter(output_part, "dp", scatter_dimension=1, tiled=True)
    mixed_grad = mixed_grad.reshape(TOK_GRP, local_groups, group_ratio, HD)
    output_weight_grad = lax.psum_scatter(
        output_part, "tensor", scatter_dimension=0, tiled=True
    ).astype(jnp.float32)
    key_grad = jnp.zeros((TOK_GRP, local_groups, HD), jnp.float32)
    value_grad = jnp.zeros((TOK_GRP, local_groups, HD), jnp.float32)
    query_blocks = []
    for block_index in range(block_count):
        row_start = block_index * QBLK
        key_end = row_start + QBLK
        scores, queries = block_scores(
            query_rot, key_rot, segments, row_start, key_end, local_groups, group_ratio
        )
        soft_full = jnp.exp(scores - logsum_blocks[block_index])
        soft_low = soft_full.astype(jnp.bfloat16)
        out_block = mixed_grad[row_start:key_end]
        weight_grad = jnp.einsum(
            "qgrd,kgd->grqk", out_block, value_low[:key_end], preferred_element_type=jnp.float32
        )
        delta = jnp.sum(soft_full * weight_grad, axis=-1, keepdims=True)
        score_grad = (soft_full * (weight_grad - delta)).astype(jnp.bfloat16)
        query_blocks.append(
            jnp.einsum(
                "grqk,kgd->qgrd", score_grad, key_rot[:key_end], preferred_element_type=jnp.float32
            )
            * ATTN_SCALE
        )
        key_grad = key_grad.at[:key_end].add(
            jnp.einsum("grqk,qgrd->kgd", score_grad, queries, preferred_element_type=jnp.float32)
            * ATTN_SCALE
        )
        value_grad = value_grad.at[:key_end].add(
            jnp.einsum("grqk,qgrd->kgd", soft_low, out_block, preferred_element_type=jnp.float32)
        )
    query_rot_grad = jnp.concatenate(query_blocks, axis=0).reshape(TOK_GRP, local_heads, HD)
    query_grad = (
        rotate_back(query_rot_grad, cosine_table, sine_table)
        .astype(jnp.bfloat16)
        .reshape(TOK_GRP, local_heads * HD)
    )
    key_grad_low = (
        rotate_back(key_grad, cosine_table, sine_table)
        .astype(jnp.bfloat16)
        .reshape(TOK_GRP, local_groups * HD)
    )
    value_grad_low = value_grad.astype(jnp.bfloat16).reshape(TOK_GRP, local_groups * HD)
    projection_grad = jnp.concatenate([query_grad, key_grad_low, value_grad_low], axis=1)
    projection_grad_own = lax.all_to_all(projection_grad, "tensor", 0, 1, tiled=True)
    (
        projection_grad_own,
        expert_grads,
        router_weight_grad,
        output_weight_grad,
        mixture_gain_grad,
    ) = lax.optimization_barrier(
        (
            projection_grad_own,
            expert_grads,
            router_weight_grad,
            output_weight_grad,
            mixture_gain_grad,
        )
    )
    gate_weight_grad, up_weight_grad, down_weight_grad = expert_grads
    normed_grad = jnp.einsum(
        "tf,df->td", projection_grad_own, projection_all, preferred_element_type=jnp.float32
    )
    query_part = jnp.einsum(
        "td,tf->df", normed_full, query_grad, preferred_element_type=jnp.float32
    )
    key_part = jnp.einsum(
        "td,tf->df", normed_full, key_grad_low, preferred_element_type=jnp.float32
    )
    value_part = jnp.einsum(
        "td,tf->df", normed_full, value_grad_low, preferred_element_type=jnp.float32
    )
    projection_parts = jnp.concatenate(
        [query_part, key_part, value_part], axis=1
    ).astype(jnp.bfloat16)
    projection_parts, normed_grad = lax.optimization_barrier((projection_parts, normed_grad))
    input_norm_grad, gain_one_grad = rms_backward(normed_grad, unit_one, inverse_one, gain_one)
    input_grad = middle_grad + input_norm_grad
    projection_grads = lax.psum_scatter(
        projection_parts, "dp", scatter_dimension=0, tiled=True
    ).astype(jnp.float32)
    query_width, key_width = query_part.shape[1], key_part.shape[1]
    query_weight_grad = projection_grads[:, :query_width]
    key_weight_grad = projection_grads[:, query_width : query_width + key_width]
    value_weight_grad = projection_grads[:, query_width + key_width :]

    attention_gain_grad = lax.psum_scatter(
        gain_one_grad, ("dp", "tensor"), scatter_dimension=0, tiled=True
    )
    return (
        block_output,
        input_grad,
        attention_gain_grad,
        query_weight_grad,
        key_weight_grad,
        value_weight_grad,
        output_weight_grad,
        mixture_gain_grad,
        router_weight_grad,
        gate_weight_grad,
        up_weight_grad,
        down_weight_grad,
    )


def solution(mesh):
    in_specs = (
        P(("dp", "tensor"), None),
        P(("dp", "tensor"), None),
        P("dp", None),
        P("dp", None),
        P("dp", None),
        P("dp"),
        P("dp", "tensor"),
        P("dp", "tensor"),
        P("dp", "tensor"),
        P("tensor", "dp"),
        P("dp"),
        P("dp", None),
        P("tensor", "dp", None),
        P("tensor", "dp", None),
        P("tensor", None, "dp"),
    )
    out_specs = (
        P(("dp", "tensor"), None),
        P(("dp", "tensor"), None),
        P(("dp", "tensor")),
        P("dp", "tensor"),
        P("dp", "tensor"),
        P("dp", "tensor"),
        P("tensor", "dp"),
        P(("dp", "tensor")),
        P(("dp", "tensor"), None),
        P("tensor", "dp", None),
        P("tensor", "dp", None),
        P("tensor", None, "dp"),
    )
    return jax.shard_map(local, mesh=mesh, in_specs=in_specs, out_specs=out_specs, check_vma=False)
```

```python
import jax
import jax.numpy as jnp
from jax import lax
from jax.experimental import pallas as pl
from jax.experimental.pallas import tpu as pltpu
from jax.sharding import PartitionSpec as P

D = 1536
HD = 64
EXPERTS = 40
TOPK = 8
PROMPT = 2048
NCONT = 4
QBLK = 512
TOK_GRP = 3072
CAP = 768


ATTN_SCALE = 0.015625
RESIDUAL_SCALE = 0.22
NORM_EPS = 1e-06
ROPE_BASE = 10000.0
MASKED = -1e30
HIGHEST = lax.Precision.HIGHEST


def rms_forward(values, gain_row):
    inverse_rms = lax.rsqrt(jnp.mean(values * values, axis=-1, keepdims=True) + NORM_EPS)
    unit_rows = values * inverse_rms
    return (unit_rows * gain_row, unit_rows, inverse_rms)


def rms_backward(gradient, unit_rows, inverse_rms, gain_row):
    gain_grad = jnp.sum(gradient * unit_rows, axis=0)
    scaled = gradient * gain_row
    mean_term = jnp.mean(scaled * unit_rows, axis=-1, keepdims=True)
    return (inverse_rms * (scaled - unit_rows * mean_term), gain_grad)


def group_layout(segment_row, prompt_length):
    cont_length = segment_row.shape[0]
    segment_marks = (segment_row[:, None] == jnp.arange(NCONT, dtype=jnp.int32)[None, :]).astype(
        jnp.int32
    )
    segment_sizes = jnp.sum(segment_marks, axis=0)
    segment_starts = jnp.cumsum(segment_sizes) - segment_sizes
    token_starts = jnp.sum(segment_marks * segment_starts[None, :], axis=1)
    inside = jnp.arange(cont_length, dtype=jnp.int32) - token_starts
    positions = jnp.concatenate(
        [jnp.arange(prompt_length, dtype=jnp.int32), prompt_length + inside]
    )
    segments = jnp.concatenate([jnp.zeros((prompt_length,), jnp.int32), segment_row + 1])
    return (positions, segments)


def allowed(query_index, query_segment, key_index, key_segment):
    causal = key_index[None, :] <= query_index[:, None]
    shared = (key_segment[None, :] == 0) | (key_segment[None, :] == query_segment[:, None])
    return causal & shared


def rope_tables(positions, head_size):
    halfway = head_size // 2
    frequency = ROPE_BASE ** (-(2.0 * jnp.arange(halfway, dtype=jnp.float32)) / head_size)
    angles = positions.astype(jnp.float32)[:, None] * frequency[None, :]
    return (jnp.cos(angles), jnp.sin(angles))


def rotate(values, cosine_table, sine_table):
    halfway = values.shape[-1] // 2
    first_half = values[..., :halfway]
    second_half = values[..., halfway:]
    cosine_part = cosine_table[:, None, :]
    sine_part = sine_table[:, None, :]
    return jnp.concatenate(
        [
            first_half * cosine_part - second_half * sine_part,
            second_half * cosine_part + first_half * sine_part,
        ],
        axis=-1,
    )


def rotate_back(gradient, cosine_table, sine_table):
    halfway = gradient.shape[-1] // 2
    first_half = gradient[..., :halfway]
    second_half = gradient[..., halfway:]
    cosine_part = cosine_table[:, None, :]
    sine_part = sine_table[:, None, :]
    return jnp.concatenate(
        [
            first_half * cosine_part + second_half * sine_part,
            second_half * cosine_part - first_half * sine_part,
        ],
        axis=-1,
    )


def silu_slope(values):
    sigmoid_part = jax.nn.sigmoid(values)
    return sigmoid_part * (1.0 + values * (1.0 - sigmoid_part))


def route_slots(expert_row, order_row, first_slot, slot_count):
    pair_count = expert_row.shape[0] * expert_row.shape[1]
    ordered = table_lookup(expert_row.reshape(pair_count), order_row)
    onehot = ordered[:, None] == jnp.arange(EXPERTS, dtype=jnp.int32)[None, :]
    rank_block = 256
    blocks = pair_count // rank_block
    pair_marks = onehot.astype(jnp.bfloat16).reshape(blocks, rank_block, EXPERTS)
    lower_ones = (jnp.arange(rank_block)[:, None] >= jnp.arange(rank_block)[None, :]).astype(
        jnp.bfloat16
    )
    within = jnp.einsum(
        "ij,bje->bie", lower_ones, pair_marks, preferred_element_type=jnp.float32
    ).astype(jnp.int32)
    totals = within[:, -1, :]
    before = jnp.cumsum(totals, axis=0) - totals
    counts = (within + before[:, None, :]).reshape(pair_count, EXPERTS)
    pair_rank = jnp.sum(jnp.where(onehot, counts, 0), axis=1) - 1
    local_slot = ordered * CAP + pair_rank - first_slot
    kept = (pair_rank < CAP) & (local_slot >= 0) & (local_slot < slot_count)
    local_slot = jnp.where(kept, local_slot, -1)
    return invert_slots(local_slot, order_row, slot_count)


def _gather_rows_kernel(tok_ref, *refs):
    count = (len(refs) - 1) // 4
    sources, outs = refs[:count], refs[count : 2 * count]
    copies, rows_bufs, sem = refs[2 * count : 3 * count], refs[3 * count : 4 * count], refs[-1]
    rows = rows_bufs[0].shape[0]
    step = pl.program_id(0)

    @pl.when(step == 0)
    def _():
        for source, copy in zip(sources, copies):
            transfer = pltpu.make_async_copy(source, copy, sem)
            transfer.start()
            transfer.wait()

    base = step * rows

    def body(s, carry):
        t = tok_ref[base + s]
        for copy, rows_buf in zip(copies, rows_bufs):
            rows_buf[pl.ds(s, 1), :] = copy[pl.ds(t, 1), :]
        return carry

    lax.fori_loop(0, rows, body, 0, unroll=8)
    for out, rows_buf in zip(outs, rows_bufs):
        out[...] = rows_buf[...].astype(out.dtype)


def gather_rows(tok, sources, rows, out_dtypes):
    blocks = tok.shape[0] // rows
    return pl.pallas_call(
        _gather_rows_kernel,
        grid_spec=pltpu.PrefetchScalarGridSpec(
            num_scalar_prefetch=1,
            grid=(blocks,),
            in_specs=[pl.BlockSpec(memory_space=pl.ANY) for _ in sources],
            out_specs=[
                pl.BlockSpec((rows, source.shape[1]), lambda b, tok: (b, 0)) for source in sources
            ],
            scratch_shapes=[pltpu.VMEM(source.shape, jnp.float32) for source in sources]
            + [pltpu.VMEM((rows, source.shape[1]), jnp.float32) for source in sources]
            + [pltpu.SemaphoreType.DMA(())],
        ),
        out_shape=[
            jax.ShapeDtypeStruct((tok.shape[0], source.shape[1]), dtype)
            for source, dtype in zip(sources, out_dtypes)
        ],
        compiler_params=pltpu.CompilerParams(vmem_limit_bytes=56 * 1024 * 1024),
    )(tok, *sources)


def _combine_rows_kernel(tok_ref, *refs):
    count = (len(refs) - 1) // 4
    addends, outs = refs[:count], refs[count : 2 * count]
    totals, rows_bufs, sem = refs[2 * count : 3 * count], refs[3 * count : 4 * count], refs[-1]
    rows = rows_bufs[0].shape[0]
    step = pl.program_id(0)

    @pl.when(step == 0)
    def _():
        for total in totals:
            total[...] = jnp.zeros_like(total)

    for addend, rows_buf in zip(addends, rows_bufs):
        rows_buf[...] = addend[...].astype(jnp.float32)
    base = step * rows

    def body(s, carry):
        t = tok_ref[base + s]
        for total, rows_buf in zip(totals, rows_bufs):
            total[pl.ds(t, 1), :] += rows_buf[pl.ds(s, 1), :]
        return carry

    lax.fori_loop(0, rows, body, 0, unroll=8)

    @pl.when(step == pl.num_programs(0) - 1)
    def _():
        for total, out in zip(totals, outs):
            transfer = pltpu.make_async_copy(total, out, sem)
            transfer.start()
            transfer.wait()


def combine_rows(tok, addends, rows, total_rows):
    blocks = tok.shape[0] // rows
    return pl.pallas_call(
        _combine_rows_kernel,
        grid_spec=pltpu.PrefetchScalarGridSpec(
            num_scalar_prefetch=1,
            grid=(blocks,),
            in_specs=[
                pl.BlockSpec((rows, addend.shape[1]), lambda b, tok: (b, 0)) for addend in addends
            ],
            out_specs=[pl.BlockSpec(memory_space=pl.ANY) for _ in addends],
            scratch_shapes=[
                pltpu.VMEM((total_rows, addend.shape[1]), jnp.float32) for addend in addends
            ]
            + [pltpu.VMEM((rows, addend.shape[1]), jnp.float32) for addend in addends]
            + [pltpu.SemaphoreType.DMA(())],
        ),
        out_shape=[
            jax.ShapeDtypeStruct((total_rows, addend.shape[1]), jnp.float32) for addend in addends
        ],
        compiler_params=pltpu.CompilerParams(vmem_limit_bytes=56 * 1024 * 1024),
    )(tok, *addends)


def table_lookup(table, index):
    lanes = 128
    high_count = table.shape[0] // lanes
    low_marks = (index[:, None] % lanes == jnp.arange(lanes)[None, :]).astype(jnp.bfloat16)
    picked = jnp.dot(
        low_marks,
        table.reshape(high_count, lanes).astype(jnp.bfloat16).T,
        preferred_element_type=jnp.float32,
    )
    high_marks = index[:, None] // lanes == jnp.arange(high_count)[None, :]
    return jnp.sum(jnp.where(high_marks, picked, 0.0), axis=1).astype(jnp.int32)


def invert_slots(local_slot, values, slot_count):
    lanes = 128
    high_count = slot_count // lanes
    column_marks = (local_slot[:, None] // lanes == jnp.arange(high_count)[None, :]).astype(
        jnp.bfloat16
    )
    lane_marks = local_slot[:, None] % lanes == jnp.arange(lanes)[None, :]
    shifted = values + 1
    parts = []
    for digit in (shifted // 256, shifted % 256):
        spread = jnp.where(lane_marks, digit[:, None], 0).astype(jnp.bfloat16)
        parts.append(
            jnp.einsum("ic,il->cl", column_marks, spread, preferred_element_type=jnp.float32)
        )
    return (256.0 * parts[0] + parts[1]).astype(jnp.int32).reshape(slot_count) - 1


def block_scores(query_rot, key_rot, segments, row_start, key_end, local_groups, group_ratio):
    queries = query_rot[row_start:key_end].reshape(
        key_end - row_start, local_groups, group_ratio, HD
    )
    raw_scores = (
        jnp.einsum("qgrd,kgd->grqk", queries, key_rot[:key_end], preferred_element_type=jnp.float32)
        * ATTN_SCALE
    )
    visible = allowed(
        jnp.arange(row_start, key_end, dtype=jnp.int32),
        segments[row_start:key_end],
        jnp.arange(key_end, dtype=jnp.int32),
        segments[:key_end],
    )
    return (jnp.where(visible[None, None], raw_scores, MASKED), queries)


def fetch_experts(gate_weight, up_weight, down_weight):
    return (
        lax.all_gather(gate_weight, "dp", axis=1, tiled=True),
        lax.all_gather(up_weight, "dp", axis=1, tiled=True),
        lax.all_gather(down_weight, "dp", axis=2, tiled=True),
    )


def reduce_experts(grads):
    return (
        lax.psum_scatter(grads[0], "dp", scatter_dimension=1, tiled=True).astype(jnp.float32),
        lax.psum_scatter(grads[1], "dp", scatter_dimension=1, tiled=True).astype(jnp.float32),
        jnp.swapaxes(
            lax.psum_scatter(grads[2], "dp", scatter_dimension=1, tiled=True).astype(jnp.float32),
            1,
            2,
        ),
    )


def local(
    hidden_in,
    out_grad,
    segment_ids,
    expert_ids,
    fill_order,
    attention_gain,
    query_weight,
    key_weight,
    value_weight,
    output_weight,
    mixture_gain,
    router_weight,
    gate_weight,
    up_weight,
    down_weight,
):
    local_heads = query_weight.shape[1] // HD
    local_groups = key_weight.shape[1] // HD
    group_ratio = local_heads // local_groups
    block_count = TOK_GRP // QBLK
    local_experts = gate_weight.shape[0]
    gain_one, query_full, key_full, value_full, gain_two, router_full = (
        lax.all_gather(attention_gain, "dp", axis=0, tiled=True),
        lax.all_gather(query_weight, "dp", axis=0, tiled=True),
        lax.all_gather(key_weight, "dp", axis=0, tiled=True),
        lax.all_gather(value_weight, "dp", axis=0, tiled=True),
        lax.all_gather(mixture_gain, "dp", axis=0, tiled=True),
        lax.all_gather(router_weight, "dp", axis=0, tiled=True),
    )
    output_all = lax.all_gather(
        lax.all_gather(output_weight, "tensor", axis=0, tiled=True), "dp", axis=1, tiled=True
    )
    gain_one = gain_one.astype(jnp.float32)
    gain_two = gain_two.astype(jnp.float32)
    residual = hidden_in.astype(jnp.float32)
    normed_shard, unit_one, inverse_one = rms_forward(residual, gain_one)
    normed_full = lax.all_gather(normed_shard.astype(jnp.bfloat16), "tensor", axis=0, tiled=True)
    gate_weight, up_weight, normed_full = lax.optimization_barrier(
        (gate_weight, up_weight, normed_full)
    )
    gate_full = lax.all_gather(gate_weight, "dp", axis=1, tiled=True)
    up_full = lax.all_gather(up_weight, "dp", axis=1, tiled=True)
    positions, segments = group_layout(segment_ids[0], PROMPT)
    cosine_table, sine_table = rope_tables(positions, HD)
    query_pre = jnp.dot(normed_full, query_full, preferred_element_type=jnp.float32).reshape(
        TOK_GRP, local_heads, HD
    )
    key_pre = jnp.dot(normed_full, key_full, preferred_element_type=jnp.float32).reshape(
        TOK_GRP, local_groups, HD
    )
    value_low = (
        jnp.dot(normed_full, value_full, preferred_element_type=jnp.float32)
        .astype(jnp.bfloat16)
        .reshape(TOK_GRP, local_groups, HD)
    )
    query_rot = rotate(query_pre, cosine_table, sine_table).astype(jnp.bfloat16)
    key_rot = rotate(key_pre, cosine_table, sine_table).astype(jnp.bfloat16)
    mixed_blocks = []
    logsum_blocks = []
    for block_index in range(block_count):
        row_start = block_index * QBLK
        key_end = row_start + QBLK
        scores, queries = block_scores(
            query_rot, key_rot, segments, row_start, key_end, local_groups, group_ratio
        )
        top_score = jnp.max(scores, axis=-1, keepdims=True)
        shifted_exp = jnp.exp(scores - top_score)
        total_exp = jnp.sum(shifted_exp, axis=-1, keepdims=True)
        soft_weights = (shifted_exp / total_exp).astype(jnp.bfloat16)
        logsum_blocks.append(top_score + jnp.log(total_exp))
        mixed = jnp.einsum(
            "grqk,kgd->qgrd", soft_weights, value_low[:key_end], preferred_element_type=jnp.float32
        )
        mixed_blocks.append(mixed.astype(jnp.bfloat16).reshape(QBLK, local_heads * HD))
    mixed_full = jnp.concatenate(mixed_blocks, axis=0)
    mixed_full, gate_full, up_full = lax.optimization_barrier((mixed_full, gate_full, up_full))
    mixed_own = lax.all_to_all(mixed_full, "tensor", 0, 1, tiled=True)
    attended = jnp.dot(mixed_own, output_all, preferred_element_type=jnp.float32)
    middle = residual + RESIDUAL_SCALE * attended
    normed_two, unit_two, inverse_two = rms_forward(middle, gain_two)
    mixture_in = lax.all_gather(normed_two.astype(jnp.bfloat16), "tensor", axis=0, tiled=True)
    down_weight, mixture_in = lax.optimization_barrier((down_weight, mixture_in))
    down_full = lax.all_gather(down_weight, "dp", axis=2, tiled=True)
    logits = jnp.dot(mixture_in, router_full, preferred_element_type=jnp.float32)
    routed_marks = (
        expert_ids[:, :, None] == jnp.arange(EXPERTS, dtype=jnp.int32)[None, None, :]
    ).astype(jnp.float32)
    routed = jnp.sum(routed_marks * logits[:, None, :], axis=-1)
    gates = jax.nn.softmax(routed, axis=-1)
    slot_count = local_experts * CAP
    first_slot = lax.axis_index("tensor") * slot_count
    slot_pair = route_slots(expert_ids, fill_order[0], first_slot, slot_count)
    slot_valid = slot_pair >= 0
    safe_pair = jnp.maximum(slot_pair, 0)
    slot_token = safe_pair // TOPK
    slot_choice = safe_pair % TOPK
    side_lanes = 128
    gate_table = jnp.pad(gates, ((0, 0), (0, side_lanes - TOPK)))
    inputs, gate_rows = gather_rows(
        slot_token,
        (mixture_in.astype(jnp.float32), gate_table),
        CAP,
        (jnp.bfloat16, jnp.float32),
    )
    inputs = inputs.reshape(local_experts, CAP, D)
    choice_marks = slot_choice[:, None] == jnp.arange(side_lanes)[None, :]
    slot_gate = jnp.sum(jnp.where(choice_marks, gate_rows, 0.0), axis=1)
    slot_gate = jnp.where(slot_valid, slot_gate, 0.0).reshape(local_experts, CAP, 1)
    gate_pre = jnp.einsum("ecd,edf->ecf", inputs, gate_full, preferred_element_type=jnp.float32)
    up_pre = jnp.einsum("ecd,edf->ecf", inputs, up_full, preferred_element_type=jnp.float32)
    activated = jax.nn.silu(gate_pre)
    hidden_units = (slot_gate * activated * up_pre).astype(jnp.bfloat16)
    expert_out = jnp.einsum(
        "ecf,efd->ecd", hidden_units, down_full, preferred_element_type=jnp.float32
    )
    (mixture_sum,) = combine_rows(slot_token, (expert_out.reshape(slot_count, D),), CAP, TOK_GRP)
    out_grad_held, down_full = lax.optimization_barrier((out_grad, down_full))
    cotangent_full = lax.all_gather(out_grad_held, "tensor", axis=0, tiled=True)
    scaled_cotangent = (
        (RESIDUAL_SCALE * cotangent_full.astype(jnp.float32)).astype(jnp.bfloat16).astype(jnp.float32)
    )
    scaled_cotangent, mixture_sum, projection_local = lax.optimization_barrier(
        (
            scaled_cotangent,
            mixture_sum,
            jnp.concatenate([query_weight, key_weight, value_weight], axis=1),
        )
    )
    projection_all = lax.all_gather(
        lax.all_gather(projection_local, "tensor", axis=1, tiled=True), "dp", axis=0, tiled=True
    )
    mixture_part = lax.psum_scatter(
        mixture_sum.astype(jnp.bfloat16), "tensor", scatter_dimension=0, tiled=True
    ).astype(jnp.float32)
    (out_rows,) = gather_rows(slot_token, (scaled_cotangent,), CAP, (jnp.bfloat16,))
    out_rows = out_rows.reshape(local_experts, CAP, D)
    hidden_grad = jnp.einsum("ecd,efd->ecf", out_rows, down_full, preferred_element_type=jnp.float32)
    gate_grad_slot = jnp.sum(activated * up_pre * hidden_grad, axis=-1).reshape(slot_count)
    gate_grad_rows = jnp.where(
        choice_marks & slot_valid[:, None], gate_grad_slot[:, None], 0.0
    )
    product_grad = slot_gate * hidden_grad
    gate_pre_grad = (product_grad * up_pre * silu_slope(gate_pre)).astype(jnp.bfloat16)
    up_pre_grad = (product_grad * activated).astype(jnp.bfloat16)
    input_rows = jnp.einsum(
        "ecf,edf->ecd", gate_pre_grad, gate_full, preferred_element_type=jnp.float32
    ) + jnp.einsum("ecf,edf->ecd", up_pre_grad, up_full, preferred_element_type=jnp.float32)
    input_rows = input_rows.astype(jnp.bfloat16).reshape(slot_count, D)
    grad_in_mixture, gate_grad_table = combine_rows(
        slot_token, (input_rows, gate_grad_rows), CAP, TOK_GRP
    )
    (inputs, gate_pre_grad, up_pre_grad, hidden_units, out_rows), grad_in_mixture, projection_all = (
        lax.optimization_barrier(
            (
                (inputs, gate_pre_grad, up_pre_grad, hidden_units, out_rows),
                grad_in_mixture,
                projection_all,
            )
        )
    )
    expert_parts = (
        jnp.einsum("ecd,ecf->edf", inputs, gate_pre_grad, preferred_element_type=jnp.float32),
        jnp.einsum("ecd,ecf->edf", inputs, up_pre_grad, preferred_element_type=jnp.float32),
        jnp.einsum("ecd,ecf->edf", out_rows, hidden_units, preferred_element_type=jnp.float32),
    )
    expert_parts = tuple(part.astype(jnp.bfloat16) for part in expert_parts)
    gates_grad = gate_grad_table[:, :TOPK]
    routed_grad = gates * (gates_grad - jnp.sum(gates * gates_grad, axis=-1, keepdims=True))
    logits_grad = jnp.sum(routed_marks * routed_grad[:, :, None], axis=1)
    router_part = jnp.einsum(
        "td,te->de", mixture_in, logits_grad, precision=HIGHEST, preferred_element_type=jnp.float32
    )
    grad_in_mixture = grad_in_mixture + jnp.einsum(
        "te,de->td", logits_grad, router_full.astype(jnp.float32), precision=HIGHEST
    )
    mixture_grad_low, mixture_part = lax.optimization_barrier(
        (grad_in_mixture.astype(jnp.bfloat16), mixture_part)
    )
    block_output = (middle + RESIDUAL_SCALE * mixture_part).astype(jnp.bfloat16)
    mixture_grad_shard = lax.psum_scatter(
        mixture_grad_low, "tensor", scatter_dimension=0, tiled=True
    ).astype(jnp.float32)
    middle_norm_grad, gain_two_grad = rms_backward(
        mixture_grad_shard, unit_two, inverse_two, gain_two
    )
    middle_grad = out_grad.astype(jnp.float32) + middle_norm_grad
    attended_grad = (RESIDUAL_SCALE * middle_grad).astype(jnp.bfloat16)
    mixed_grad_own = jnp.einsum(
        "td,fd->tf", attended_grad, output_all, preferred_element_type=jnp.float32
    ).astype(jnp.bfloat16)
    mixed_grad = lax.all_to_all(mixed_grad_own, "tensor", 1, 0, tiled=True)
    expert_parts, router_part, mixed_grad = lax.optimization_barrier(
        (expert_parts, router_part, mixed_grad)
    )
    expert_grads = reduce_experts(expert_parts)
    router_and_gain = lax.psum_scatter(
        jnp.concatenate([router_part, gain_two_grad[:, None]], axis=1),
        ("dp", "tensor"),
        scatter_dimension=0,
        tiled=True,
    )
    router_weight_grad = router_and_gain[:, : router_part.shape[1]]
    mixture_gain_grad = router_and_gain[:, router_part.shape[1]]
    output_part = jnp.einsum(
        "tf,td->fd", mixed_own, attended_grad, preferred_element_type=jnp.float32
    ).astype(jnp.bfloat16)
    output_part = lax.psum_scatter(output_part, "dp", scatter_dimension=1, tiled=True)
    mixed_grad = mixed_grad.reshape(TOK_GRP, local_groups, group_ratio, HD)
    output_weight_grad = lax.psum_scatter(
        output_part, "tensor", scatter_dimension=0, tiled=True
    ).astype(jnp.float32)
    key_grad = jnp.zeros((TOK_GRP, local_groups, HD), jnp.float32)
    value_grad = jnp.zeros((TOK_GRP, local_groups, HD), jnp.float32)
    query_blocks = []
    for block_index in range(block_count):
        row_start = block_index * QBLK
        key_end = row_start + QBLK
        scores, queries = block_scores(
            query_rot, key_rot, segments, row_start, key_end, local_groups, group_ratio
        )
        soft_full = jnp.exp(scores - logsum_blocks[block_index])
        soft_low = soft_full.astype(jnp.bfloat16)
        out_block = mixed_grad[row_start:key_end]
        weight_grad = jnp.einsum(
            "qgrd,kgd->grqk", out_block, value_low[:key_end], preferred_element_type=jnp.float32
        )
        delta = jnp.sum(soft_full * weight_grad, axis=-1, keepdims=True)
        score_grad = (soft_full * (weight_grad - delta)).astype(jnp.bfloat16)
        query_blocks.append(
            jnp.einsum(
                "grqk,kgd->qgrd", score_grad, key_rot[:key_end], preferred_element_type=jnp.float32
            )
            * ATTN_SCALE
        )
        key_grad = key_grad.at[:key_end].add(
            jnp.einsum("grqk,qgrd->kgd", score_grad, queries, preferred_element_type=jnp.float32)
            * ATTN_SCALE
        )
        value_grad = value_grad.at[:key_end].add(
            jnp.einsum("grqk,qgrd->kgd", soft_low, out_block, preferred_element_type=jnp.float32)
        )
    query_rot_grad = jnp.concatenate(query_blocks, axis=0).reshape(TOK_GRP, local_heads, HD)
    query_grad = (
        rotate_back(query_rot_grad, cosine_table, sine_table)
        .astype(jnp.bfloat16)
        .reshape(TOK_GRP, local_heads * HD)
    )
    key_grad_low = (
        rotate_back(key_grad, cosine_table, sine_table)
        .astype(jnp.bfloat16)
        .reshape(TOK_GRP, local_groups * HD)
    )
    value_grad_low = value_grad.astype(jnp.bfloat16).reshape(TOK_GRP, local_groups * HD)
    projection_grad = jnp.concatenate([query_grad, key_grad_low, value_grad_low], axis=1)
    projection_grad_own = lax.all_to_all(projection_grad, "tensor", 0, 1, tiled=True)
    (
        projection_grad_own,
        expert_grads,
        router_weight_grad,
        output_weight_grad,
        mixture_gain_grad,
    ) = lax.optimization_barrier(
        (
            projection_grad_own,
            expert_grads,
            router_weight_grad,
            output_weight_grad,
            mixture_gain_grad,
        )
    )
    gate_weight_grad, up_weight_grad, down_weight_grad = expert_grads
    normed_grad = jnp.einsum(
        "tf,df->td", projection_grad_own, projection_all, preferred_element_type=jnp.float32
    )
    query_part = jnp.einsum(
        "td,tf->df", normed_full, query_grad, preferred_element_type=jnp.float32
    )
    key_part = jnp.einsum(
        "td,tf->df", normed_full, key_grad_low, preferred_element_type=jnp.float32
    )
    value_part = jnp.einsum(
        "td,tf->df", normed_full, value_grad_low, preferred_element_type=jnp.float32
    )
    projection_parts = jnp.concatenate(
        [query_part, key_part, value_part], axis=1
    ).astype(jnp.bfloat16)
    projection_parts, normed_grad = lax.optimization_barrier((projection_parts, normed_grad))
    input_norm_grad, gain_one_grad = rms_backward(normed_grad, unit_one, inverse_one, gain_one)
    input_grad = middle_grad + input_norm_grad
    projection_grads = lax.psum_scatter(
        projection_parts, "dp", scatter_dimension=0, tiled=True
    ).astype(jnp.float32)
    query_width, key_width = query_part.shape[1], key_part.shape[1]
    query_weight_grad = projection_grads[:, :query_width]
    key_weight_grad = projection_grads[:, query_width : query_width + key_width]
    value_weight_grad = projection_grads[:, query_width + key_width :]

    attention_gain_grad = lax.psum_scatter(
        lax.psum_scatter(gain_one_grad, "dp", scatter_dimension=0, tiled=True),
        "tensor",
        scatter_dimension=0,
        tiled=True,
    )
    return (
        block_output,
        input_grad,
        attention_gain_grad,
        query_weight_grad,
        key_weight_grad,
        value_weight_grad,
        output_weight_grad,
        mixture_gain_grad,
        router_weight_grad,
        gate_weight_grad,
        up_weight_grad,
        down_weight_grad,
    )


def solution(mesh):
    in_specs = (
        P(("dp", "tensor"), None),
        P(("dp", "tensor"), None),
        P("dp", None),
        P("dp", None),
        P("dp", None),
        P("dp"),
        P("dp", "tensor"),
        P("dp", "tensor"),
        P("dp", "tensor"),
        P("tensor", "dp"),
        P("dp"),
        P("dp", None),
        P("tensor", "dp", None),
        P("tensor", "dp", None),
        P("tensor", None, "dp"),
    )
    out_specs = (
        P(("dp", "tensor"), None),
        P(("dp", "tensor"), None),
        P(("dp", "tensor")),
        P("dp", "tensor"),
        P("dp", "tensor"),
        P("dp", "tensor"),
        P("tensor", "dp"),
        P(("dp", "tensor")),
        P(("dp", "tensor"), None),
        P("tensor", "dp", None),
        P("tensor", "dp", None),
        P("tensor", None, "dp"),
    )
    return jax.shard_map(local, mesh=mesh, in_specs=in_specs, out_specs=out_specs, check_vma=False)
```

```python
import jax
import jax.numpy as jnp
from jax import lax
from jax.experimental import pallas as pl
from jax.experimental.pallas import tpu as pltpu
from jax.sharding import PartitionSpec as P

D = 1536
HD = 64
EXPERTS = 40
TOPK = 8
PROMPT = 2048
NCONT = 4
QBLK = 512
TOK_GRP = 3072
CAP = 768


ATTN_SCALE = 0.015625
RESIDUAL_SCALE = 0.22
NORM_EPS = 1e-06
ROPE_BASE = 10000.0
MASKED = -1e30
HIGHEST = lax.Precision.HIGHEST


def rms_forward(values, gain_row):
    inverse_rms = lax.rsqrt(jnp.mean(values * values, axis=-1, keepdims=True) + NORM_EPS)
    unit_rows = values * inverse_rms
    return (unit_rows * gain_row, unit_rows, inverse_rms)


def rms_backward(gradient, unit_rows, inverse_rms, gain_row):
    gain_grad = jnp.sum(gradient * unit_rows, axis=0)
    scaled = gradient * gain_row
    mean_term = jnp.mean(scaled * unit_rows, axis=-1, keepdims=True)
    return (inverse_rms * (scaled - unit_rows * mean_term), gain_grad)


def group_layout(segment_row, prompt_length):
    cont_length = segment_row.shape[0]
    segment_marks = (segment_row[:, None] == jnp.arange(NCONT, dtype=jnp.int32)[None, :]).astype(
        jnp.int32
    )
    segment_sizes = jnp.sum(segment_marks, axis=0)
    segment_starts = jnp.cumsum(segment_sizes) - segment_sizes
    token_starts = jnp.sum(segment_marks * segment_starts[None, :], axis=1)
    inside = jnp.arange(cont_length, dtype=jnp.int32) - token_starts
    positions = jnp.concatenate(
        [jnp.arange(prompt_length, dtype=jnp.int32), prompt_length + inside]
    )
    segments = jnp.concatenate([jnp.zeros((prompt_length,), jnp.int32), segment_row + 1])
    return (positions, segments)


def allowed(query_index, query_segment, key_index, key_segment):
    causal = key_index[None, :] <= query_index[:, None]
    shared = (key_segment[None, :] == 0) | (key_segment[None, :] == query_segment[:, None])
    return causal & shared


def rope_tables(positions, head_size):
    halfway = head_size // 2
    frequency = ROPE_BASE ** (-(2.0 * jnp.arange(halfway, dtype=jnp.float32)) / head_size)
    angles = positions.astype(jnp.float32)[:, None] * frequency[None, :]
    return (jnp.cos(angles), jnp.sin(angles))


def rotate(values, cosine_table, sine_table):
    halfway = values.shape[-1] // 2
    first_half = values[..., :halfway]
    second_half = values[..., halfway:]
    cosine_part = cosine_table[:, None, :]
    sine_part = sine_table[:, None, :]
    return jnp.concatenate(
        [
            first_half * cosine_part - second_half * sine_part,
            second_half * cosine_part + first_half * sine_part,
        ],
        axis=-1,
    )


def rotate_back(gradient, cosine_table, sine_table):
    halfway = gradient.shape[-1] // 2
    first_half = gradient[..., :halfway]
    second_half = gradient[..., halfway:]
    cosine_part = cosine_table[:, None, :]
    sine_part = sine_table[:, None, :]
    return jnp.concatenate(
        [
            first_half * cosine_part + second_half * sine_part,
            second_half * cosine_part - first_half * sine_part,
        ],
        axis=-1,
    )


def silu_slope(values):
    sigmoid_part = jax.nn.sigmoid(values)
    return sigmoid_part * (1.0 + values * (1.0 - sigmoid_part))


def route_slots(expert_row, order_row, first_slot, slot_count):
    pair_count = expert_row.shape[0] * expert_row.shape[1]
    ordered = table_lookup(expert_row.reshape(pair_count), order_row)
    onehot = ordered[:, None] == jnp.arange(EXPERTS, dtype=jnp.int32)[None, :]
    rank_block = 256
    blocks = pair_count // rank_block
    pair_marks = onehot.astype(jnp.bfloat16).reshape(blocks, rank_block, EXPERTS)
    lower_ones = (jnp.arange(rank_block)[:, None] >= jnp.arange(rank_block)[None, :]).astype(
        jnp.bfloat16
    )
    within = jnp.einsum(
        "ij,bje->bie", lower_ones, pair_marks, preferred_element_type=jnp.float32
    ).astype(jnp.int32)
    totals = within[:, -1, :]
    before = jnp.cumsum(totals, axis=0) - totals
    counts = (within + before[:, None, :]).reshape(pair_count, EXPERTS)
    pair_rank = jnp.sum(jnp.where(onehot, counts, 0), axis=1) - 1
    local_slot = ordered * CAP + pair_rank - first_slot
    kept = (pair_rank < CAP) & (local_slot >= 0) & (local_slot < slot_count)
    local_slot = jnp.where(kept, local_slot, -1)
    return invert_slots(local_slot, order_row, slot_count)


def _gather_rows_kernel(tok_ref, *refs):
    count = (len(refs) - 1) // 4
    sources, outs = refs[:count], refs[count : 2 * count]
    copies, rows_bufs, sem = refs[2 * count : 3 * count], refs[3 * count : 4 * count], refs[-1]
    rows = rows_bufs[0].shape[0]
    step = pl.program_id(0)

    @pl.when(step == 0)
    def _():
        for source, copy in zip(sources, copies):
            transfer = pltpu.make_async_copy(source, copy, sem)
            transfer.start()
            transfer.wait()

    base = step * rows

    def body(s, carry):
        t = tok_ref[base + s]
        for copy, rows_buf in zip(copies, rows_bufs):
            rows_buf[pl.ds(s, 1), :] = copy[pl.ds(t, 1), :]
        return carry

    lax.fori_loop(0, rows, body, 0, unroll=8)
    for out, rows_buf in zip(outs, rows_bufs):
        out[...] = rows_buf[...].astype(out.dtype)


def gather_rows(tok, sources, rows, out_dtypes):
    blocks = tok.shape[0] // rows
    return pl.pallas_call(
        _gather_rows_kernel,
        grid_spec=pltpu.PrefetchScalarGridSpec(
            num_scalar_prefetch=1,
            grid=(blocks,),
            in_specs=[pl.BlockSpec(memory_space=pl.ANY) for _ in sources],
            out_specs=[
                pl.BlockSpec((rows, source.shape[1]), lambda b, tok: (b, 0)) for source in sources
            ],
            scratch_shapes=[pltpu.VMEM(source.shape, jnp.float32) for source in sources]
            + [pltpu.VMEM((rows, source.shape[1]), jnp.float32) for source in sources]
            + [pltpu.SemaphoreType.DMA(())],
        ),
        out_shape=[
            jax.ShapeDtypeStruct((tok.shape[0], source.shape[1]), dtype)
            for source, dtype in zip(sources, out_dtypes)
        ],
        compiler_params=pltpu.CompilerParams(vmem_limit_bytes=56 * 1024 * 1024),
    )(tok, *sources)


def _combine_rows_kernel(tok_ref, *refs):
    count = (len(refs) - 1) // 4
    addends, outs = refs[:count], refs[count : 2 * count]
    totals, rows_bufs, sem = refs[2 * count : 3 * count], refs[3 * count : 4 * count], refs[-1]
    rows = rows_bufs[0].shape[0]
    step = pl.program_id(0)

    @pl.when(step == 0)
    def _():
        for total in totals:
            total[...] = jnp.zeros_like(total)

    for addend, rows_buf in zip(addends, rows_bufs):
        rows_buf[...] = addend[...].astype(jnp.float32)
    base = step * rows

    def body(s, carry):
        t = tok_ref[base + s]
        for total, rows_buf in zip(totals, rows_bufs):
            total[pl.ds(t, 1), :] += rows_buf[pl.ds(s, 1), :]
        return carry

    lax.fori_loop(0, rows, body, 0, unroll=8)

    @pl.when(step == pl.num_programs(0) - 1)
    def _():
        for total, out in zip(totals, outs):
            transfer = pltpu.make_async_copy(total, out, sem)
            transfer.start()
            transfer.wait()


def combine_rows(tok, addends, rows, total_rows):
    blocks = tok.shape[0] // rows
    return pl.pallas_call(
        _combine_rows_kernel,
        grid_spec=pltpu.PrefetchScalarGridSpec(
            num_scalar_prefetch=1,
            grid=(blocks,),
            in_specs=[
                pl.BlockSpec((rows, addend.shape[1]), lambda b, tok: (b, 0)) for addend in addends
            ],
            out_specs=[pl.BlockSpec(memory_space=pl.ANY) for _ in addends],
            scratch_shapes=[
                pltpu.VMEM((total_rows, addend.shape[1]), jnp.float32) for addend in addends
            ]
            + [pltpu.VMEM((rows, addend.shape[1]), jnp.float32) for addend in addends]
            + [pltpu.SemaphoreType.DMA(())],
        ),
        out_shape=[
            jax.ShapeDtypeStruct((total_rows, addend.shape[1]), jnp.float32) for addend in addends
        ],
        compiler_params=pltpu.CompilerParams(vmem_limit_bytes=56 * 1024 * 1024),
    )(tok, *addends)


def table_lookup(table, index):
    lanes = 128
    high_count = table.shape[0] // lanes
    low_marks = (index[:, None] % lanes == jnp.arange(lanes)[None, :]).astype(jnp.bfloat16)
    picked = jnp.dot(
        low_marks,
        table.reshape(high_count, lanes).astype(jnp.bfloat16).T,
        preferred_element_type=jnp.float32,
    )
    high_marks = index[:, None] // lanes == jnp.arange(high_count)[None, :]
    return jnp.sum(jnp.where(high_marks, picked, 0.0), axis=1).astype(jnp.int32)


def invert_slots(local_slot, values, slot_count):
    lanes = 128
    high_count = slot_count // lanes
    column_marks = (local_slot[:, None] // lanes == jnp.arange(high_count)[None, :]).astype(
        jnp.bfloat16
    )
    lane_marks = local_slot[:, None] % lanes == jnp.arange(lanes)[None, :]
    shifted = values + 1
    parts = []
    for digit in (shifted // 256, shifted % 256):
        spread = jnp.where(lane_marks, digit[:, None], 0).astype(jnp.bfloat16)
        parts.append(
            jnp.einsum("ic,il->cl", column_marks, spread, preferred_element_type=jnp.float32)
        )
    return (256.0 * parts[0] + parts[1]).astype(jnp.int32).reshape(slot_count) - 1


def block_scores(query_rot, key_rot, segments, row_start, key_end, local_groups, group_ratio):
    queries = query_rot[row_start:key_end].reshape(
        key_end - row_start, local_groups, group_ratio, HD
    )
    raw_scores = (
        jnp.einsum("qgrd,kgd->grqk", queries, key_rot[:key_end], preferred_element_type=jnp.float32)
        * ATTN_SCALE
    )
    visible = allowed(
        jnp.arange(row_start, key_end, dtype=jnp.int32),
        segments[row_start:key_end],
        jnp.arange(key_end, dtype=jnp.int32),
        segments[:key_end],
    )
    return (jnp.where(visible[None, None], raw_scores, MASKED), queries)


def fetch_experts(gate_weight, up_weight, down_weight):
    return (
        lax.all_gather(gate_weight, "dp", axis=1, tiled=True),
        lax.all_gather(up_weight, "dp", axis=1, tiled=True),
        lax.all_gather(down_weight, "dp", axis=2, tiled=True),
    )


def reduce_experts(grads):
    return (
        lax.psum_scatter(grads[0], "dp", scatter_dimension=1, tiled=True).astype(jnp.float32),
        lax.psum_scatter(grads[1], "dp", scatter_dimension=1, tiled=True).astype(jnp.float32),
        jnp.swapaxes(
            lax.psum_scatter(grads[2], "dp", scatter_dimension=1, tiled=True).astype(jnp.float32),
            1,
            2,
        ),
    )


def local(
    hidden_in,
    out_grad,
    segment_ids,
    expert_ids,
    fill_order,
    attention_gain,
    query_weight,
    key_weight,
    value_weight,
    output_weight,
    mixture_gain,
    router_weight,
    gate_weight,
    up_weight,
    down_weight,
):
    local_heads = query_weight.shape[1] // HD
    local_groups = key_weight.shape[1] // HD
    group_ratio = local_heads // local_groups
    block_count = TOK_GRP // QBLK
    local_experts = gate_weight.shape[0]
    gain_one, query_full, key_full, value_full, gain_two, router_full = (
        lax.all_gather(attention_gain, "dp", axis=0, tiled=True),
        lax.all_gather(query_weight, "dp", axis=0, tiled=True),
        lax.all_gather(key_weight, "dp", axis=0, tiled=True),
        lax.all_gather(value_weight, "dp", axis=0, tiled=True),
        lax.all_gather(mixture_gain, "dp", axis=0, tiled=True),
        lax.all_gather(router_weight, "dp", axis=0, tiled=True),
    )
    output_all = lax.all_gather(
        lax.all_gather(output_weight, "tensor", axis=0, tiled=True), "dp", axis=1, tiled=True
    )
    gain_one = gain_one.astype(jnp.float32)
    gain_two = gain_two.astype(jnp.float32)
    residual = hidden_in.astype(jnp.float32)
    normed_shard, unit_one, inverse_one = rms_forward(residual, gain_one)
    normed_full = lax.all_gather(normed_shard.astype(jnp.bfloat16), "tensor", axis=0, tiled=True)
    gate_weight, up_weight, normed_full = lax.optimization_barrier(
        (gate_weight, up_weight, normed_full)
    )
    gate_full = lax.all_gather(gate_weight, "dp", axis=1, tiled=True)
    up_full = lax.all_gather(up_weight, "dp", axis=1, tiled=True)
    positions, segments = group_layout(segment_ids[0], PROMPT)
    cosine_table, sine_table = rope_tables(positions, HD)
    query_pre = jnp.dot(normed_full, query_full, preferred_element_type=jnp.float32).reshape(
        TOK_GRP, local_heads, HD
    )
    key_pre = jnp.dot(normed_full, key_full, preferred_element_type=jnp.float32).reshape(
        TOK_GRP, local_groups, HD
    )
    value_low = (
        jnp.dot(normed_full, value_full, preferred_element_type=jnp.float32)
        .astype(jnp.bfloat16)
        .reshape(TOK_GRP, local_groups, HD)
    )
    query_rot = rotate(query_pre, cosine_table, sine_table).astype(jnp.bfloat16)
    key_rot = rotate(key_pre, cosine_table, sine_table).astype(jnp.bfloat16)
    mixed_blocks = []
    logsum_blocks = []
    for block_index in range(block_count):
        row_start = block_index * QBLK
        key_end = row_start + QBLK
        scores, queries = block_scores(
            query_rot, key_rot, segments, row_start, key_end, local_groups, group_ratio
        )
        top_score = jnp.max(scores, axis=-1, keepdims=True)
        shifted_exp = jnp.exp(scores - top_score)
        total_exp = jnp.sum(shifted_exp, axis=-1, keepdims=True)
        soft_weights = (shifted_exp / total_exp).astype(jnp.bfloat16)
        logsum_blocks.append(top_score + jnp.log(total_exp))
        mixed = jnp.einsum(
            "grqk,kgd->qgrd", soft_weights, value_low[:key_end], preferred_element_type=jnp.float32
        )
        mixed_blocks.append(mixed.astype(jnp.bfloat16).reshape(QBLK, local_heads * HD))
    mixed_full = jnp.concatenate(mixed_blocks, axis=0)
    mixed_full, gate_full, up_full = lax.optimization_barrier((mixed_full, gate_full, up_full))
    mixed_own = lax.all_to_all(mixed_full, "tensor", 0, 1, tiled=True)
    attended = jnp.dot(mixed_own, output_all, preferred_element_type=jnp.float32)
    middle = residual + RESIDUAL_SCALE * attended
    normed_two, unit_two, inverse_two = rms_forward(middle, gain_two)
    mixture_in = lax.all_gather(normed_two.astype(jnp.bfloat16), "tensor", axis=0, tiled=True)
    down_weight, mixture_in = lax.optimization_barrier((down_weight, mixture_in))
    down_full = lax.all_gather(down_weight, "dp", axis=2, tiled=True)
    logits = jnp.dot(mixture_in, router_full, preferred_element_type=jnp.float32)
    routed_marks = (
        expert_ids[:, :, None] == jnp.arange(EXPERTS, dtype=jnp.int32)[None, None, :]
    ).astype(jnp.float32)
    routed = jnp.sum(routed_marks * logits[:, None, :], axis=-1)
    gates = jax.nn.softmax(routed, axis=-1)
    slot_count = local_experts * CAP
    first_slot = lax.axis_index("tensor") * slot_count
    slot_pair = route_slots(expert_ids, fill_order[0], first_slot, slot_count)
    slot_valid = slot_pair >= 0
    safe_pair = jnp.maximum(slot_pair, 0)
    slot_token = safe_pair // TOPK
    slot_choice = safe_pair % TOPK
    side_lanes = 128
    gate_table = jnp.pad(gates, ((0, 0), (0, side_lanes - TOPK)))
    inputs, gate_rows = gather_rows(
        slot_token,
        (mixture_in.astype(jnp.float32), gate_table),
        CAP,
        (jnp.bfloat16, jnp.float32),
    )
    inputs = inputs.reshape(local_experts, CAP, D)
    choice_marks = slot_choice[:, None] == jnp.arange(side_lanes)[None, :]
    slot_gate = jnp.sum(jnp.where(choice_marks, gate_rows, 0.0), axis=1)
    slot_gate = jnp.where(slot_valid, slot_gate, 0.0).reshape(local_experts, CAP, 1)
    gate_pre = jnp.einsum("ecd,edf->ecf", inputs, gate_full, preferred_element_type=jnp.float32)
    up_pre = jnp.einsum("ecd,edf->ecf", inputs, up_full, preferred_element_type=jnp.float32)
    activated = jax.nn.silu(gate_pre)
    hidden_units = (slot_gate * activated * up_pre).astype(jnp.bfloat16)
    expert_out = jnp.einsum(
        "ecf,efd->ecd", hidden_units, down_full, preferred_element_type=jnp.float32
    )
    (mixture_sum,) = combine_rows(slot_token, (expert_out.reshape(slot_count, D),), CAP, TOK_GRP)
    out_grad_held, down_full = lax.optimization_barrier((out_grad, down_full))
    cotangent_full = lax.all_gather(out_grad_held, "tensor", axis=0, tiled=True)
    scaled_cotangent = (
        (RESIDUAL_SCALE * cotangent_full.astype(jnp.float32)).astype(jnp.bfloat16).astype(jnp.float32)
    )
    scaled_cotangent, mixture_sum, projection_local = lax.optimization_barrier(
        (
            scaled_cotangent,
            mixture_sum,
            jnp.concatenate([query_weight, key_weight, value_weight], axis=1),
        )
    )
    projection_all = lax.all_gather(
        lax.all_gather(projection_local, "tensor", axis=1, tiled=True), "dp", axis=0, tiled=True
    )
    mixture_part = lax.psum_scatter(
        mixture_sum.astype(jnp.bfloat16), "tensor", scatter_dimension=0, tiled=True
    ).astype(jnp.float32)
    (out_rows,) = gather_rows(slot_token, (scaled_cotangent,), CAP, (jnp.bfloat16,))
    out_rows = out_rows.reshape(local_experts, CAP, D)
    hidden_grad = jnp.einsum("ecd,efd->ecf", out_rows, down_full, preferred_element_type=jnp.float32)
    gate_grad_slot = jnp.sum(activated * up_pre * hidden_grad, axis=-1).reshape(slot_count)
    gate_grad_rows = jnp.where(
        choice_marks & slot_valid[:, None], gate_grad_slot[:, None], 0.0
    )
    product_grad = slot_gate * hidden_grad
    gate_pre_grad = (product_grad * up_pre * silu_slope(gate_pre)).astype(jnp.bfloat16)
    up_pre_grad = (product_grad * activated).astype(jnp.bfloat16)
    input_rows = jnp.einsum(
        "ecf,edf->ecd", gate_pre_grad, gate_full, preferred_element_type=jnp.float32
    ) + jnp.einsum("ecf,edf->ecd", up_pre_grad, up_full, preferred_element_type=jnp.float32)
    input_rows = input_rows.astype(jnp.bfloat16).reshape(slot_count, D)
    grad_in_mixture, gate_grad_table = combine_rows(
        slot_token, (input_rows, gate_grad_rows), CAP, TOK_GRP
    )
    (inputs, gate_pre_grad, up_pre_grad, hidden_units, out_rows), grad_in_mixture, projection_all = (
        lax.optimization_barrier(
            (
                (inputs, gate_pre_grad, up_pre_grad, hidden_units, out_rows),
                grad_in_mixture,
                projection_all,
            )
        )
    )
    expert_parts = (
        jnp.einsum("ecd,ecf->edf", inputs, gate_pre_grad, preferred_element_type=jnp.float32),
        jnp.einsum("ecd,ecf->edf", inputs, up_pre_grad, preferred_element_type=jnp.float32),
        jnp.einsum("ecd,ecf->edf", out_rows, hidden_units, preferred_element_type=jnp.float32),
    )
    expert_parts = tuple(part.astype(jnp.bfloat16) for part in expert_parts)
    gates_grad = gate_grad_table[:, :TOPK]
    routed_grad = gates * (gates_grad - jnp.sum(gates * gates_grad, axis=-1, keepdims=True))
    logits_grad = jnp.sum(routed_marks * routed_grad[:, :, None], axis=1)
    router_part = jnp.einsum(
        "td,te->de", mixture_in, logits_grad, precision=HIGHEST, preferred_element_type=jnp.float32
    )
    grad_in_mixture = grad_in_mixture + jnp.einsum(
        "te,de->td", logits_grad, router_full.astype(jnp.float32), precision=HIGHEST
    )
    mixture_grad_low, mixture_part = lax.optimization_barrier(
        (grad_in_mixture.astype(jnp.bfloat16), mixture_part)
    )
    block_output = (middle + RESIDUAL_SCALE * mixture_part).astype(jnp.bfloat16)
    mixture_grad_shard = lax.psum_scatter(
        mixture_grad_low, "tensor", scatter_dimension=0, tiled=True
    ).astype(jnp.float32)
    middle_norm_grad, gain_two_grad = rms_backward(
        mixture_grad_shard, unit_two, inverse_two, gain_two
    )
    middle_grad = out_grad.astype(jnp.float32) + middle_norm_grad
    attended_grad = (RESIDUAL_SCALE * middle_grad).astype(jnp.bfloat16)
    mixed_grad_own = jnp.einsum(
        "td,fd->tf", attended_grad, output_all, preferred_element_type=jnp.float32
    ).astype(jnp.bfloat16)
    mixed_grad = lax.all_to_all(mixed_grad_own, "tensor", 1, 0, tiled=True)
    expert_parts, router_part, mixed_grad = lax.optimization_barrier(
        (expert_parts, router_part, mixed_grad)
    )
    expert_grads = reduce_experts(expert_parts)
    router_and_gain = lax.psum_scatter(
        lax.psum_scatter(
            jnp.concatenate([router_part, gain_two_grad[:, None]], axis=1),
            "dp",
            scatter_dimension=0,
            tiled=True,
        ),
        "tensor",
        scatter_dimension=0,
        tiled=True,
    )
    router_weight_grad = router_and_gain[:, : router_part.shape[1]]
    mixture_gain_grad = router_and_gain[:, router_part.shape[1]]
    output_part = jnp.einsum(
        "tf,td->fd", mixed_own, attended_grad, preferred_element_type=jnp.float32
    ).astype(jnp.bfloat16)
    output_part = lax.psum_scatter(output_part, "dp", scatter_dimension=1, tiled=True)
    mixed_grad = mixed_grad.reshape(TOK_GRP, local_groups, group_ratio, HD)
    output_weight_grad = lax.psum_scatter(
        output_part, "tensor", scatter_dimension=0, tiled=True
    ).astype(jnp.float32)
    key_grad = jnp.zeros((TOK_GRP, local_groups, HD), jnp.float32)
    value_grad = jnp.zeros((TOK_GRP, local_groups, HD), jnp.float32)
    query_blocks = []
    for block_index in range(block_count):
        row_start = block_index * QBLK
        key_end = row_start + QBLK
        scores, queries = block_scores(
            query_rot, key_rot, segments, row_start, key_end, local_groups, group_ratio
        )
        soft_full = jnp.exp(scores - logsum_blocks[block_index])
        soft_low = soft_full.astype(jnp.bfloat16)
        out_block = mixed_grad[row_start:key_end]
        weight_grad = jnp.einsum(
            "qgrd,kgd->grqk", out_block, value_low[:key_end], preferred_element_type=jnp.float32
        )
        delta = jnp.sum(soft_full * weight_grad, axis=-1, keepdims=True)
        score_grad = (soft_full * (weight_grad - delta)).astype(jnp.bfloat16)
        query_blocks.append(
            jnp.einsum(
                "grqk,kgd->qgrd", score_grad, key_rot[:key_end], preferred_element_type=jnp.float32
            )
            * ATTN_SCALE
        )
        key_grad = key_grad.at[:key_end].add(
            jnp.einsum("grqk,qgrd->kgd", score_grad, queries, preferred_element_type=jnp.float32)
            * ATTN_SCALE
        )
        value_grad = value_grad.at[:key_end].add(
            jnp.einsum("grqk,qgrd->kgd", soft_low, out_block, preferred_element_type=jnp.float32)
        )
    query_rot_grad = jnp.concatenate(query_blocks, axis=0).reshape(TOK_GRP, local_heads, HD)
    query_grad = (
        rotate_back(query_rot_grad, cosine_table, sine_table)
        .astype(jnp.bfloat16)
        .reshape(TOK_GRP, local_heads * HD)
    )
    key_grad_low = (
        rotate_back(key_grad, cosine_table, sine_table)
        .astype(jnp.bfloat16)
        .reshape(TOK_GRP, local_groups * HD)
    )
    value_grad_low = value_grad.astype(jnp.bfloat16).reshape(TOK_GRP, local_groups * HD)
    projection_grad = jnp.concatenate([query_grad, key_grad_low, value_grad_low], axis=1)
    projection_grad_own = lax.all_to_all(projection_grad, "tensor", 0, 1, tiled=True)
    (
        projection_grad_own,
        expert_grads,
        router_weight_grad,
        output_weight_grad,
        mixture_gain_grad,
    ) = lax.optimization_barrier(
        (
            projection_grad_own,
            expert_grads,
            router_weight_grad,
            output_weight_grad,
            mixture_gain_grad,
        )
    )
    gate_weight_grad, up_weight_grad, down_weight_grad = expert_grads
    normed_grad = jnp.einsum(
        "tf,df->td", projection_grad_own, projection_all, preferred_element_type=jnp.float32
    )
    query_part = jnp.einsum(
        "td,tf->df", normed_full, query_grad, preferred_element_type=jnp.float32
    )
    key_part = jnp.einsum(
        "td,tf->df", normed_full, key_grad_low, preferred_element_type=jnp.float32
    )
    value_part = jnp.einsum(
        "td,tf->df", normed_full, value_grad_low, preferred_element_type=jnp.float32
    )
    projection_parts = jnp.concatenate(
        [query_part, key_part, value_part], axis=1
    ).astype(jnp.bfloat16)
    projection_parts, normed_grad = lax.optimization_barrier((projection_parts, normed_grad))
    input_norm_grad, gain_one_grad = rms_backward(normed_grad, unit_one, inverse_one, gain_one)
    input_grad = middle_grad + input_norm_grad
    projection_grads = lax.psum_scatter(
        projection_parts, "dp", scatter_dimension=0, tiled=True
    ).astype(jnp.float32)
    query_width, key_width = query_part.shape[1], key_part.shape[1]
    query_weight_grad = projection_grads[:, :query_width]
    key_weight_grad = projection_grads[:, query_width : query_width + key_width]
    value_weight_grad = projection_grads[:, query_width + key_width :]

    attention_gain_grad = lax.psum_scatter(
        lax.psum_scatter(gain_one_grad, "dp", scatter_dimension=0, tiled=True),
        "tensor",
        scatter_dimension=0,
        tiled=True,
    )
    return (
        block_output,
        input_grad,
        attention_gain_grad,
        query_weight_grad,
        key_weight_grad,
        value_weight_grad,
        output_weight_grad,
        mixture_gain_grad,
        router_weight_grad,
        gate_weight_grad,
        up_weight_grad,
        down_weight_grad,
    )


def solution(mesh):
    in_specs = (
        P(("dp", "tensor"), None),
        P(("dp", "tensor"), None),
        P("dp", None),
        P("dp", None),
        P("dp", None),
        P("dp"),
        P("dp", "tensor"),
        P("dp", "tensor"),
        P("dp", "tensor"),
        P("tensor", "dp"),
        P("dp"),
        P("dp", None),
        P("tensor", "dp", None),
        P("tensor", "dp", None),
        P("tensor", None, "dp"),
    )
    out_specs = (
        P(("dp", "tensor"), None),
        P(("dp", "tensor"), None),
        P(("dp", "tensor")),
        P("dp", "tensor"),
        P("dp", "tensor"),
        P("dp", "tensor"),
        P("tensor", "dp"),
        P(("dp", "tensor")),
        P(("dp", "tensor"), None),
        P("tensor", "dp", None),
        P("tensor", "dp", None),
        P("tensor", None, "dp"),
    )
    return jax.shard_map(local, mesh=mesh, in_specs=in_specs, out_specs=out_specs, check_vma=False)
```
